32 devices in a mesh: grp: 2 (over y), slab: 4 (over z), head: 2 (over x), seq: 2 (over core).
Axes of the slice: x: 2, y: 2, z: 4, core: 2. Of those that a mesh axis runs over, the one named last changes fastest.
Arguments:
- queries: bfloat16 [1024, 5120], P(('grp', 'seq'), 'head'), parts along dimension 0, may hold values from -140 to 140
- query_gain: float32 [5120], P('head'), may hold values from 1.5 to 3
- cache_keys: bfloat16 [4096, 5120], P(('grp', 'slab'), 'head'), parts along dimension 0, may hold values from -120 to 120
- cache_values: bfloat16 [4096, 5120], P(('grp', 'slab'), 'head'), parts along dimension 0, may hold values from -6 to 6
- finished_keys: bfloat16 [1024, 5120], P(('grp', 'slab', 'seq'), 'head'), parts along dimension 0, may hold values from -6 to 6
- finished_values: bfloat16 [1024, 5120], P(('grp', 'slab', 'seq'), 'head'), parts along dimension 0, may hold values from -6 to 6
- new_keys: bfloat16 [1024, 5120], P(('grp', 'slab', 'seq'), 'head'), parts along dimension 0, may hold values from -6 to 6
- new_values: bfloat16 [1024, 5120], P(('grp', 'slab', 'seq'), 'head'), parts along dimension 0, may hold values from -6 to 6
- out_weight: bfloat16 [5120, 5120], P('head', 'slab'), may hold values from -0.25 to 0.25
- time_weight: float32 [256, 5120], P(None, ('slab', 'head')), may hold values from -0.375 to 0.375
- owner: int32 [2], P('grp'), parts along dimension 0, may hold values from 0 to 3
- step: int32 [2], P('grp'), parts along dimension 0, may hold values from 0 to 999
Outputs:
- branch: bfloat16 [1024, 5120], P(('grp', 'seq'), ('slab', 'head')), parts along dimension 0
The draws below stay inside these ranges and needn't reach their ends.
There are 2 independent parts, one for each index of `grp`. The reference program is written for one: setup_inputs(seed, part) draws one part's arguments, and reference() takes and returns one part's arrays. A program takes and returns all parts, laid end to end along the dimension named above; an argument that names none is the same for every part. Nothing has to cross between parts.
All inputs are finite; a program needn't handle non-finite values.
Results may differ from the reference program's by a relative error of at most 0.012.
Values may be sent and summed in bfloat16 or wider, within the bound.
A program may use at most 64 MiB of HBM per device.

```python
import math
import jax
import jax.numpy as jnp
from jax import lax

D = 5120
HEADS = 40
HD = 128
FREQ = 256
SPAN = 512
CACHE = 2048
N_SLAB = 4


def draw_cache_keys(key, part):
    shape_pair = (SPAN * N_SLAB, HEADS * HD)
    entries = jnp.clip(jax.random.normal(jax.random.fold_in(key, 11), shape_pair, jnp.float32), -4.5, 4.5)
    return entries.astype(jnp.bfloat16)


def draw_queries(key, part):
    width_total = HEADS * HD
    shape_pair = (SPAN, width_total)
    row_scale = jnp.exp(jax.random.uniform(jax.random.fold_in(key, 21), (SPAN, 1), jnp.float32, jnp.log(0.5), jnp.log(5.0)))
    column_rise = 3.0 ** (jnp.arange(width_total, dtype=jnp.float32) / (width_total - 1))
    jitter = jnp.exp(jax.random.uniform(jax.random.fold_in(key, 22), (width_total,), jnp.float32, jnp.log(0.5), jnp.log(2.0)))
    entries = jnp.clip(jax.random.normal(jax.random.fold_in(key, 23), shape_pair, jnp.float32), -4.5, 4.5)
    entries = entries * row_scale * column_rise * jitter
    return entries.astype(jnp.bfloat16)


def shard_levels(key, shape, cuts, least, largest):
    gain, own = 1.0, jax.random.fold_in(key, 6)
    for axis_at, blocks in cuts:
        draws = jnp.exp(jax.random.uniform(jax.random.fold_in(own, axis_at), (blocks,), jnp.float32, least / len(cuts), largest / len(cuts)))
        gain = gain * jnp.repeat(draws, shape[axis_at] // blocks).reshape([-1 if axis == axis_at else 1 for axis in range(len(shape))])
    return gain


def bell_draw(rng, dims, width, bound, pieces=(), kind=jnp.bfloat16):
    values = width * jax.random.normal(rng, dims, jnp.float32)
    if pieces:
        values = values * shard_levels(rng, dims, pieces, -0.22, 0.18)
    return jnp.clip(values, -bound, bound).astype(kind)


def setup_inputs(seed: int = 0, part: int = 0) -> dict:
    arg_keys = jax.random.split(jax.random.key(seed), 13)
    own_keys = jax.random.split(jax.random.fold_in(arg_keys[12], part), 13)
    return {
        "queries": draw_queries(jax.random.fold_in(jax.random.fold_in(arg_keys[12], part), 71), part),
        "query_gain": jnp.clip(jnp.exp(math.log(3.0) - 0.6931472 * jax.random.uniform(arg_keys[1], (HEADS * HD,), jnp.float32) ** shard_levels(arg_keys[1], (HEADS * HD,), ((0, 2),), -0.2, 0.2)), 1.5, 3.0),
        "cache_keys": draw_cache_keys(jax.random.fold_in(jax.random.fold_in(arg_keys[12], part), 71), part),
        "cache_values": bell_draw(own_keys[3], (CACHE, HEADS * HD), 1.0, 6.0, ((0, 4), (1, 2))),
        "finished_keys": bell_draw(own_keys[4], (SPAN, HEADS * HD), 1.0, 6.0, ((0, 8), (1, 2))),
        "finished_values": bell_draw(own_keys[5], (SPAN, HEADS * HD), 1.0, 6.0, ((0, 8), (1, 2))),
        "new_keys": bell_draw(own_keys[6], (SPAN, HEADS * HD), 1.0, 6.0, ((0, 8), (1, 2))),
        "new_values": bell_draw(own_keys[7], (SPAN, HEADS * HD), 1.0, 6.0, ((0, 8), (1, 2))),
        "out_weight": bell_draw(arg_keys[8], (HEADS * HD, D), (HEADS * HD // 8) ** -0.5, 0.25, ((0, 2), (1, 4))),
        "time_weight": bell_draw(arg_keys[9], (FREQ, D), FREQ ** -0.5, 0.375, ((1, 8),), jnp.float32),
        "owner": jax.random.randint(own_keys[10], (1,), 0, N_SLAB).astype(jnp.int32),
        "step": jax.random.randint(own_keys[11], (1,), 0, 1000).astype(jnp.int32),
    }


EPSILON = 1e-06

def reference(queries, query_gain, cache_keys, cache_values, finished_keys, finished_values, new_keys, new_values, out_weight, time_weight, owner, step):
    query_float = queries.astype(jnp.float32)
    inverse = lax.rsqrt(lax.optimization_barrier(jnp.mean(query_float * query_float, axis=1)) + EPSILON)
    normed = (query_float * inverse[:, None] * query_gain).astype(jnp.bfloat16)
    start_row = (owner[0] * SPAN).astype(jnp.int32)
    swapped_keys = lax.dynamic_update_slice(cache_keys, finished_keys, (start_row, jnp.int32(0)))
    swapped_values = lax.dynamic_update_slice(cache_values, finished_values, (start_row, jnp.int32(0)))
    all_keys = jnp.concatenate([swapped_keys, new_keys], axis=0)
    all_values = jnp.concatenate([swapped_values, new_values], axis=0)
    total_rows = CACHE + SPAN
    query_heads = normed.reshape(SPAN, HEADS, HD).transpose(1, 0, 2)
    key_heads = all_keys.reshape(total_rows, HEADS, HD).transpose(1, 0, 2)
    value_heads = all_values.reshape(total_rows, HEADS, HD).transpose(1, 0, 2)
    score_scale = 1.0 / HD ** 0.5

    def one_head(head_items):
        query_head, key_head, value_head = head_items
        scores = jnp.dot(query_head, key_head.T, preferred_element_type=jnp.float32) * score_scale
        row_top = lax.optimization_barrier(jnp.max(scores, axis=1, keepdims=True))
        raw_weights = jnp.exp(scores - row_top)
        row_mass = lax.optimization_barrier(jnp.sum(raw_weights, axis=1, keepdims=True))
        weighted = jnp.dot(raw_weights.astype(jnp.bfloat16), value_head, preferred_element_type=jnp.float32)
        return (weighted / row_mass).astype(jnp.bfloat16)
    attended = lax.map(one_head, (query_heads, key_heads, value_heads))
    weight_heads = out_weight.reshape(HEADS, HD, D)
    projected = jnp.einsum('hrd,hdc->rc', attended.astype(jnp.float32), weight_heads.astype(jnp.float32))
    half = FREQ // 2
    frequency = jnp.exp(-jnp.log(10000.0) * jnp.arange(half, dtype=jnp.float32) / half)
    phases = step[0].astype(jnp.float32) * frequency
    embedding = jnp.concatenate([jnp.cos(phases), jnp.sin(phases)])
    time_gate = 1.0 + jnp.dot(embedding, time_weight, precision=lax.Precision.HIGHEST)
    return (time_gate * projected).astype(jnp.bfloat16)
```

```python
import functools
import math

import jax
import jax.numpy as jnp
from jax import lax
from jax.experimental import pallas as pl
from jax.experimental.pallas import tpu as pltpu
from jax.sharding import PartitionSpec as P

HEADS = 40
HD = 128
EPSILON = 1e-06
LOW = -1e30
LAG = 5
MESH = pl.DeviceIdType.MESH
F32 = jnp.float32
BF16 = jnp.bfloat16


def kernel(
    dims,
    aligned,
    q_ref,
    gain_ref,
    ck_ref,
    cv_ref,
    fk_ref,
    fv_ref,
    nk_ref,
    nv_ref,
    w_ref,
    tw_ref,
    owner_ref,
    step_ref,
    out_ref,
    q,
    qg,
    gain,
    kc,
    vc,
    kf,
    vf,
    w,
    tw,
    squares,
    scale,
    own_o,
    own_s,
    pre_o,
    pre_s,
    suf_o,
    suf_s,
    right_o,
    right_s,
    left_o,
    left_s,
    att,
    acc,
    gate,
    xs,
    xr,
    load_sem,
    fresh_sem,
    fresh_send,
    fresh_recv,
    sq_send,
    sq_recv,
    right_send,
    right_recv,
    left_send,
    left_recv,
    x_send,
    x_recv,
    s_buf,
    p_buf,
    m_buf,
):
    n, heads_n, seq_n = dims
    rows, width = q_ref.shape
    hcount = width // HD
    z = lax.axis_index("slab")
    hx = lax.axis_index("head")
    sq = lax.axis_index("seq")

    groups = rows // HD
    chunks = groups * hcount
    loads = [
        pltpu.make_async_copy(src, dst, load_sem.at[i])
        for i, (src, dst) in enumerate(
            [(q_ref, q), (gain_ref, gain), (ck_ref, kc), (cv_ref, vc), (w_ref, w), (tw_ref, tw)]
        )
    ]
    loads[0].start()
    loads[1].start()
    barrier = pltpu.get_barrier_semaphore()
    for d in range(1, seq_n):
        pl.semaphore_signal(
            barrier, inc=1, device_id={"seq": lax.rem(sq + d, seq_n)}, device_id_type=MESH
        )
    for d in range(1, heads_n):
        pl.semaphore_signal(
            barrier, inc=1, device_id={"head": lax.rem(hx + d, heads_n)}, device_id_type=MESH
        )

    @pl.when(z > 0)
    def _():
        pl.semaphore_signal(barrier, inc=1, device_id={"slab": z - 1}, device_id_type=MESH)

    @pl.when(z < n - 1)
    def _():
        pl.semaphore_signal(barrier, inc=1, device_id={"slab": z + 1}, device_id_type=MESH)

    def clear(o_ref, s_ref):
        o_ref[...] = jnp.zeros_like(o_ref)
        s_ref[:, 0:1, :] = jnp.full((chunks, 1, HD), LOW, F32)
        s_ref[:, 1:2, :] = jnp.zeros((chunks, 1, HD), F32)

    @pl.when(z == 0)
    def _():
        clear(pre_o, pre_s)

    @pl.when(z == n - 1)
    def _():
        clear(suf_o, suf_s)

    ends = (z == 0).astype(jnp.int32) + (z == n - 1).astype(jnp.int32)
    pl.semaphore_wait(barrier, seq_n - 1 + heads_n - 1 + 2 - ends)

    fresh_src = [(fk_ref, kf, 0), (nk_ref, kf, 1), (fv_ref, vf, 0), (nv_ref, vf, 1)]
    ahead = min(max(hcount // 5, 3), hcount)
    edges = [0, ahead * HD, width] if ahead < hcount else [0, width]
    cuts = [slice(a, b) for a, b in zip(edges, edges[1:])]
    fresh_remote = [[] for _ in cuts]
    for k, cols in enumerate(cuts):
        for d in range(1, seq_n):
            for i, (src, dst, part) in enumerate(fresh_src):
                c = pltpu.make_async_remote_copy(
                    src_ref=src.at[:, cols],
                    dst_ref=dst.at[sq, part, :, cols],
                    send_sem=fresh_send.at[d - 1, k, i],
                    recv_sem=fresh_recv.at[d - 1, k, i],
                    device_id={"seq": lax.rem(sq + d, seq_n)},
                    device_id_type=MESH,
                )
                c.start()
                fresh_remote[k].append(c)

    loads[0].wait()
    loads[1].wait()
    loads[5].start()
    loads[2].start()
    loads[3].start()
    fresh_local = []
    for i, (src, dst, part) in enumerate(fresh_src):
        c = pltpu.make_async_copy(src, dst.at[sq, part], fresh_sem.at[i])
        c.start()
        fresh_local.append(c)
    loads[4].start()

    def squares_step(h, total):
        x = q[:, pl.ds(pl.multiple_of(h * HD, HD), HD)].astype(F32)
        return total + x * x

    total = lax.fori_loop(0, hcount, squares_step, jnp.zeros((rows, HD), F32))
    row_total = jnp.sum(total.T, axis=0, keepdims=True)
    squares[hx] = jnp.broadcast_to(row_total, (8, rows))
    sq_copies = []
    for d in range(1, heads_n):
        c = pltpu.make_async_remote_copy(
            src_ref=squares.at[hx],
            dst_ref=squares.at[hx],
            send_sem=sq_send.at[d - 1],
            recv_sem=sq_recv.at[d - 1],
            device_id={"head": lax.rem(hx + d, heads_n)},
            device_id_type=MESH,
        )
        c.start()
        sq_copies.append(c)

    def gain_step(h, carry):
        cols = pl.ds(pl.multiple_of(h * HD, HD), HD)
        qg[:, cols] = (q[:, cols].astype(F32) * gain[cols][None, :]).astype(BF16)
        return carry

    lax.fori_loop(0, hcount, gain_step, 0)
    loads[5].wait()
    if aligned:
        half = tw.shape[0] // 2
        j = lax.broadcasted_iota(jnp.int32, (half, HD), 0).astype(F32)
        frequency = jnp.exp(F32(-math.log(10000.0)) * j / half)
        phases = jnp.full((half, HD), step_ref[0], jnp.int32).astype(F32) * frequency
        cos, sin = jnp.cos(phases), jnp.sin(phases)
        for c in range(tw.shape[1] // HD):
            cols = slice(c * HD, (c + 1) * HD)
            terms = tw[:half, cols] * cos + tw[half:, cols] * sin
            gate[:, cols] = 1.0 + jnp.sum(terms, axis=0, keepdims=True)


    def send(h, direction):
        if direction > 0:
            pairs, ss, rs = ((right_o, pre_o), (right_s, pre_s)), right_send, right_recv
        else:
            pairs, ss, rs = ((left_o, suf_o), (left_s, suf_s)), left_send, left_recv
        return [
            pltpu.make_async_remote_copy(
                src_ref=src.at[h],
                dst_ref=dst.at[h],
                send_sem=ss.at[h, i],
                recv_sem=rs.at[h, i],
                device_id={"slab": z + direction},
                device_id_type=MESH,
            )
            for i, (src, dst) in enumerate(pairs)
        ]

    pair = 2 if hcount % 2 == 0 else 1
    fresh_rows = seq_n * 2 * fk_ref.shape[0]
    lag_end = LAG * jnp.maximum(z, n - 1 - z)

    def combine(h, other_o, other_s, dest_o, dest_s):
        m_a, l_a = own_s[h, 0:1], own_s[h, 1:2]
        m_b, l_b = other_s[h, 0:1], other_s[h, 1:2]
        top = jnp.maximum(m_a, m_b)
        e_a, e_b = jnp.exp2(m_a - top), jnp.exp2(m_b - top)
        dest_o[h] = (own_o[h] * e_a + other_o[h].astype(F32) * e_b).astype(BF16)
        dest_s[h, 0:1] = top
        dest_s[h, 1:2] = l_a * e_a + l_b * e_b

    nt = (((1,), (1,)), ((), ()))
    tn = (((0,), (0,)), ((), ()))

    penalty = jnp.where(
        jnp.full((1, rows), owner_ref[0], jnp.int32) == z, F32(LOW), F32(0.0)
    )
    cached = kc.shape[0]
    step_keys = 256 if cached % 256 == 0 else cached
    blocks = [(i, i + step_keys) for i in range(0, cached, step_keys)]

    def head_cols(h):
        return pl.ds(pl.multiple_of(h * HD, HD), HD)

    def scores(h, slot):
        cols = head_cols(h)
        q_head = qg[:, cols]
        top = None
        for a, b in blocks:
            part = lax.dot_general(kc[a:b, cols], q_head, nt, preferred_element_type=F32)
            s_buf[slot, a:b, :] = part
            high = jnp.max(part, axis=0, keepdims=True)
            top = high if top is None else jnp.maximum(top, high)
        k_fresh = kf[:, :, :, cols].reshape(fresh_rows, HD)
        part = lax.dot_general(k_fresh, q_head, nt, preferred_element_type=F32)
        s_buf[slot, cached:, :] = part
        m_buf[slot, 0:1, :] = top
        m_buf[slot, 1:2, :] = jnp.max(part, axis=0, keepdims=True)

    def soften(h, slot):
        s_row = scale[0:1]
        top = jnp.maximum(m_buf[slot, 0:1, :] * s_row + penalty, m_buf[slot, 1:2, :] * s_row)
        top_c = top - penalty
        mass = jnp.zeros((1, rows), F32)
        for a, b in blocks + [(cached, cached + fresh_rows)]:
            p = jnp.exp2(s_buf[slot, a:b, :] * s_row - (top_c if a < cached else top))
            p_buf[slot, a:b, :] = p.astype(BF16)
            mass = mass + jnp.sum(p, axis=0, keepdims=True)
        for g in range(groups):
            part = slice(g * HD, (g + 1) * HD)
            own_s[g * hcount + h, 0:1] = top[:, part]
            own_s[g * hcount + h, 1:2] = mass[:, part]

    def weigh(h, slot):
        cols = head_cols(h)
        v_fresh = vf[:, :, :, cols].reshape(fresh_rows, HD)
        o = lax.dot_general(v_fresh, p_buf[slot, cached:, :], tn, preferred_element_type=F32)
        for a, b in blocks:
            o += lax.dot_general(
                vc[a:b, cols], p_buf[slot, a:b, :], tn, preferred_element_type=F32
            )
        for g in range(groups):
            own_o[g * hcount + h] = o[:, g * HD : (g + 1) * HD]

    def project(g, p):
        deep = pl.ds(pl.multiple_of(p * pair * HD, HD), pair * HD)
        term = lax.dot_general(att[g, deep, :], w[deep, :], tn, preferred_element_type=F32)

        @pl.when(p == 0)
        def _():
            acc[g] = term

        @pl.when(p > 0)
        def _():
            acc[g] += term

    def exchange(g):
        copies = []
        for d in range(1, heads_n):
            copies.append(
                pltpu.make_async_remote_copy(
                    src_ref=xs.at[d - 1, g],
                    dst_ref=xr.at[d - 1, g],
                    send_sem=x_send.at[d - 1, g],
                    recv_sem=x_recv.at[d - 1, g],
                    device_id={"head": lax.rem(hx + d, heads_n)},
                    device_id_type=MESH,
                )
            )
        return copies

    def exchange_start(g):
        cp = out_ref.shape[1]
        for d, c in enumerate(exchange(g)):
            peer = lax.rem(hx + d + 1, heads_n)
            cols = pl.ds(pl.multiple_of(peer * cp, HD), cp)
            xs[d, g] = acc[g, :, cols].astype(BF16)
            c.start()

    pairs = hcount // pair
    last = (groups - 1) * hcount

    def service(t):
        cp_ = t - LAG * z
        in_p = (cp_ >= 0) & (cp_ < chunks)
        cs = t - LAG * (n - 1 - z)
        in_s = (cs >= 0) & (cs < chunks)

        @pl.when(in_p & (z > 0))
        def _():
            for c in send(cp_, 1):
                c.wait_recv()

        @pl.when(in_p & (z < n - 1))
        def _():
            combine(cp_, pre_o, pre_s, right_o, right_s)
            for c in send(cp_, 1):
                c.start()

        @pl.when(in_s & (z < n - 1))
        def _():
            for c in send(cs, -1):
                c.wait_recv()

        @pl.when(in_s & (z > 0))
        def _():
            combine(cs, suf_o, suf_s, left_o, left_s)
            for c in send(cs, -1):
                c.start()

    def finish(t):
        f = t - lag_end

        @pl.when((f >= 0) & (f < chunks))
        def _():
            m_a, m_b, m_c = own_s[f, 0:1], pre_s[f, 0:1], suf_s[f, 0:1]
            top = jnp.maximum(m_a, jnp.maximum(m_b, m_c))
            e_a, e_b, e_c = jnp.exp2(m_a - top), jnp.exp2(m_b - top), jnp.exp2(m_c - top)
            mass = own_s[f, 1:2] * e_a + pre_s[f, 1:2] * e_b + suf_s[f, 1:2] * e_c
            total_o = (
                own_o[f] * e_a + pre_o[f].astype(F32) * e_b + suf_o[f].astype(F32) * e_c
            )
            h = lax.rem(f, hcount)
            att[f // hcount, pl.ds(pl.multiple_of(h * HD, HD), HD), :] = (
                total_o / mass
            ).astype(BF16)

        @pl.when(f == last)
        def _():
            loads[4].wait()

        for g in range(groups - 1):

            @pl.when((f >= last) & (f < last + pairs))
            def _(g=g):
                project(g, f - last)

            if aligned:

                @pl.when(f == last + pairs - 1)
                def _(g=g):
                    exchange_start(g)

        done = f - last + 1

        @pl.when((done > 0) & (done <= hcount) & (lax.rem(done, pair) == 0))
        def _():
            project(groups - 1, done // pair - 1)

    def near(h):
        return jnp.minimum(h, hcount - 1)

    loads[2].wait()
    for c in fresh_local:
        c.wait()
    for c in fresh_remote[0]:
        c.wait_recv()
    scores(0, 0)
    scores(min(1, hcount - 1), 1)
    for c in sq_copies:
        c.wait_recv()
    norm_total = jnp.sum(squares[...], axis=0)
    scale[...] = lax.rsqrt(norm_total / (HEADS * HD) + EPSILON) * (
        math.log2(math.e) / HD**0.5
    )
    soften(0, 0)
    loads[3].wait()
    weigh(0, 0)
    service(0)
    soften(min(1, hcount - 1), 1)
    scores(min(2, hcount - 1), 0)

    def body(i, carry):
        for u in range(2):
            t = 2 * i + u
            if len(cuts) > 1:

                @pl.when(t + 3 == ahead)
                def _():
                    for c in fresh_remote[1]:
                        c.wait_recv()

            @pl.when(t + 1 < hcount)
            def _(t=t, u=u):
                scores(near(t + 3), 1 - u)
                soften(near(t + 2), u)
                weigh(near(t + 1), 1 - u)

            finish(t)
            service(t + 1)
        return carry

    lax.fori_loop(0, (chunks + LAG * (n - 1) + 1) // 2, body, 0)

    def drain(h, carry):
        @pl.when(z < n - 1)
        def _():
            for c in send(h, 1):
                c.wait_send()

        @pl.when(z > 0)
        def _():
            for c in send(h, -1):
                c.wait_send()

        return carry

    def settle():
        for c in [c for cut in fresh_remote for c in cut] + sq_copies:
            c.wait_send()
        lax.fori_loop(0, chunks, drain, 0)

    if aligned:
        cp = out_ref.shape[1]
        mine = pl.ds(pl.multiple_of(hx * cp, HD), cp)
        exchange_start(groups - 1)
        settle()
        for g in range(groups):
            summed = acc[g, :, mine]
            for d, c in enumerate(exchange(g)):
                c.wait_recv()
                summed = summed + xr[d, g].astype(F32)
            out_ref[g * HD : (g + 1) * HD, :] = (summed * gate[...]).astype(out_ref.dtype)
        for g in range(groups):
            for c in exchange(g):
                c.wait_send()
    else:
        for g in range(groups):
            out_ref[g * HD : (g + 1) * HD, :] = acc[g]
        settle()


def local(sizes, *args):
    (
        queries,
        query_gain,
        cache_keys,
        cache_values,
        finished_keys,
        finished_values,
        new_keys,
        new_values,
        out_weight,
        time_weight,
        owner,
        step,
    ) = args
    n, heads_n, seq_n = sizes
    rows, width = queries.shape
    hcount = width // HD
    cached, fresh = cache_keys.shape[0], finished_keys.shape[0]
    columns, cp = out_weight.shape[1], time_weight.shape[1]
    freq = time_weight.shape[0]
    aligned = cp % HD == 0
    any_spec = pl.BlockSpec(memory_space=pl.ANY)
    smem = pl.BlockSpec(memory_space=pltpu.SMEM)
    vmem = pl.BlockSpec(memory_space=pltpu.VMEM)
    dma = pltpu.SemaphoreType.DMA
    xcount = max(heads_n - 1, 1)
    groups = rows // HD
    chunks = groups * hcount
    stat = (chunks, 2, HD)
    keys = cached + seq_n * 2 * fresh
    part = (chunks, HD, HD)
    result = pl.pallas_call(
        functools.partial(kernel, sizes, aligned),
        out_shape=jax.ShapeDtypeStruct(
            (rows, cp if aligned else columns), BF16 if aligned else F32
        ),
        in_specs=[any_spec] * 10 + [smem] * 2,
        out_specs=vmem,
        scratch_shapes=[
            pltpu.VMEM((rows, width), BF16),
            pltpu.VMEM((rows, width), BF16),
            pltpu.VMEM((width,), F32),
            pltpu.VMEM((cached, width), BF16),
            pltpu.VMEM((cached, width), BF16),
            pltpu.VMEM((seq_n, 2, fresh, width), BF16),
            pltpu.VMEM((seq_n, 2, fresh, width), BF16),
            pltpu.VMEM((width, columns), BF16),
            pltpu.VMEM((freq, cp), F32),
            pltpu.VMEM((heads_n, 8, rows), F32),
            pltpu.VMEM((8, rows), F32),
            pltpu.VMEM(part, F32),
            pltpu.VMEM(stat, F32),
            pltpu.VMEM(part, BF16),
            pltpu.VMEM(stat, F32),
            pltpu.VMEM(part, BF16),
            pltpu.VMEM(stat, F32),
            pltpu.VMEM(part, BF16),
            pltpu.VMEM(stat, F32),
            pltpu.VMEM(part, BF16),
            pltpu.VMEM(stat, F32),
            pltpu.VMEM((groups, width, HD), BF16),
            pltpu.VMEM((groups, HD, columns), F32),
            pltpu.VMEM((1, cp), F32),
            pltpu.VMEM((xcount, groups, HD, cp), BF16),
            pltpu.VMEM((xcount, groups, HD, cp), BF16),
            dma((6,)),
            dma((4,)),
            dma((max(seq_n - 1, 1), 2, 4)),
            dma((max(seq_n - 1, 1), 2, 4)),
            dma((xcount,)),
            dma((xcount,)),
            dma((chunks, 2)),
            dma((chunks, 2)),
            dma((chunks, 2)),
            dma((chunks, 2)),
            dma((xcount, groups)),
            dma((xcount, groups)),
            pltpu.VMEM((2, keys, rows), F32),
            pltpu.VMEM((2, keys, rows), BF16),
            pltpu.VMEM((2, 2, rows), F32),
        ],
        compiler_params=pltpu.CompilerParams(
            collective_id=0, has_side_effects=True, vmem_limit_bytes=60 * 1024 * 1024
        ),
        name="sweep_attention",
    )(
        queries,
        query_gain,
        cache_keys,
        cache_values,
        finished_keys,
        finished_values,
        new_keys,
        new_values,
        out_weight,
        time_weight,
        owner,
        step,
    )
    if aligned:
        return result
    summed = lax.psum_scatter(result, "head", scatter_dimension=1, tiled=True)
    half = freq // 2
    frequency = jnp.exp(-jnp.log(10000.0) * jnp.arange(half, dtype=F32) / half)
    phases = step[0].astype(F32) * frequency
    embedding = jnp.concatenate([jnp.cos(phases), jnp.sin(phases)])
    time_gate = 1.0 + jnp.dot(embedding, time_weight, precision=lax.Precision.HIGHEST)
    return (time_gate * summed).astype(BF16)


def solution(mesh):
    in_specs = (
        P(("grp", "seq"), "head"),
        P("head"),
        P(("grp", "slab"), "head"),
        P(("grp", "slab"), "head"),
        P(("grp", "slab", "seq"), "head"),
        P(("grp", "slab", "seq"), "head"),
        P(("grp", "slab", "seq"), "head"),
        P(("grp", "slab", "seq"), "head"),
        P("head", "slab"),
        P(None, ("slab", "head")),
        P("grp"),
        P("grp"),
    )
    out_specs = P(("grp", "seq"), ("slab", "head"))
    sizes = (mesh.shape["slab"], mesh.shape["head"], mesh.shape["seq"])
    return jax.shard_map(
        functools.partial(local, sizes),
        mesh=mesh,
        in_specs=in_specs,
        out_specs=out_specs,
        check_vma=False,
    )
```

```python
import functools
import math

import jax
import jax.numpy as jnp
from jax import lax
from jax.experimental import pallas as pl
from jax.experimental.pallas import tpu as pltpu
from jax.sharding import PartitionSpec as P

HEADS = 40
HD = 128
EPSILON = 1e-06
LOW = -1e30
LAG = 5
MESH = pl.DeviceIdType.MESH
F32 = jnp.float32
BF16 = jnp.bfloat16


def kernel(
    dims,
    aligned,
    q_ref,
    gain_ref,
    ck_ref,
    cv_ref,
    fk_ref,
    fv_ref,
    nk_ref,
    nv_ref,
    w_ref,
    tw_ref,
    owner_ref,
    step_ref,
    out_ref,
    q,
    qg,
    gain,
    kc,
    vc,
    kf,
    vf,
    w,
    tw,
    squares,
    scale,
    own_o,
    own_s,
    pre_o,
    pre_s,
    suf_o,
    suf_s,
    right_o,
    right_s,
    left_o,
    left_s,
    att,
    acc,
    gate,
    xs,
    xr,
    load_sem,
    fresh_sem,
    fresh_send,
    fresh_recv,
    sq_send,
    sq_recv,
    right_send,
    right_recv,
    left_send,
    left_recv,
    x_send,
    x_recv,
    s_buf,
    p_buf,
    m_buf,
):
    n, heads_n, seq_n = dims
    rows, width = q_ref.shape
    hcount = width // HD
    z = lax.axis_index("slab")
    hx = lax.axis_index("head")
    sq = lax.axis_index("seq")

    groups = rows // HD
    chunks = groups * hcount
    loads = [
        pltpu.make_async_copy(src, dst, load_sem.at[i])
        for i, (src, dst) in enumerate(
            [(q_ref, q), (gain_ref, gain), (ck_ref, kc), (cv_ref, vc), (w_ref, w), (tw_ref, tw)]
        )
    ]
    loads[0].start()
    loads[1].start()
    barrier = pltpu.get_barrier_semaphore()
    for d in range(1, seq_n):
        pl.semaphore_signal(
            barrier, inc=1, device_id={"seq": lax.rem(sq + d, seq_n)}, device_id_type=MESH
        )
    for d in range(1, heads_n):
        pl.semaphore_signal(
            barrier, inc=1, device_id={"head": lax.rem(hx + d, heads_n)}, device_id_type=MESH
        )

    @pl.when(z > 0)
    def _():
        pl.semaphore_signal(barrier, inc=1, device_id={"slab": z - 1}, device_id_type=MESH)

    @pl.when(z < n - 1)
    def _():
        pl.semaphore_signal(barrier, inc=1, device_id={"slab": z + 1}, device_id_type=MESH)

    def clear(o_ref, s_ref):
        o_ref[...] = jnp.zeros_like(o_ref)
        s_ref[:, 0:1, :] = jnp.full((chunks, 1, HD), LOW, F32)
        s_ref[:, 1:2, :] = jnp.zeros((chunks, 1, HD), F32)

    @pl.when(z == 0)
    def _():
        clear(pre_o, pre_s)

    @pl.when(z == n - 1)
    def _():
        clear(suf_o, suf_s)

    ends = (z == 0).astype(jnp.int32) + (z == n - 1).astype(jnp.int32)
    pl.semaphore_wait(barrier, seq_n - 1 + heads_n - 1 + 2 - ends)

    fresh_src = [(fk_ref, kf, 0), (nk_ref, kf, 1), (fv_ref, vf, 0), (nv_ref, vf, 1)]
    ahead = min(max(hcount // 5, 3), hcount)
    edges = [0, ahead * HD, width] if ahead < hcount else [0, width]
    cuts = [slice(a, b) for a, b in zip(edges, edges[1:])]
    fresh_remote = [[] for _ in cuts]
    for k, cols in enumerate(cuts):
        for d in range(1, seq_n):
            for i, (src, dst, part) in enumerate(fresh_src):
                c = pltpu.make_async_remote_copy(
                    src_ref=src.at[:, cols],
                    dst_ref=dst.at[sq, part, :, cols],
                    send_sem=fresh_send.at[d - 1, k, i],
                    recv_sem=fresh_recv.at[d - 1, k, i],
                    device_id={"seq": lax.rem(sq + d, seq_n)},
                    device_id_type=MESH,
                )
                c.start()
                fresh_remote[k].append(c)

    loads[0].wait()
    loads[1].wait()
    loads[5].start()
    loads[2].start()
    loads[3].start()
    fresh_local = []
    for i, (src, dst, part) in enumerate(fresh_src):
        c = pltpu.make_async_copy(src, dst.at[sq, part], fresh_sem.at[i])
        c.start()
        fresh_local.append(c)
    loads[4].start()

    def squares_step(h, total):
        x = q[:, pl.ds(pl.multiple_of(h * HD, HD), HD)].astype(F32)
        return total + x * x

    total = lax.fori_loop(0, hcount, squares_step, jnp.zeros((rows, HD), F32))
    row_total = jnp.sum(total.T, axis=0, keepdims=True)
    squares[hx] = jnp.broadcast_to(row_total, (8, rows))
    sq_copies = []
    for d in range(1, heads_n):
        c = pltpu.make_async_remote_copy(
            src_ref=squares.at[hx],
            dst_ref=squares.at[hx],
            send_sem=sq_send.at[d - 1],
            recv_sem=sq_recv.at[d - 1],
            device_id={"head": lax.rem(hx + d, heads_n)},
            device_id_type=MESH,
        )
        c.start()
        sq_copies.append(c)

    def gain_step(h, carry):
        cols = pl.ds(pl.multiple_of(h * HD, HD), HD)
        qg[:, cols] = (q[:, cols].astype(F32) * gain[cols][None, :]).astype(BF16)
        return carry

    lax.fori_loop(0, hcount, gain_step, 0)
    loads[5].wait()
    if aligned:
        half = tw.shape[0] // 2
        j = lax.broadcasted_iota(jnp.int32, (half, HD), 0).astype(F32)
        frequency = jnp.exp(F32(-math.log(10000.0)) * j / half)
        phases = jnp.full((half, HD), step_ref[0], jnp.int32).astype(F32) * frequency
        cos, sin = jnp.cos(phases), jnp.sin(phases)
        for c in range(tw.shape[1] // HD):
            cols = slice(c * HD, (c + 1) * HD)
            terms = tw[:half, cols] * cos + tw[half:, cols] * sin
            gate[:, cols] = 1.0 + jnp.sum(terms, axis=0, keepdims=True)


    def send(h, direction):
        if direction > 0:
            pairs, ss, rs = ((right_o, pre_o), (right_s, pre_s)), right_send, right_recv
        else:
            pairs, ss, rs = ((left_o, suf_o), (left_s, suf_s)), left_send, left_recv
        return [
            pltpu.make_async_remote_copy(
                src_ref=src.at[h],
                dst_ref=dst.at[h],
                send_sem=ss.at[h, i],
                recv_sem=rs.at[h, i],
                device_id={"slab": z + direction},
                device_id_type=MESH,
            )
            for i, (src, dst) in enumerate(pairs)
        ]

    pair = 2 if hcount % 2 == 0 else 1
    splits = pair
    sub = HD // splits
    pairs = hcount // pair
    last = (groups - 1) * hcount
    fresh_rows = seq_n * 2 * fk_ref.shape[0]
    lag_end = LAG * jnp.maximum(z, n - 1 - z)

    def combine(h, other_o, other_s, dest_o, dest_s):
        m_a, l_a = own_s[h, 0:1], own_s[h, 1:2]
        m_b, l_b = other_s[h, 0:1], other_s[h, 1:2]
        top = jnp.maximum(m_a, m_b)
        e_a, e_b = jnp.exp2(m_a - top), jnp.exp2(m_b - top)
        dest_o[h] = (own_o[h] * e_a + other_o[h].astype(F32) * e_b).astype(BF16)
        dest_s[h, 0:1] = top
        dest_s[h, 1:2] = l_a * e_a + l_b * e_b

    nt = (((1,), (1,)), ((), ()))
    tn = (((0,), (0,)), ((), ()))

    penalty = jnp.where(
        jnp.full((1, rows), owner_ref[0], jnp.int32) == z, F32(LOW), F32(0.0)
    )
    cached = kc.shape[0]
    step_keys = 256 if cached % 256 == 0 else cached
    blocks = [(i, i + step_keys) for i in range(0, cached, step_keys)]

    def head_cols(h):
        return pl.ds(pl.multiple_of(h * HD, HD), HD)

    def scores(h, slot):
        cols = head_cols(h)
        q_head = qg[:, cols]
        top = None
        for a, b in blocks:
            part = lax.dot_general(kc[a:b, cols], q_head, nt, preferred_element_type=F32)
            s_buf[slot, a:b, :] = part
            high = jnp.max(part, axis=0, keepdims=True)
            top = high if top is None else jnp.maximum(top, high)
        k_fresh = kf[:, :, :, cols].reshape(fresh_rows, HD)
        part = lax.dot_general(k_fresh, q_head, nt, preferred_element_type=F32)
        s_buf[slot, cached:, :] = part
        m_buf[slot, 0:1, :] = top
        m_buf[slot, 1:2, :] = jnp.max(part, axis=0, keepdims=True)

    def soften(h, slot):
        s_row = scale[0:1]
        top = jnp.maximum(m_buf[slot, 0:1, :] * s_row + penalty, m_buf[slot, 1:2, :] * s_row)
        top_c = top - penalty
        mass = jnp.zeros((1, rows), F32)
        for a, b in blocks + [(cached, cached + fresh_rows)]:
            p = jnp.exp2(s_buf[slot, a:b, :] * s_row - (top_c if a < cached else top))
            p_buf[slot, a:b, :] = p.astype(BF16)
            mass = mass + jnp.sum(p, axis=0, keepdims=True)
        m_buf[slot, 2:3, :] = top
        m_buf[slot, 3:4, :] = mass

    def place(g, h, slot, value, store):
        if g < groups - 1 or splits == 1:
            store(g * hcount + h, slice(0, HD), value)
            return
        turned = pltpu.roll(value, sub, 1)
        lanes = slice(slot * sub, (slot + 1) * sub)
        for s in range(splits):
            source = value if s == slot else turned
            store(last + s * pairs + lax.div(h, 2), lanes, source[:, lanes])

    def weigh(h, slot):
        cols = head_cols(h)
        v_fresh = vf[:, :, :, cols].reshape(fresh_rows, HD)
        o = lax.dot_general(v_fresh, p_buf[slot, cached:, :], tn, preferred_element_type=F32)
        for a, b in blocks:
            o += lax.dot_general(
                vc[a:b, cols], p_buf[slot, a:b, :], tn, preferred_element_type=F32
            )
        for g in range(groups):
            part = slice(g * HD, (g + 1) * HD)

            def store_o(c, lanes, value):
                own_o[c, :, lanes] = value

            def store_s(c, lanes, value):
                own_s[c, :, lanes] = value

            place(g, h, slot, o[:, part], store_o)
            place(g, h, slot, m_buf[slot, 2:4, part], store_s)

    def project(g, p):
        deep = pl.ds(pl.multiple_of(p * pair * HD, HD), pair * HD)
        term = lax.dot_general(att[g, deep, :], w[deep, :], tn, preferred_element_type=F32)
        add(acc.at[g * HD : (g + 1) * HD, :], term, p)

    def project_last(s, p):
        deep = pl.ds(pl.multiple_of(p * pair * HD, HD), pair * HD)
        term = lax.dot_general(
            att[groups - 1 + s, deep, 0:sub], w[deep, :], tn, preferred_element_type=F32
        )
        add(acc.at[(groups - 1) * HD + s * sub : (groups - 1) * HD + (s + 1) * sub, :], term, p)

    def add(dest, term, p):
        @pl.when(p == 0)
        def _():
            dest[...] = term

        @pl.when(p > 0)
        def _():
            dest[...] += term

    pieces = [(g * HD, (g + 1) * HD) for g in range(groups - 1)]
    pieces += [((groups - 1) * HD + s * sub, (groups - 1) * HD + (s + 1) * sub) for s in range(splits)]

    def exchange(k):
        a, b = pieces[k]
        copies = []
        for d in range(1, heads_n):
            copies.append(
                pltpu.make_async_remote_copy(
                    src_ref=xs.at[d - 1, a:b],
                    dst_ref=xr.at[d - 1, a:b],
                    send_sem=x_send.at[d - 1, k],
                    recv_sem=x_recv.at[d - 1, k],
                    device_id={"head": lax.rem(hx + d, heads_n)},
                    device_id_type=MESH,
                )
            )
        return copies

    def exchange_start(k):
        a, b = pieces[k]
        cp = out_ref.shape[1]
        for d, c in enumerate(exchange(k)):
            peer = lax.rem(hx + d + 1, heads_n)
            cols = pl.ds(pl.multiple_of(peer * cp, HD), cp)
            xs[d, a:b] = acc[a:b, cols].astype(BF16)
            c.start()

    def service(t):
        cp_ = t - LAG * z
        in_p = (cp_ >= 0) & (cp_ < chunks)
        cs = t - LAG * (n - 1 - z)
        in_s = (cs >= 0) & (cs < chunks)

        @pl.when(in_p & (z > 0))
        def _():
            for c in send(cp_, 1):
                c.wait_recv()

        @pl.when(in_p & (z < n - 1))
        def _():
            combine(cp_, pre_o, pre_s, right_o, right_s)
            for c in send(cp_, 1):
                c.start()

        @pl.when(in_s & (z < n - 1))
        def _():
            for c in send(cs, -1):
                c.wait_recv()

        @pl.when(in_s & (z > 0))
        def _():
            combine(cs, suf_o, suf_s, left_o, left_s)
            for c in send(cs, -1):
                c.start()

    def finish(t):
        f = t - lag_end

        @pl.when((f >= 0) & (f < chunks))
        def _():
            m_a, m_b, m_c = own_s[f, 0:1], pre_s[f, 0:1], suf_s[f, 0:1]
            top = jnp.maximum(m_a, jnp.maximum(m_b, m_c))
            e_a, e_b, e_c = jnp.exp2(m_a - top), jnp.exp2(m_b - top), jnp.exp2(m_c - top)
            mass = own_s[f, 1:2] * e_a + pre_s[f, 1:2] * e_b + suf_s[f, 1:2] * e_c
            total_o = (
                own_o[f] * e_a + pre_o[f].astype(F32) * e_b + suf_o[f].astype(F32) * e_c
            )
            value = (total_o / mass).astype(BF16)

            @pl.when(f < last)
            def _():
                h = lax.rem(f, hcount)
                att[f // hcount, head_cols(h), :] = value

            @pl.when(f >= last)
            def _():
                k = f - last
                s, p = lax.div(k, pairs), lax.rem(k, pairs)
                for i in range(pair):
                    turned = value if i == 0 else pltpu.roll(total_o / mass, HD - i * sub, 1).astype(BF16)
                    att[groups - 1 + s, head_cols(p * pair + i), :] = turned

        @pl.when(f == last)
        def _():
            loads[4].wait()

        for g in range(groups - 1):

            @pl.when((f >= last) & (f < last + pairs))
            def _(g=g):
                project(g, f - last)

            if aligned:

                @pl.when(f == last + pairs - 1)
                def _(g=g):
                    exchange_start(g)

        for s in range(splits):
            begin = last + s * pairs

            @pl.when((f >= begin) & (f < begin + pairs))
            def _(s=s, begin=begin):
                project_last(s, f - begin)

            if aligned and s < splits - 1:

                @pl.when(f == begin + pairs - 1)
                def _(s=s):
                    exchange_start(groups - 1 + s)

    def near(h):
        return jnp.minimum(h, hcount - 1)

    loads[2].wait()
    for c in fresh_local:
        c.wait()
    for c in fresh_remote[0]:
        c.wait_recv()
    scores(0, 0)
    scores(min(1, hcount - 1), 1)
    for c in sq_copies:
        c.wait_recv()
    norm_total = jnp.sum(squares[...], axis=0)
    scale[...] = lax.rsqrt(norm_total / (HEADS * HD) + EPSILON) * (
        math.log2(math.e) / HD**0.5
    )
    soften(0, 0)
    loads[3].wait()
    weigh(0, 0)
    service(0)
    soften(min(1, hcount - 1), 1)
    scores(min(2, hcount - 1), 0)

    def body(i, carry):
        for u in range(2):
            t = 2 * i + u
            if len(cuts) > 1:

                @pl.when(t + 3 == ahead)
                def _():
                    for c in fresh_remote[1]:
                        c.wait_recv()

            @pl.when(t + 1 < hcount)
            def _(t=t, u=u):
                scores(near(t + 3), 1 - u)
                soften(near(t + 2), u)
                weigh(near(t + 1), 1 - u)

            finish(t)
            service(t + 1)
        return carry

    lax.fori_loop(0, (chunks + LAG * (n - 1) + 1) // 2, body, 0)

    def drain(h, carry):
        @pl.when(z < n - 1)
        def _():
            for c in send(h, 1):
                c.wait_send()

        @pl.when(z > 0)
        def _():
            for c in send(h, -1):
                c.wait_send()

        return carry

    def settle():
        for c in [c for cut in fresh_remote for c in cut] + sq_copies:
            c.wait_send()
        lax.fori_loop(0, chunks, drain, 0)

    if aligned:
        cp = out_ref.shape[1]
        mine = pl.ds(pl.multiple_of(hx * cp, HD), cp)
        exchange_start(len(pieces) - 1)
        settle()
        for k, (a, b) in enumerate(pieces):
            summed = acc[a:b, mine]
            for d, c in enumerate(exchange(k)):
                c.wait_recv()
                summed = summed + xr[d, a:b].astype(F32)
            out_ref[a:b, :] = (summed * gate[...]).astype(out_ref.dtype)
        for k in range(len(pieces)):
            for c in exchange(k):
                c.wait_send()
    else:
        out_ref[...] = acc[...]
        settle()


def local(sizes, *args):
    (
        queries,
        query_gain,
        cache_keys,
        cache_values,
        finished_keys,
        finished_values,
        new_keys,
        new_values,
        out_weight,
        time_weight,
        owner,
        step,
    ) = args
    n, heads_n, seq_n = sizes
    rows, width = queries.shape
    hcount = width // HD
    cached, fresh = cache_keys.shape[0], finished_keys.shape[0]
    columns, cp = out_weight.shape[1], time_weight.shape[1]
    freq = time_weight.shape[0]
    aligned = cp % HD == 0
    any_spec = pl.BlockSpec(memory_space=pl.ANY)
    smem = pl.BlockSpec(memory_space=pltpu.SMEM)
    vmem = pl.BlockSpec(memory_space=pltpu.VMEM)
    dma = pltpu.SemaphoreType.DMA
    xcount = max(heads_n - 1, 1)
    groups = rows // HD
    chunks = groups * hcount
    stat = (chunks, 2, HD)
    keys = cached + seq_n * 2 * fresh
    part = (chunks, HD, HD)
    result = pl.pallas_call(
        functools.partial(kernel, sizes, aligned),
        out_shape=pltpu.VMEM((rows, cp), BF16) if aligned else jax.ShapeDtypeStruct((rows, columns), F32),
        in_specs=[any_spec] * 10 + [smem] * 2,
        out_specs=vmem,
        scratch_shapes=[
            pltpu.VMEM((rows, width), BF16),
            pltpu.VMEM((rows, width), BF16),
            pltpu.VMEM((width,), F32),
            pltpu.VMEM((cached, width), BF16),
            pltpu.VMEM((cached, width), BF16),
            pltpu.VMEM((seq_n, 2, fresh, width), BF16),
            pltpu.VMEM((seq_n, 2, fresh, width), BF16),
            pltpu.VMEM((width, columns), BF16),
            pltpu.VMEM((freq, cp), F32),
            pltpu.VMEM((heads_n, 8, rows), F32),
            pltpu.VMEM((8, rows), F32),
            pltpu.VMEM(part, F32),
            pltpu.VMEM(stat, F32),
            pltpu.VMEM(part, BF16),
            pltpu.VMEM(stat, F32),
            pltpu.VMEM(part, BF16),
            pltpu.VMEM(stat, F32),
            pltpu.VMEM(part, BF16),
            pltpu.VMEM(stat, F32),
            pltpu.VMEM(part, BF16),
            pltpu.VMEM(stat, F32),
            pltpu.VMEM((groups + 1, width, HD), BF16),
            pltpu.VMEM((rows, columns), F32),
            pltpu.VMEM((1, cp), F32),
            pltpu.VMEM((xcount, rows, cp), BF16),
            pltpu.VMEM((xcount, rows, cp), BF16),
            dma((6,)),
            dma((4,)),
            dma((max(seq_n - 1, 1), 2, 4)),
            dma((max(seq_n - 1, 1), 2, 4)),
            dma((xcount,)),
            dma((xcount,)),
            dma((chunks, 2)),
            dma((chunks, 2)),
            dma((chunks, 2)),
            dma((chunks, 2)),
            dma((xcount, groups + 1)),
            dma((xcount, groups + 1)),
            pltpu.VMEM((2, keys, rows), F32),
            pltpu.VMEM((2, keys, rows), BF16),
            pltpu.VMEM((2, 4, rows), F32),
        ],
        compiler_params=pltpu.CompilerParams(
            collective_id=0, has_side_effects=True, vmem_limit_bytes=60 * 1024 * 1024
        ),
        name="sweep_attention",
    )(
        queries,
        query_gain,
        cache_keys,
        cache_values,
        finished_keys,
        finished_values,
        new_keys,
        new_values,
        out_weight,
        time_weight,
        owner,
        step,
    )
    if aligned:
        return result
    summed = lax.psum_scatter(result, "head", scatter_dimension=1, tiled=True)
    half = freq // 2
    frequency = jnp.exp(-jnp.log(10000.0) * jnp.arange(half, dtype=F32) / half)
    phases = step[0].astype(F32) * frequency
    embedding = jnp.concatenate([jnp.cos(phases), jnp.sin(phases)])
    time_gate = 1.0 + jnp.dot(embedding, time_weight, precision=lax.Precision.HIGHEST)
    return (time_gate * summed).astype(BF16)


def solution(mesh):
    in_specs = (
        P(("grp", "seq"), "head"),
        P("head"),
        P(("grp", "slab"), "head"),
        P(("grp", "slab"), "head"),
        P(("grp", "slab", "seq"), "head"),
        P(("grp", "slab", "seq"), "head"),
        P(("grp", "slab", "seq"), "head"),
        P(("grp", "slab", "seq"), "head"),
        P("head", "slab"),
        P(None, ("slab", "head")),
        P("grp"),
        P("grp"),
    )
    out_specs = P(("grp", "seq"), ("slab", "head"))
    sizes = (mesh.shape["slab"], mesh.shape["head"], mesh.shape["seq"])
    return jax.shard_map(
        functools.partial(local, sizes),
        mesh=mesh,
        in_specs=in_specs,
        out_specs=out_specs,
        check_vma=False,
    )
```

```python
import functools
import math

import jax
import jax.numpy as jnp
from jax import lax
from jax.experimental import pallas as pl
from jax.experimental.pallas import tpu as pltpu
from jax.sharding import PartitionSpec as P

HEADS = 40
HD = 128
EPSILON = 1e-06
LOW = -1e30
LAG = 5
SPLIT = 4
PARTS = 4
MESH = pl.DeviceIdType.MESH
F32 = jnp.float32
BF16 = jnp.bfloat16


def kernel(
    dims,
    aligned,
    q_ref,
    gain_ref,
    ck_ref,
    cv_ref,
    fk_ref,
    fv_ref,
    nk_ref,
    nv_ref,
    w_ref,
    tw_ref,
    owner_ref,
    step_ref,
    out_ref,
    q,
    qg,
    gain,
    kc,
    vc,
    kf,
    vf,
    w,
    tw,
    squares,
    scale,
    own_o,
    own_s,
    pre_o,
    pre_s,
    suf_o,
    suf_s,
    right_o,
    right_s,
    left_o,
    left_s,
    att,
    acc,
    gate,
    xs,
    xr,
    load_sem,
    fresh_sem,
    fresh_send,
    fresh_recv,
    sq_send,
    sq_recv,
    right_send,
    right_recv,
    left_send,
    left_recv,
    x_send,
    x_recv,
    s_buf,
    p_buf,
    m_buf,
    q_sem,
    kv_sem,
):
    n, heads_n, seq_n = dims
    rows, width = q_ref.shape
    hcount = width // HD
    z = lax.axis_index("slab")
    hx = lax.axis_index("head")
    sq = lax.axis_index("seq")

    groups = rows // HD
    chunks = groups * hcount
    loads = [
        pltpu.make_async_copy(src, dst, load_sem.at[i])
        for i, (src, dst) in enumerate(
            [(q_ref, q), (gain_ref, gain), (ck_ref, kc), (cv_ref, vc), (w_ref, w), (tw_ref, tw)]
        )
    ]
    ahead = min(max(hcount // 5, 3), hcount)
    parts = PARTS if hcount % PARTS == 0 else 1
    span = width // parts
    q_loads = [
        pltpu.make_async_copy(
            q_ref.at[:, k * span : (k + 1) * span], q.at[:, k * span : (k + 1) * span], q_sem.at[k]
        )
        for k in range(parts)
    ]
    for c in q_loads:
        c.start()
    loads[1].start()
    barrier = pltpu.get_barrier_semaphore()
    for d in range(1, seq_n):
        pl.semaphore_signal(
            barrier, inc=1, device_id={"seq": lax.rem(sq + d, seq_n)}, device_id_type=MESH
        )
    for d in range(1, heads_n):
        pl.semaphore_signal(
            barrier, inc=1, device_id={"head": lax.rem(hx + d, heads_n)}, device_id_type=MESH
        )

    @pl.when(z > 0)
    def _():
        pl.semaphore_signal(barrier, inc=1, device_id={"slab": z - 1}, device_id_type=MESH)

    @pl.when(z < n - 1)
    def _():
        pl.semaphore_signal(barrier, inc=1, device_id={"slab": z + 1}, device_id_type=MESH)

    def clear(o_ref, s_ref):
        o_ref[...] = jnp.zeros_like(o_ref)
        s_ref[:, 0:1, :] = jnp.full((chunks, 1, HD), LOW, F32)
        s_ref[:, 1:2, :] = jnp.zeros((chunks, 1, HD), F32)

    @pl.when(z == 0)
    def _():
        clear(pre_o, pre_s)

    @pl.when(z == n - 1)
    def _():
        clear(suf_o, suf_s)

    def squares_step(h, total):
        x = q[:, pl.ds(pl.multiple_of(h * HD, HD), HD)].astype(F32)
        return total + x * x

    total = jnp.zeros((rows, HD), F32)
    for k, c in enumerate(q_loads):
        c.wait()
        total = lax.fori_loop(k * hcount // parts, (k + 1) * hcount // parts, squares_step, total)
    head_cut = ahead * HD
    kv_cuts = [slice(0, head_cut), slice(head_cut, width)] if head_cut < width else [slice(0, width)]
    kv_loads = []
    for k, cols in enumerate(kv_cuts):
        for i, (src, dst) in enumerate([(ck_ref, kc), (cv_ref, vc)]):
            kv_loads.append(pltpu.make_async_copy(src.at[:, cols], dst.at[:, cols], kv_sem.at[k, i]))
    fresh_src = [(fk_ref, kf, 0), (nk_ref, kf, 1), (fv_ref, vf, 0), (nv_ref, vf, 1)]
    loads[5].start()
    for c in kv_loads:
        c.start()
    fresh_local = []
    for i, (src, dst, part) in enumerate(fresh_src):
        pltpu.make_async_copy(src, dst.at[sq, part], fresh_sem.at[i // 2]).start()
    for side, whole in enumerate((kf, vf)):
        fresh_local.append(pltpu.make_async_copy(whole.at[sq], whole.at[sq], fresh_sem.at[side]))
    row_total = jnp.sum(total.T, axis=0, keepdims=True)
    squares[hx] = jnp.broadcast_to(row_total, (8, rows))

    ends = (z == 0).astype(jnp.int32) + (z == n - 1).astype(jnp.int32)
    pl.semaphore_wait(barrier, seq_n - 1 + heads_n - 1 + 2 - ends)

    sq_copies = []
    for d in range(1, heads_n):
        c = pltpu.make_async_remote_copy(
            src_ref=squares.at[hx],
            dst_ref=squares.at[hx],
            send_sem=sq_send.at[d - 1],
            recv_sem=sq_recv.at[d - 1],
            device_id={"head": lax.rem(hx + d, heads_n)},
            device_id_type=MESH,
        )
        c.start()
        sq_copies.append(c)

    edges = [0, ahead * HD, width] if ahead < hcount else [0, width]
    cuts = [slice(a, b) for a, b in zip(edges, edges[1:])]
    fresh_remote = [[] for _ in cuts]

    def fresh_wait(d, side, cols, k=0):
        whole = (kf, vf)[side].at[sq, :, :, cols]
        return pltpu.make_async_remote_copy(
            src_ref=whole,
            dst_ref=whole,
            send_sem=fresh_send.at[d - 1, side],
            recv_sem=fresh_recv.at[d - 1, k, side],
            device_id={"seq": lax.rem(sq + d, seq_n)},
            device_id_type=MESH,
        )

    for k, cols in enumerate(cuts):
        for d in range(1, seq_n):
            for i, (src, dst, part) in enumerate(fresh_src):
                pltpu.make_async_remote_copy(
                    src_ref=src.at[:, cols],
                    dst_ref=dst.at[sq, part, :, cols],
                    send_sem=fresh_send.at[d - 1, i // 2],
                    recv_sem=fresh_recv.at[d - 1, k, i // 2],
                    device_id={"seq": lax.rem(sq + d, seq_n)},
                    device_id_type=MESH,
                ).start()
            fresh_remote[k] += [fresh_wait(d, side, cols, k) for side in (0, 1)]

    loads[1].wait()

    def gain_step(h, carry):
        cols = pl.ds(pl.multiple_of(h * HD, HD), HD)
        qg[:, cols] = (q[:, cols].astype(F32) * gain[cols][None, :]).astype(BF16)
        return carry

    lax.fori_loop(0, hcount, gain_step, 0)
    loads[5].wait()
    if aligned:
        half = tw.shape[0] // 2
        j = lax.broadcasted_iota(jnp.int32, (half, HD), 0).astype(F32)
        frequency = jnp.exp(F32(-math.log(10000.0)) * j / half)
        phases = jnp.full((half, HD), step_ref[0], jnp.int32).astype(F32) * frequency
        cos, sin = jnp.cos(phases), jnp.sin(phases)
        for c in range(tw.shape[1] // HD):
            cols = slice(c * HD, (c + 1) * HD)
            terms = tw[:half, cols] * cos + tw[half:, cols] * sin
            gate[:, cols] = 1.0 + jnp.sum(terms, axis=0, keepdims=True)


    ring = min(chunks, LAG * (n - 1) + 1)

    def send(h, direction):
        if direction > 0:
            pairs, ss, rs = ((right_o, pre_o), (right_s, pre_s)), right_send, right_recv
        else:
            pairs, ss, rs = ((left_o, suf_o), (left_s, suf_s)), left_send, left_recv
        return [
            pltpu.make_async_remote_copy(
                src_ref=src.at[h],
                dst_ref=dst.at[h],
                send_sem=ss.at[i],
                recv_sem=rs.at[lax.rem(h, ring), i],
                device_id={"slab": z + direction},
                device_id_type=MESH,
            )
            for i, (src, dst) in enumerate(pairs)
        ]

    def settle_sends(direction):
        if direction > 0:
            pairs, ss, rs = ((right_o, pre_o), (right_s, pre_s)), right_send, right_recv
        else:
            pairs, ss, rs = ((left_o, suf_o), (left_s, suf_s)), left_send, left_recv
        for i, (src, dst) in enumerate(pairs):
            pltpu.make_async_remote_copy(
                src_ref=src,
                dst_ref=dst,
                send_sem=ss.at[i],
                recv_sem=rs.at[0, i],
                device_id={"slab": z + direction},
                device_id_type=MESH,
            ).wait_send()

    pair = 2 if hcount % 2 == 0 else 1
    splits = next(k for k in (SPLIT, 2, 1) if hcount % k == 0)
    sub = HD // splits
    tuples = hcount // splits
    pairs = hcount // pair
    last = (groups - 1) * hcount
    fresh_rows = seq_n * 2 * fk_ref.shape[0]
    lag_end = LAG * jnp.maximum(z, n - 1 - z)

    def combine(h, other_o, other_s, dest_o, dest_s):
        m_a, l_a = own_s[h, 0:1], own_s[h, 1:2]
        m_b, l_b = other_s[h, 0:1], other_s[h, 1:2]
        top = jnp.maximum(m_a, m_b)
        e_a, e_b = jnp.exp2(m_a - top), jnp.exp2(m_b - top)
        dest_o[h] = (own_o[h] * e_a + other_o[h].astype(F32) * e_b).astype(BF16)
        dest_s[h, 0:1] = top
        dest_s[h, 1:2] = l_a * e_a + l_b * e_b

    nt = (((1,), (1,)), ((), ()))
    tn = (((0,), (0,)), ((), ()))

    penalty = jnp.where(
        jnp.full((1, rows), owner_ref[0], jnp.int32) == z, F32(LOW), F32(0.0)
    )
    cached = kc.shape[0]
    step_keys = 256 if cached % 256 == 0 else cached
    blocks = [(i, i + step_keys) for i in range(0, cached, step_keys)]

    def head_cols(h):
        return pl.ds(pl.multiple_of(h * HD, HD), HD)

    def scores(h, slot):
        cols = head_cols(h)
        q_head = qg[:, cols]
        top = None
        for a, b in blocks:
            part = lax.dot_general(kc[a:b, cols], q_head, nt, preferred_element_type=F32)
            s_buf[slot, a:b, :] = part
            high = jnp.max(part, axis=0, keepdims=True)
            top = high if top is None else jnp.maximum(top, high)
        k_fresh = kf[:, :, :, cols].reshape(fresh_rows, HD)
        part = lax.dot_general(k_fresh, q_head, nt, preferred_element_type=F32)
        s_buf[slot, cached:, :] = part
        m_buf[slot, 0:1, :] = top
        m_buf[slot, 1:2, :] = jnp.max(part, axis=0, keepdims=True)

    def soften(h, slot):
        s_row = scale[0:1]
        top = jnp.maximum(m_buf[slot, 0:1, :] * s_row + penalty, m_buf[slot, 1:2, :] * s_row)
        top_c = top - penalty
        mass = jnp.zeros((1, rows), F32)
        for a, b in blocks + [(cached, cached + fresh_rows)]:
            p = jnp.exp2(s_buf[slot, a:b, :] * s_row - (top_c if a < cached else top))
            p_buf[slot, a:b, :] = p.astype(BF16)
            mass = mass + jnp.sum(p, axis=0, keepdims=True)
        m_buf[slot, 2:3, :] = top
        m_buf[slot, 3:4, :] = mass

    def place(g, h, seat, value, store):
        if g < groups - 1 or splits == 1:
            store(g * hcount + h, slice(0, HD), value)
            return
        lanes = slice(seat * sub, (seat + 1) * sub)
        for s in range(splits):
            source = value if s == seat else pltpu.roll(value, (seat - s) % splits * sub, 1)
            store(last + s * tuples + lax.div(h, splits), lanes, source[:, lanes])

    def weigh(h, slot, seat):
        cols = head_cols(h)
        v_fresh = vf[:, :, :, cols].reshape(fresh_rows, HD)
        o = lax.dot_general(v_fresh, p_buf[slot, cached:, :], tn, preferred_element_type=F32)
        for a, b in blocks:
            o += lax.dot_general(
                vc[a:b, cols], p_buf[slot, a:b, :], tn, preferred_element_type=F32
            )
        for g in range(groups):
            part = slice(g * HD, (g + 1) * HD)

            def store_o(c, lanes, value):
                own_o[c, :, lanes] = value

            def store_s(c, lanes, value):
                own_s[c, :, lanes] = value

            place(g, h, seat, o[:, part], store_o)
            place(g, h, seat, m_buf[slot, 2:4, part], store_s)

    def project(g, p):
        deep = pl.ds(pl.multiple_of(p * pair * HD, HD), pair * HD)
        term = lax.dot_general(att[g, deep, :], w[deep, :], tn, preferred_element_type=F32)
        add(acc.at[g * HD : (g + 1) * HD, :], term, p)

    def project_last(s, p):
        deep = pl.ds(pl.multiple_of(p * splits * HD, HD), splits * HD)
        term = lax.dot_general(
            att[groups - 1 + s, deep, 0:sub], w[deep, :], tn, preferred_element_type=F32
        )
        add(acc.at[(groups - 1) * HD + s * sub : (groups - 1) * HD + (s + 1) * sub, :], term, p)

    def add(dest, term, p):
        @pl.when(p == 0)
        def _():
            dest[...] = term

        @pl.when(p > 0)
        def _():
            dest[...] += term

    pieces = [(g * HD, (g + 1) * HD) for g in range(groups - 1)]
    pieces += [((groups - 1) * HD + s * sub, (groups - 1) * HD + (s + 1) * sub) for s in range(splits)]

    def exchange(k):
        a, b = pieces[k]
        copies = []
        for d in range(1, heads_n):
            copies.append(
                pltpu.make_async_remote_copy(
                    src_ref=xs.at[d - 1, a:b],
                    dst_ref=xr.at[d - 1, a:b],
                    send_sem=x_send.at[d - 1],
                    recv_sem=x_recv.at[d - 1, k],
                    device_id={"head": lax.rem(hx + d, heads_n)},
                    device_id_type=MESH,
                )
            )
        return copies

    def exchange_start(k):
        a, b = pieces[k]
        cp = out_ref.shape[1]
        for d, c in enumerate(exchange(k)):
            peer = lax.rem(hx + d + 1, heads_n)
            cols = pl.ds(pl.multiple_of(peer * cp, HD), cp)
            xs[d, a:b] = acc[a:b, cols].astype(BF16)
            c.start()

    def service(t):
        cp_ = t - LAG * z
        in_p = (cp_ >= 0) & (cp_ < chunks)
        cs = t - LAG * (n - 1 - z)
        in_s = (cs >= 0) & (cs < chunks)

        @pl.when(in_p & (z > 0))
        def _():
            for c in send(cp_, 1):
                c.wait_recv()

        @pl.when(in_p & (z < n - 1))
        def _():
            combine(cp_, pre_o, pre_s, right_o, right_s)
            for c in send(cp_, 1):
                c.start()

        @pl.when(in_s & (z < n - 1))
        def _():
            for c in send(cs, -1):
                c.wait_recv()

        @pl.when(in_s & (z > 0))
        def _():
            combine(cs, suf_o, suf_s, left_o, left_s)
            for c in send(cs, -1):
                c.start()

    def finish(t):
        f = t - lag_end

        @pl.when((f >= 0) & (f < chunks))
        def _():
            m_a, m_b, m_c = own_s[f, 0:1], pre_s[f, 0:1], suf_s[f, 0:1]
            top = jnp.maximum(m_a, jnp.maximum(m_b, m_c))
            e_a, e_b, e_c = jnp.exp2(m_a - top), jnp.exp2(m_b - top), jnp.exp2(m_c - top)
            mass = own_s[f, 1:2] * e_a + pre_s[f, 1:2] * e_b + suf_s[f, 1:2] * e_c
            total_o = (
                own_o[f] * e_a + pre_o[f].astype(F32) * e_b + suf_o[f].astype(F32) * e_c
            )
            value = (total_o / mass).astype(BF16)

            @pl.when(f < last)
            def _():
                h = lax.rem(f, hcount)
                att[f // hcount, head_cols(h), :] = value

            @pl.when(f >= last)
            def _():
                k = f - last
                s, p = lax.div(k, tuples), lax.rem(k, tuples)
                for i in range(splits):
                    turned = value if i == 0 else pltpu.roll(total_o / mass, HD - i * sub, 1).astype(BF16)
                    att[groups - 1 + s, head_cols(p * splits + i), :] = turned

        @pl.when(f == hcount - pairs)
        def _():
            loads[4].wait()

        for g in range(groups - 1):
            begin = (g + 1) * hcount - pairs

            @pl.when((f >= begin) & (f < begin + pairs))
            def _(g=g, begin=begin):
                project(g, f - begin)

            if aligned:

                @pl.when(f == begin + pairs - 1)
                def _(g=g):
                    exchange_start(g)

        for s in range(splits):
            begin = last + s * tuples

            @pl.when((f >= begin) & (f < begin + tuples))
            def _(s=s, begin=begin):
                project_last(s, f - begin)

            if aligned and s < splits - 1:

                @pl.when(f == begin + tuples - 1)
                def _(s=s):
                    exchange_start(groups - 1 + s)

    def near(h):
        return jnp.minimum(h, hcount - 1)

    kv_loads[0].wait()
    for c in fresh_local:
        c.wait()
    for c in fresh_remote[0]:
        c.wait_recv()
    scores(0, 0)
    scores(min(1, hcount - 1), 1)
    for c in sq_copies:
        c.wait_recv()
    norm_total = jnp.sum(squares[...], axis=0)
    scale[...] = lax.rsqrt(norm_total / (HEADS * HD) + EPSILON) * (
        math.log2(math.e) / HD**0.5
    )
    soften(0, 0)
    kv_loads[1].wait()
    weigh(0, 0, 0)
    service(0)
    loads[4].start()
    soften(min(1, hcount - 1), 1)
    scores(min(2, hcount - 1), 0)

    unroll = max(splits, 2)

    def body(i, carry):
        for u in range(unroll):
            t = unroll * i + u
            if len(cuts) > 1:

                @pl.when(t + 3 == ahead)
                def _():
                    for c in fresh_remote[1]:
                        c.wait_recv()
                    for c in kv_loads[2:]:
                        c.wait()

            @pl.when(t + 1 < hcount)
            def _(t=t, u=u):
                scores(near(t + 3), (u + 1) % 2)
                soften(near(t + 2), u % 2)
                weigh(t + 1, (u + 1) % 2, (u + 1) % splits)

            finish(t)
            service(t + 1)
        return carry

    lax.fori_loop(0, -(-(chunks + LAG * (n - 1)) // unroll), body, 0)

    def settle():
        for d in range(1, seq_n):
            for side in (0, 1):
                fresh_wait(d, side, slice(0, width)).wait_send()
        for c in sq_copies:
            c.wait_send()

        @pl.when(z < n - 1)
        def _():
            settle_sends(1)

        @pl.when(z > 0)
        def _():
            settle_sends(-1)

    if aligned:
        cp = out_ref.shape[1]
        mine = pl.ds(pl.multiple_of(hx * cp, HD), cp)
        exchange_start(len(pieces) - 1)
        settle()
        for k, (a, b) in enumerate(pieces):
            summed = acc[a:b, mine]
            for d, c in enumerate(exchange(k)):
                c.wait_recv()
                summed = summed + xr[d, a:b].astype(F32)
            out_ref[a:b, :] = (summed * gate[...]).astype(out_ref.dtype)
        for d in range(1, heads_n):
            pltpu.make_async_remote_copy(
                src_ref=xs.at[d - 1],
                dst_ref=xr.at[d - 1],
                send_sem=x_send.at[d - 1],
                recv_sem=x_recv.at[d - 1, 0],
                device_id={"head": lax.rem(hx + d, heads_n)},
                device_id_type=MESH,
            ).wait_send()
    else:
        out_ref[...] = acc[...]
        settle()


def local(sizes, *args):
    (
        queries,
        query_gain,
        cache_keys,
        cache_values,
        finished_keys,
        finished_values,
        new_keys,
        new_values,
        out_weight,
        time_weight,
        owner,
        step,
    ) = args
    n, heads_n, seq_n = sizes
    rows, width = queries.shape
    hcount = width // HD
    cached, fresh = cache_keys.shape[0], finished_keys.shape[0]
    columns, cp = out_weight.shape[1], time_weight.shape[1]
    freq = time_weight.shape[0]
    aligned = cp % HD == 0
    any_spec = pl.BlockSpec(memory_space=pl.ANY)
    smem = pl.BlockSpec(memory_space=pltpu.SMEM)
    vmem = pl.BlockSpec(memory_space=pltpu.VMEM)
    dma = pltpu.SemaphoreType.DMA
    xcount = max(heads_n - 1, 1)
    groups = rows // HD
    chunks = groups * hcount
    ring = min(chunks, LAG * (n - 1) + 1)
    stat = (chunks, 2, HD)
    keys = cached + seq_n * 2 * fresh
    part = (chunks, HD, HD)
    result = pl.pallas_call(
        functools.partial(kernel, sizes, aligned),
        out_shape=pltpu.VMEM((rows, cp), BF16) if aligned else jax.ShapeDtypeStruct((rows, columns), F32),
        in_specs=[any_spec] * 10 + [smem] * 2,
        out_specs=vmem,
        scratch_shapes=[
            pltpu.VMEM((rows, width), BF16),
            pltpu.VMEM((rows, width), BF16),
            pltpu.VMEM((width,), F32),
            pltpu.VMEM((cached, width), BF16),
            pltpu.VMEM((cached, width), BF16),
            pltpu.VMEM((seq_n, 2, fresh, width), BF16),
            pltpu.VMEM((seq_n, 2, fresh, width), BF16),
            pltpu.VMEM((width, columns), BF16),
            pltpu.VMEM((freq, cp), F32),
            pltpu.VMEM((heads_n, 8, rows), F32),
            pltpu.VMEM((8, rows), F32),
            pltpu.VMEM(part, F32),
            pltpu.VMEM(stat, F32),
            pltpu.VMEM(part, BF16),
            pltpu.VMEM(stat, F32),
            pltpu.VMEM(part, BF16),
            pltpu.VMEM(stat, F32),
            pltpu.VMEM(part, BF16),
            pltpu.VMEM(stat, F32),
            pltpu.VMEM(part, BF16),
            pltpu.VMEM(stat, F32),
            pltpu.VMEM((groups + SPLIT - 1, width, HD), BF16),
            pltpu.VMEM((rows, columns), F32),
            pltpu.VMEM((1, cp), F32),
            pltpu.VMEM((xcount, rows, cp), BF16),
            pltpu.VMEM((xcount, rows, cp), BF16),
            dma((6,)),
            dma((2,)),
            dma((max(seq_n - 1, 1), 2)),
            dma((max(seq_n - 1, 1), 2, 2)),
            dma((xcount,)),
            dma((xcount,)),
            dma((2,)),
            dma((ring, 2)),
            dma((2,)),
            dma((ring, 2)),
            dma((xcount,)),
            dma((xcount, groups + SPLIT - 1)),
            pltpu.VMEM((2, keys, rows), F32),
            pltpu.VMEM((2, keys, rows), BF16),
            pltpu.VMEM((2, 4, rows), F32),
            dma((PARTS,)),
            dma((2, 2)),
        ],
        compiler_params=pltpu.CompilerParams(
            collective_id=0, has_side_effects=True, vmem_limit_bytes=60 * 1024 * 1024
        ),
        name="sweep_attention",
    )(
        queries,
        query_gain,
        cache_keys,
        cache_values,
        finished_keys,
        finished_values,
        new_keys,
        new_values,
        out_weight,
        time_weight,
        owner,
        step,
    )
    if aligned:
        return result
    summed = lax.psum_scatter(result, "head", scatter_dimension=1, tiled=True)
    half = freq // 2
    frequency = jnp.exp(-jnp.log(10000.0) * jnp.arange(half, dtype=F32) / half)
    phases = step[0].astype(F32) * frequency
    embedding = jnp.concatenate([jnp.cos(phases), jnp.sin(phases)])
    time_gate = 1.0 + jnp.dot(embedding, time_weight, precision=lax.Precision.HIGHEST)
    return (time_gate * summed).astype(BF16)


def solution(mesh):
    in_specs = (
        P(("grp", "seq"), "head"),
        P("head"),
        P(("grp", "slab"), "head"),
        P(("grp", "slab"), "head"),
        P(("grp", "slab", "seq"), "head"),
        P(("grp", "slab", "seq"), "head"),
        P(("grp", "slab", "seq"), "head"),
        P(("grp", "slab", "seq"), "head"),
        P("head", "slab"),
        P(None, ("slab", "head")),
        P("grp"),
        P("grp"),
    )
    out_specs = P(("grp", "seq"), ("slab", "head"))
    sizes = (mesh.shape["slab"], mesh.shape["head"], mesh.shape["seq"])
    return jax.shard_map(
        functools.partial(local, sizes),
        mesh=mesh,
        in_specs=in_specs,
        out_specs=out_specs,
        check_vma=False,
    )
```

```python
import functools
import math

import jax
import jax.numpy as jnp
from jax import lax
from jax.experimental import pallas as pl
from jax.experimental.pallas import tpu as pltpu
from jax.sharding import PartitionSpec as P

HEADS = 40
HD = 128
EPSILON = 1e-06
LOW = -1e30
LAG = 5
SPLIT = 2
PARTS = 4
MESH = pl.DeviceIdType.MESH
F32 = jnp.float32
BF16 = jnp.bfloat16


def kernel(
    dims,
    aligned,
    q_ref,
    gain_ref,
    ck_ref,
    cv_ref,
    fk_ref,
    fv_ref,
    nk_ref,
    nv_ref,
    w_ref,
    tw_ref,
    owner_ref,
    step_ref,
    out_ref,
    q,
    qg,
    gain,
    kc,
    vc,
    kf,
    vf,
    w,
    tw,
    squares,
    scale,
    own_o,
    own_s,
    pre_o,
    pre_s,
    suf_o,
    suf_s,
    right_o,
    right_s,
    left_o,
    left_s,
    att,
    acc,
    gate,
    xs,
    xr,
    load_sem,
    fresh_sem,
    fresh_send,
    fresh_recv,
    sq_send,
    sq_recv,
    right_send,
    right_recv,
    left_send,
    left_recv,
    x_send,
    x_recv,
    s_buf,
    p_buf,
    m_buf,
    q_sem,
    kv_sem,
    gauge,
):
    n, heads_n, seq_n = dims
    rows, width = q_ref.shape
    hcount = width // HD
    z = lax.axis_index("slab")
    hx = lax.axis_index("head")
    sq = lax.axis_index("seq")

    groups = rows // HD
    chunks = groups * hcount
    gain_load, w_load, tw_load = [
        pltpu.make_async_copy(src, dst, load_sem.at[i])
        for i, (src, dst) in enumerate([(gain_ref, gain), (w_ref, w), (tw_ref, tw)])
    ]
    ahead = min(max(hcount // 5, 3), hcount)
    parts = PARTS if hcount % PARTS == 0 else 1
    span = width // parts
    q_loads = [
        pltpu.make_async_copy(
            q_ref.at[:, k * span : (k + 1) * span], q.at[:, k * span : (k + 1) * span], q_sem.at[k]
        )
        for k in range(parts)
    ]
    for c in q_loads:
        c.start()
    gain_load.start()
    barrier = pltpu.get_barrier_semaphore()
    for d in range(1, seq_n):
        pl.semaphore_signal(
            barrier, inc=1, device_id={"seq": lax.rem(sq + d, seq_n)}, device_id_type=MESH
        )
    for d in range(1, heads_n):
        pl.semaphore_signal(
            barrier, inc=1, device_id={"head": lax.rem(hx + d, heads_n)}, device_id_type=MESH
        )

    @pl.when(z > 0)
    def _():
        pl.semaphore_signal(barrier, inc=1, device_id={"slab": z - 1}, device_id_type=MESH)

    @pl.when(z < n - 1)
    def _():
        pl.semaphore_signal(barrier, inc=1, device_id={"slab": z + 1}, device_id_type=MESH)

    def clear(o_ref, s_ref):
        o_ref[...] = jnp.zeros_like(o_ref)
        s_ref[:, 0:1, :] = jnp.full((chunks, 1, HD), LOW, F32)
        s_ref[:, 1:2, :] = jnp.zeros((chunks, 1, HD), F32)

    @pl.when(z == 0)
    def _():
        clear(pre_o, pre_s)

    @pl.when(z == n - 1)
    def _():
        clear(suf_o, suf_s)

    def squares_step(h, total):
        x = q[:, pl.ds(pl.multiple_of(h * HD, HD), HD)].astype(F32)
        return total + x * x

    total = jnp.zeros((rows, HD), F32)
    for k, c in enumerate(q_loads):
        c.wait()
        total = lax.fori_loop(k * hcount // parts, (k + 1) * hcount // parts, squares_step, total)
    head_cut = ahead * HD
    kv_cuts = [slice(0, head_cut), slice(head_cut, width)] if head_cut < width else [slice(0, width)]
    kv_loads = []
    for k, cols in enumerate(kv_cuts):
        for i, (src, dst) in enumerate([(ck_ref, kc), (cv_ref, vc)]):
            kv_loads.append(pltpu.make_async_copy(src.at[:, cols], dst.at[:, cols], kv_sem.at[k, i]))
    fresh_src = [(fk_ref, kf, 0), (nk_ref, kf, 1), (fv_ref, vf, 0), (nv_ref, vf, 1)]
    tw_load.start()
    for c in kv_loads:
        c.start()
    fresh_local = []
    for i, (src, dst, part) in enumerate(fresh_src):
        pltpu.make_async_copy(src, dst.at[sq, part], fresh_sem.at[i // 2]).start()
    for side, whole in enumerate((kf, vf)):
        fresh_local.append(pltpu.make_async_copy(whole.at[sq], whole.at[sq], fresh_sem.at[side]))
    row_total = jnp.sum(total.T, axis=0, keepdims=True)
    squares[hx] = row_total

    ends = (z == 0).astype(jnp.int32) + (z == n - 1).astype(jnp.int32)
    pl.semaphore_wait(barrier, seq_n - 1 + heads_n - 1 + 2 - ends)

    sq_copies = []
    for d in range(1, heads_n):
        c = pltpu.make_async_remote_copy(
            src_ref=squares.at[hx],
            dst_ref=squares.at[hx],
            send_sem=sq_send.at[d - 1],
            recv_sem=sq_recv.at[d - 1],
            device_id={"head": lax.rem(hx + d, heads_n)},
            device_id_type=MESH,
        )
        c.start()
        sq_copies.append(c)

    edges = [0, ahead * HD, width] if ahead < hcount else [0, width]
    cuts = [slice(a, b) for a, b in zip(edges, edges[1:])]
    fresh_remote = [[] for _ in cuts]

    def fresh_wait(d, side, cols, k=0):
        whole = (kf, vf)[side].at[sq, :, :, cols]
        return pltpu.make_async_remote_copy(
            src_ref=whole,
            dst_ref=whole,
            send_sem=fresh_send.at[d - 1, side],
            recv_sem=fresh_recv.at[d - 1, k, side],
            device_id={"seq": lax.rem(sq + d, seq_n)},
            device_id_type=MESH,
        )

    for k, cols in enumerate(cuts):
        for d in range(1, seq_n):
            for i, (src, dst, part) in enumerate(fresh_src):
                pltpu.make_async_remote_copy(
                    src_ref=src.at[:, cols],
                    dst_ref=dst.at[sq, part, :, cols],
                    send_sem=fresh_send.at[d - 1, i // 2],
                    recv_sem=fresh_recv.at[d - 1, k, i // 2],
                    device_id={"seq": lax.rem(sq + d, seq_n)},
                    device_id_type=MESH,
                ).start()
            fresh_remote[k] += [fresh_wait(d, side, cols, k) for side in (0, 1)]

    gain_load.wait()

    def gain_step(h, carry):
        cols = pl.ds(pl.multiple_of(h * HD, HD), HD)
        qg[:, cols] = (q[:, cols].astype(F32) * gain[cols][None, :]).astype(BF16)
        return carry

    lax.fori_loop(0, hcount, gain_step, 0)
    tw_load.wait()
    if aligned:
        half = tw.shape[0] // 2
        j = lax.broadcasted_iota(jnp.int32, (half, HD), 0).astype(F32)
        frequency = jnp.exp(F32(-math.log(10000.0)) * j / half)
        phases = jnp.full((half, HD), step_ref[0], jnp.int32).astype(F32) * frequency
        cos, sin = jnp.cos(phases), jnp.sin(phases)
        for c in range(tw.shape[1] // HD):
            cols = slice(c * HD, (c + 1) * HD)
            terms = tw[:half, cols] * cos + tw[half:, cols] * sin
            gate[:, cols] = 1.0 + jnp.sum(terms, axis=0, keepdims=True)


    ring = min(chunks, LAG * (n - 1) + 1)

    def send(h, direction):
        if direction > 0:
            pairs, ss, rs = ((right_o, pre_o), (right_s, pre_s)), right_send, right_recv
        else:
            pairs, ss, rs = ((left_o, suf_o), (left_s, suf_s)), left_send, left_recv
        return [
            pltpu.make_async_remote_copy(
                src_ref=src.at[h],
                dst_ref=dst.at[h],
                send_sem=ss.at[i],
                recv_sem=rs.at[lax.rem(h, ring)],
                device_id={"slab": z + direction},
                device_id_type=MESH,
            )
            for i, (src, dst) in enumerate(pairs)
        ]

    def arrived(h, direction):
        ss, rs = (right_send, right_recv) if direction > 0 else (left_send, left_recv)
        pltpu.make_async_remote_copy(
            src_ref=gauge,
            dst_ref=gauge,
            send_sem=ss.at[0],
            recv_sem=rs.at[lax.rem(h, ring)],
            device_id={"slab": z - direction},
            device_id_type=MESH,
        ).wait_recv()

    def settle_sends(direction):
        if direction > 0:
            pairs, ss, rs = ((right_o, pre_o), (right_s, pre_s)), right_send, right_recv
        else:
            pairs, ss, rs = ((left_o, suf_o), (left_s, suf_s)), left_send, left_recv
        for i, (src, dst) in enumerate(pairs):
            pltpu.make_async_remote_copy(
                src_ref=src,
                dst_ref=dst,
                send_sem=ss.at[i],
                recv_sem=rs.at[0],
                device_id={"slab": z + direction},
                device_id_type=MESH,
            ).wait_send()

    pair = 2 if hcount % 2 == 0 else 1
    splits = next(k for k in (SPLIT, 2, 1) if hcount % k == 0)
    sub = HD // splits
    tuples = hcount // splits
    pairs = hcount // pair
    last = (groups - 1) * hcount
    fresh_rows = seq_n * 2 * fk_ref.shape[0]
    lag_end = LAG * jnp.maximum(z, n - 1 - z)

    def combine(h, other_o, other_s, dest_o, dest_s):
        m_a, l_a = own_s[h, 0:1], own_s[h, 1:2]
        m_b, l_b = other_s[h, 0:1], other_s[h, 1:2]
        top = jnp.maximum(m_a, m_b)
        e_a, e_b = jnp.exp2(m_a - top), jnp.exp2(m_b - top)
        dest_o[h] = (own_o[h] * e_a + other_o[h].astype(F32) * e_b).astype(BF16)
        dest_s[h, 0:1] = top
        dest_s[h, 1:2] = l_a * e_a + l_b * e_b

    nt = (((1,), (1,)), ((), ()))
    tn = (((0,), (0,)), ((), ()))

    penalty = jnp.where(
        jnp.full((1, rows), owner_ref[0], jnp.int32) == z, F32(LOW), F32(0.0)
    )
    cached = kc.shape[0]
    step_keys = 256 if cached % 256 == 0 else cached
    blocks = [(i, i + step_keys) for i in range(0, cached, step_keys)]

    def head_cols(h):
        return pl.ds(pl.multiple_of(h * HD, HD), HD)

    def scores(h, slot):
        cols = head_cols(h)
        q_head = qg[:, cols]
        top = None
        for a, b in blocks:
            part = lax.dot_general(kc[a:b, cols], q_head, nt, preferred_element_type=F32)
            s_buf[slot, a:b, :] = part
            high = jnp.max(part, axis=0, keepdims=True)
            top = high if top is None else jnp.maximum(top, high)
        k_fresh = kf[:, :, :, cols].reshape(fresh_rows, HD)
        part = lax.dot_general(k_fresh, q_head, nt, preferred_element_type=F32)
        s_buf[slot, cached:, :] = part
        m_buf[slot, 0:1, :] = top
        m_buf[slot, 1:2, :] = jnp.max(part, axis=0, keepdims=True)

    def soften(slot, r=slice(None)):
        s_row = scale[0:1, r]
        mask = penalty[:, r]
        top = jnp.maximum(m_buf[slot, 0:1, r] * s_row + mask, m_buf[slot, 1:2, r] * s_row)
        top_c = top - mask
        mass = jnp.zeros_like(top)
        for a, b in blocks + [(cached, cached + fresh_rows)]:
            p = jnp.exp2(s_buf[slot, a:b, r] * s_row - (top_c if a < cached else top))
            p_buf[slot, a:b, r] = p.astype(BF16)
            mass = mass + jnp.sum(p, axis=0, keepdims=True)
        m_buf[slot, 2:3, r] = top
        m_buf[slot, 3:4, r] = mass

    def place(g, h, seat, value, store):
        if g < groups - 1 or splits == 1:
            store(g * hcount + h, slice(0, HD), value)
            return
        lanes = slice(seat * sub, (seat + 1) * sub)
        for s in range(splits):
            source = value if s == seat else pltpu.roll(value, (seat - s) % splits * sub, 1)
            store(last + s * tuples + lax.div(h, splits), lanes, source[:, lanes])

    def weigh(h, slot, seat, first=0, end=None):
        cols = head_cols(h)
        end = groups if end is None else end
        r = slice(first * HD, end * HD)
        v_fresh = vf[:, :, :, cols].reshape(fresh_rows, HD)
        o = lax.dot_general(v_fresh, p_buf[slot, cached:, r], tn, preferred_element_type=F32)
        for a, b in blocks:
            o += lax.dot_general(
                vc[a:b, cols], p_buf[slot, a:b, r], tn, preferred_element_type=F32
            )

        def store_o(c, lanes, value):
            own_o[c, :, lanes] = value

        def store_s(c, lanes, value):
            own_s[c, :, lanes] = value

        for g in range(first, end):
            place(g, h, seat, o[:, (g - first) * HD : (g - first + 1) * HD], store_o)
            place(g, h, seat, m_buf[slot, 2:4, g * HD : (g + 1) * HD], store_s)

    def project(g, p):
        deep = pl.ds(pl.multiple_of(p * pair * HD, HD), pair * HD)
        term = lax.dot_general(att[g, deep, :], w[deep, :], tn, preferred_element_type=F32)
        add(acc.at[g * HD : (g + 1) * HD, :], term, p)

    def project_last(s, p):
        deep = pl.ds(pl.multiple_of(p * splits * HD, HD), splits * HD)
        term = lax.dot_general(
            att[groups - 1 + s, deep, 0:sub], w[deep, :], tn, preferred_element_type=F32
        )
        add(acc.at[(groups - 1) * HD + s * sub : (groups - 1) * HD + (s + 1) * sub, :], term, p)

    def add(dest, term, p):
        @pl.when(p == 0)
        def _():
            dest[...] = term

        @pl.when(p > 0)
        def _():
            dest[...] += term

    pieces = [(g * HD, (g + 1) * HD) for g in range(groups - 1)]
    pieces += [((groups - 1) * HD + s * sub, (groups - 1) * HD + (s + 1) * sub) for s in range(splits)]

    def exchange(k):
        a, b = pieces[k]
        copies = []
        for d in range(1, heads_n):
            copies.append(
                pltpu.make_async_remote_copy(
                    src_ref=xs.at[d - 1, a:b],
                    dst_ref=xr.at[d - 1, a:b],
                    send_sem=x_send.at[d - 1],
                    recv_sem=x_recv.at[d - 1, k],
                    device_id={"head": lax.rem(hx + d, heads_n)},
                    device_id_type=MESH,
                )
            )
        return copies

    def exchange_start(k):
        a, b = pieces[k]
        cp = out_ref.shape[1]
        for d, c in enumerate(exchange(k)):
            peer = lax.rem(hx + d + 1, heads_n)
            cols = pl.ds(pl.multiple_of(peer * cp, HD), cp)
            xs[d, a:b] = acc[a:b, cols].astype(BF16)
            c.start()

    def service(t):
        cp_ = t - LAG * z
        in_p = (cp_ >= 0) & (cp_ < chunks)
        cs = t - LAG * (n - 1 - z)
        in_s = (cs >= 0) & (cs < chunks)

        @pl.when(in_p & (z > 0))
        def _():
            arrived(cp_, 1)

        @pl.when(in_p & (z < n - 1))
        def _():
            combine(cp_, pre_o, pre_s, right_o, right_s)
            for c in send(cp_, 1):
                c.start()

        @pl.when(in_s & (z < n - 1))
        def _():
            arrived(cs, -1)

        @pl.when(in_s & (z > 0))
        def _():
            combine(cs, suf_o, suf_s, left_o, left_s)
            for c in send(cs, -1):
                c.start()

    def finish(t):
        f = t - lag_end

        @pl.when((f >= 0) & (f < chunks))
        def _():
            m_a, m_b, m_c = own_s[f, 0:1], pre_s[f, 0:1], suf_s[f, 0:1]
            top = jnp.maximum(m_a, jnp.maximum(m_b, m_c))
            e_a, e_b, e_c = jnp.exp2(m_a - top), jnp.exp2(m_b - top), jnp.exp2(m_c - top)
            mass = own_s[f, 1:2] * e_a + pre_s[f, 1:2] * e_b + suf_s[f, 1:2] * e_c
            total_o = (
                own_o[f] * e_a + pre_o[f].astype(F32) * e_b + suf_o[f].astype(F32) * e_c
            )
            value = (total_o / mass).astype(BF16)

            @pl.when(f < last)
            def _():
                h = lax.rem(f, hcount)
                att[f // hcount, head_cols(h), :] = value

            @pl.when(f >= last)
            def _():
                k = f - last
                s, p = lax.div(k, tuples), lax.rem(k, tuples)
                for i in range(splits):
                    turned = value if i == 0 else pltpu.roll(total_o / mass, HD - i * sub, 1).astype(BF16)
                    att[groups - 1 + s, head_cols(p * splits + i), :] = turned

        @pl.when(f == hcount - pairs)
        def _():
            w_load.wait()

        for g in range(groups - 1):
            begin = (g + 1) * hcount - pairs

            @pl.when((f >= begin) & (f < begin + pairs))
            def _(g=g, begin=begin):
                project(g, f - begin)

            if aligned:

                @pl.when(f == begin + pairs - 1)
                def _(g=g):
                    exchange_start(g)

        for s in range(splits):
            begin = last + s * tuples

            stop = begin + tuples - (1 if aligned and s == splits - 1 else 0)

            @pl.when((f >= begin) & (f < stop))
            def _(s=s, begin=begin):
                project_last(s, f - begin)

            if aligned and s < splits - 1:

                @pl.when(f == begin + tuples - 1)
                def _(s=s):
                    exchange_start(groups - 1 + s)

        if aligned:

            @pl.when(f == chunks - 1)
            def _():
                a, b = pieces[-1]
                cp = out_ref.shape[1]
                deep = slice((tuples - 1) * splits * HD, tuples * splits * HD)
                sums = att[groups + splits - 2, deep, 0:sub]

                def total_of(owner):
                    cols = pl.ds(pl.multiple_of(owner * cp, HD), cp)
                    before = 0.0 if tuples == 1 else acc[a:b, cols]
                    return cols, before + lax.dot_general(
                        sums, w[deep, cols], tn, preferred_element_type=F32
                    )

                for d, c in enumerate(exchange(len(pieces) - 1)):
                    xs[d, a:b] = total_of(lax.rem(hx + d + 1, heads_n))[1].astype(BF16)
                    c.start()
                cols, own = total_of(hx)
                acc[a:b, cols] = own

    def near(h):
        return jnp.minimum(h, hcount - 1)

    kv_loads[0].wait()
    for c in fresh_local:
        c.wait()
    for c in fresh_remote[0]:
        c.wait_recv()
    scores(0, 0)
    scores(min(1, hcount - 1), 1)
    for c in sq_copies:
        c.wait_recv()
    norm_total = jnp.sum(squares[...], axis=0)
    scale[...] = lax.rsqrt(norm_total / (HEADS * HD) + EPSILON) * (
        math.log2(math.e) / HD**0.5
    )
    soften(0, slice(0, HD))
    kv_loads[1].wait()
    weigh(0, 0, 0, 0, 1)
    service(0)
    w_load.start()
    if groups > 1:
        soften(0, slice(HD, rows))
        weigh(0, 0, 0, 1, groups)
    soften(1)
    scores(min(2, hcount - 1), 0)

    unroll = max(splits, 2)

    def body(i, carry):
        for u in range(unroll):
            t = unroll * i + u
            if len(cuts) > 1:

                @pl.when(t + 3 == ahead)
                def _():
                    for c in fresh_remote[1]:
                        c.wait_recv()
                    for c in kv_loads[2:]:
                        c.wait()

            @pl.when(t + 1 < hcount)
            def _(t=t, u=u):
                scores(near(t + 3), (u + 1) % 2)
                soften(u % 2)
                weigh(t + 1, (u + 1) % 2, (u + 1) % splits)

            finish(t)
            service(t + 1)
        return carry

    lax.fori_loop(0, -(-(chunks + LAG * (n - 1)) // unroll), body, 0)

    def settle():
        for d in range(1, seq_n):
            for side in (0, 1):
                fresh_wait(d, side, slice(0, width)).wait_send()
        for c in sq_copies:
            c.wait_send()

        @pl.when(z < n - 1)
        def _():
            settle_sends(1)

        @pl.when(z > 0)
        def _():
            settle_sends(-1)

    if aligned:
        cp = out_ref.shape[1]
        mine = pl.ds(pl.multiple_of(hx * cp, HD), cp)
        settle()
        for k, (a, b) in enumerate(pieces):
            summed = acc[a:b, mine]
            for d, c in enumerate(exchange(k)):
                c.wait_recv()
                summed = summed + xr[d, a:b].astype(F32)
            out_ref[a:b, :] = (summed * gate[...]).astype(out_ref.dtype)
        for d in range(1, heads_n):
            pltpu.make_async_remote_copy(
                src_ref=xs.at[d - 1],
                dst_ref=xr.at[d - 1],
                send_sem=x_send.at[d - 1],
                recv_sem=x_recv.at[d - 1, 0],
                device_id={"head": lax.rem(hx + d, heads_n)},
                device_id_type=MESH,
            ).wait_send()
    else:
        out_ref[...] = acc[...]
        settle()


def local(sizes, *args):
    (
        queries,
        query_gain,
        cache_keys,
        cache_values,
        finished_keys,
        finished_values,
        new_keys,
        new_values,
        out_weight,
        time_weight,
        owner,
        step,
    ) = args
    n, heads_n, seq_n = sizes
    rows, width = queries.shape
    hcount = width // HD
    cached, fresh = cache_keys.shape[0], finished_keys.shape[0]
    columns, cp = out_weight.shape[1], time_weight.shape[1]
    freq = time_weight.shape[0]
    aligned = cp % HD == 0
    any_spec = pl.BlockSpec(memory_space=pl.ANY)
    smem = pl.BlockSpec(memory_space=pltpu.SMEM)
    vmem = pl.BlockSpec(memory_space=pltpu.VMEM)
    dma = pltpu.SemaphoreType.DMA
    xcount = max(heads_n - 1, 1)
    groups = rows // HD
    chunks = groups * hcount
    ring = min(chunks, LAG * (n - 1) + 1)
    stat = (chunks, 2, HD)
    keys = cached + seq_n * 2 * fresh
    part = (chunks, HD, HD)
    result = pl.pallas_call(
        functools.partial(kernel, sizes, aligned),
        out_shape=pltpu.VMEM((rows, cp), BF16) if aligned else jax.ShapeDtypeStruct((rows, columns), F32),
        in_specs=[any_spec] * 10 + [smem] * 2,
        out_specs=vmem,
        scratch_shapes=[
            pltpu.VMEM((rows, width), BF16),
            pltpu.VMEM((rows, width), BF16),
            pltpu.VMEM((width,), F32),
            pltpu.VMEM((cached, width), BF16),
            pltpu.VMEM((cached, width), BF16),
            pltpu.VMEM((seq_n, 2, fresh, width), BF16),
            pltpu.VMEM((seq_n, 2, fresh, width), BF16),
            pltpu.VMEM((width, columns), BF16),
            pltpu.VMEM((freq, cp), F32),
            pltpu.VMEM((heads_n, 1, rows), F32),
            pltpu.VMEM((1, rows), F32),
            pltpu.VMEM(part, F32),
            pltpu.VMEM(stat, F32),
            pltpu.VMEM(part, BF16),
            pltpu.VMEM(stat, F32),
            pltpu.VMEM(part, BF16),
            pltpu.VMEM(stat, F32),
            pltpu.VMEM(part, BF16),
            pltpu.VMEM(stat, F32),
            pltpu.VMEM(part, BF16),
            pltpu.VMEM(stat, F32),
            pltpu.VMEM((groups + SPLIT - 1, width, HD), BF16),
            pltpu.VMEM((rows, columns), F32),
            pltpu.VMEM((1, cp), F32),
            pltpu.VMEM((xcount, rows, cp), BF16),
            pltpu.VMEM((xcount, rows, cp), BF16),
            dma((3,)),
            dma((2,)),
            dma((max(seq_n - 1, 1), 2)),
            dma((max(seq_n - 1, 1), 2, 2)),
            dma((xcount,)),
            dma((xcount,)),
            dma((2,)),
            dma((ring,)),
            dma((2,)),
            dma((ring,)),
            dma((xcount,)),
            dma((xcount, groups + SPLIT - 1)),
            pltpu.VMEM((2, keys, rows), F32),
            pltpu.VMEM((2, keys, rows), BF16),
            pltpu.VMEM((2, 4, rows), F32),
            dma((PARTS,)),
            dma((2, 2)),
            pltpu.VMEM((HD // 4 + 1, 2, HD), F32),
        ],
        compiler_params=pltpu.CompilerParams(
            collective_id=0, has_side_effects=True, vmem_limit_bytes=60 * 1024 * 1024
        ),
        name="sweep_attention",
    )(
        queries,
        query_gain,
        cache_keys,
        cache_values,
        finished_keys,
        finished_values,
        new_keys,
        new_values,
        out_weight,
        time_weight,
        owner,
        step,
    )
    if aligned:
        return result
    summed = lax.psum_scatter(result, "head", scatter_dimension=1, tiled=True)
    half = freq // 2
    frequency = jnp.exp(-jnp.log(10000.0) * jnp.arange(half, dtype=F32) / half)
    phases = step[0].astype(F32) * frequency
    embedding = jnp.concatenate([jnp.cos(phases), jnp.sin(phases)])
    time_gate = 1.0 + jnp.dot(embedding, time_weight, precision=lax.Precision.HIGHEST)
    return (time_gate * summed).astype(BF16)


def solution(mesh):
    in_specs = (
        P(("grp", "seq"), "head"),
        P("head"),
        P(("grp", "slab"), "head"),
        P(("grp", "slab"), "head"),
        P(("grp", "slab", "seq"), "head"),
        P(("grp", "slab", "seq"), "head"),
        P(("grp", "slab", "seq"), "head"),
        P(("grp", "slab", "seq"), "head"),
        P("head", "slab"),
        P(None, ("slab", "head")),
        P("grp"),
        P("grp"),
    )
    out_specs = P(("grp", "seq"), ("slab", "head"))
    sizes = (mesh.shape["slab"], mesh.shape["head"], mesh.shape["seq"])
    return jax.shard_map(
        functools.partial(local, sizes),
        mesh=mesh,
        in_specs=in_specs,
        out_specs=out_specs,
        check_vma=False,
    )
```

```python
import functools
import math

import jax
import jax.numpy as jnp
from jax import lax
from jax.experimental import pallas as pl
from jax.experimental.pallas import tpu as pltpu
from jax.sharding import PartitionSpec as P

HEADS = 40
HD = 128
EPSILON = 1e-06
LOW = -1e30
LAG = 5
SPLIT = 2
PARTS = 4
MESH = pl.DeviceIdType.MESH
F32 = jnp.float32
BF16 = jnp.bfloat16


def kernel(
    dims,
    aligned,
    q_ref,
    gain_ref,
    ck_ref,
    cv_ref,
    fk_ref,
    fv_ref,
    nk_ref,
    nv_ref,
    w_ref,
    tw_ref,
    owner_ref,
    step_ref,
    out_ref,
    q,
    qg,
    gain,
    kc,
    vc,
    kf,
    vf,
    w,
    tw,
    squares,
    scale,
    own_o,
    own_s,
    pre_o,
    pre_s,
    suf_o,
    suf_s,
    right_o,
    right_s,
    left_o,
    left_s,
    att,
    acc,
    gate,
    xs,
    xr,
    load_sem,
    fresh_sem,
    fresh_send,
    fresh_recv,
    sq_send,
    sq_recv,
    right_send,
    right_recv,
    left_send,
    left_recv,
    x_send,
    x_recv,
    s_buf,
    p_buf,
    m_buf,
    q_sem,
    kv_sem,
    gauge,
):
    n, heads_n, seq_n = dims
    rows, width = q_ref.shape
    hcount = width // HD
    z = lax.axis_index("slab")
    hx = lax.axis_index("head")
    sq = lax.axis_index("seq")

    groups = rows // HD
    chunks = groups * hcount
    gain_load, w_load, tw_load = [
        pltpu.make_async_copy(src, dst, load_sem.at[i])
        for i, (src, dst) in enumerate([(gain_ref, gain), (w_ref, w), (tw_ref, tw)])
    ]
    ahead = min(max(hcount // 5, 3), hcount)
    parts = PARTS if hcount % PARTS == 0 else 1
    span = width // parts
    q_loads = [
        pltpu.make_async_copy(
            q_ref.at[:, k * span : (k + 1) * span], q.at[:, k * span : (k + 1) * span], q_sem.at[k]
        )
        for k in range(parts)
    ]
    for c in q_loads:
        c.start()
    gain_load.start()
    barrier = pltpu.get_barrier_semaphore()
    for d in range(1, seq_n):
        pl.semaphore_signal(
            barrier, inc=1, device_id={"seq": lax.rem(sq + d, seq_n)}, device_id_type=MESH
        )
    for d in range(1, heads_n):
        pl.semaphore_signal(
            barrier, inc=1, device_id={"head": lax.rem(hx + d, heads_n)}, device_id_type=MESH
        )

    @pl.when(z > 0)
    def _():
        pl.semaphore_signal(barrier, inc=1, device_id={"slab": z - 1}, device_id_type=MESH)

    @pl.when(z < n - 1)
    def _():
        pl.semaphore_signal(barrier, inc=1, device_id={"slab": z + 1}, device_id_type=MESH)

    def clear(o_ref, s_ref):
        o_ref[...] = jnp.zeros_like(o_ref)
        s_ref[...] = jnp.full((chunks, 1, HD), LOW, F32)

    @pl.when(z == 0)
    def _():
        clear(pre_o, pre_s)

    @pl.when(z == n - 1)
    def _():
        clear(suf_o, suf_s)

    def squares_step(h, total):
        x = q[:, pl.ds(pl.multiple_of(h * HD, HD), HD)].astype(F32)
        return total + x * x

    total = jnp.zeros((rows, HD), F32)
    for k, c in enumerate(q_loads):
        c.wait()
        total = lax.fori_loop(k * hcount // parts, (k + 1) * hcount // parts, squares_step, total)
    head_cut = ahead * HD
    kv_cuts = [slice(0, head_cut), slice(head_cut, width)] if head_cut < width else [slice(0, width)]
    kv_loads = []
    for k, cols in enumerate(kv_cuts):
        for i, (src, dst) in enumerate([(ck_ref, kc), (cv_ref, vc)]):
            kv_loads.append(pltpu.make_async_copy(src.at[:, cols], dst.at[:, cols], kv_sem.at[k, i]))
    fresh_src = [(fk_ref, kf, 0), (nk_ref, kf, 1), (fv_ref, vf, 0), (nv_ref, vf, 1)]
    tw_load.start()
    row_total = jnp.sum(total.T, axis=0, keepdims=True)
    squares[hx] = row_total

    ends = (z == 0).astype(jnp.int32) + (z == n - 1).astype(jnp.int32)
    pl.semaphore_wait(barrier, seq_n - 1 + heads_n - 1 + 2 - ends)

    sq_copies = []
    for d in range(1, heads_n):
        c = pltpu.make_async_remote_copy(
            src_ref=squares.at[hx],
            dst_ref=squares.at[hx],
            send_sem=sq_send.at[d - 1],
            recv_sem=sq_recv.at[d - 1],
            device_id={"head": lax.rem(hx + d, heads_n)},
            device_id_type=MESH,
        )
        c.start()
        sq_copies.append(c)

    for c in kv_loads:
        c.start()
    fresh_local = []
    for i, (src, dst, part) in enumerate(fresh_src):
        pltpu.make_async_copy(src, dst.at[sq, part], fresh_sem.at[i // 2]).start()
    for side, whole in enumerate((kf, vf)):
        fresh_local.append(pltpu.make_async_copy(whole.at[sq], whole.at[sq], fresh_sem.at[side]))

    edges = [0, ahead * HD, width] if ahead < hcount else [0, width]
    cuts = [slice(a, b) for a, b in zip(edges, edges[1:])]
    fresh_remote = [[] for _ in cuts]

    def fresh_wait(d, side, cols, k=0):
        whole = (kf, vf)[side].at[sq, :, :, cols]
        return pltpu.make_async_remote_copy(
            src_ref=whole,
            dst_ref=whole,
            send_sem=fresh_send.at[d - 1, side],
            recv_sem=fresh_recv.at[d - 1, k, side],
            device_id={"seq": lax.rem(sq + d, seq_n)},
            device_id_type=MESH,
        )

    for k, cols in enumerate(cuts):
        for d in range(1, seq_n):
            for i, (src, dst, part) in enumerate(fresh_src):
                pltpu.make_async_remote_copy(
                    src_ref=src.at[:, cols],
                    dst_ref=dst.at[sq, part, :, cols],
                    send_sem=fresh_send.at[d - 1, i // 2],
                    recv_sem=fresh_recv.at[d - 1, k, i // 2],
                    device_id={"seq": lax.rem(sq + d, seq_n)},
                    device_id_type=MESH,
                ).start()
            fresh_remote[k] += [fresh_wait(d, side, cols, k) for side in (0, 1)]

    gain_load.wait()

    def gain_step(h, carry):
        cols = pl.ds(pl.multiple_of(h * HD, HD), HD)
        qg[:, cols] = (q[:, cols].astype(F32) * gain[cols][None, :]).astype(BF16)
        return carry

    lax.fori_loop(0, hcount, gain_step, 0)
    tw_load.wait()
    if aligned:
        half = tw.shape[0] // 2
        j = lax.broadcasted_iota(jnp.int32, (half, HD), 0).astype(F32)
        frequency = jnp.exp(F32(-math.log(10000.0)) * j / half)
        phases = jnp.full((half, HD), step_ref[0], jnp.int32).astype(F32) * frequency
        cos, sin = jnp.cos(phases), jnp.sin(phases)
        for c in range(tw.shape[1] // HD):
            cols = slice(c * HD, (c + 1) * HD)
            terms = tw[:half, cols] * cos + tw[half:, cols] * sin
            gate[:, cols] = 1.0 + jnp.sum(terms, axis=0, keepdims=True)


    ring = min(chunks, LAG * (n - 1) + 1)

    def send(h, direction):
        if direction > 0:
            pairs, ss, rs = ((right_o, pre_o), (right_s, pre_s)), right_send, right_recv
        else:
            pairs, ss, rs = ((left_o, suf_o), (left_s, suf_s)), left_send, left_recv
        return [
            pltpu.make_async_remote_copy(
                src_ref=src.at[h],
                dst_ref=dst.at[h],
                send_sem=ss.at[i],
                recv_sem=rs.at[lax.rem(h, ring)],
                device_id={"slab": z + direction},
                device_id_type=MESH,
            )
            for i, (src, dst) in enumerate(pairs)
        ]

    def arrived(h, direction):
        ss, rs = (right_send, right_recv) if direction > 0 else (left_send, left_recv)
        pltpu.make_async_remote_copy(
            src_ref=gauge,
            dst_ref=gauge,
            send_sem=ss.at[0],
            recv_sem=rs.at[lax.rem(h, ring)],
            device_id={"slab": z - direction},
            device_id_type=MESH,
        ).wait_recv()

    def settle_sends(direction):
        if direction > 0:
            pairs, ss, rs = ((right_o, pre_o), (right_s, pre_s)), right_send, right_recv
        else:
            pairs, ss, rs = ((left_o, suf_o), (left_s, suf_s)), left_send, left_recv
        for i, (src, dst) in enumerate(pairs):
            pltpu.make_async_remote_copy(
                src_ref=src,
                dst_ref=dst,
                send_sem=ss.at[i],
                recv_sem=rs.at[0],
                device_id={"slab": z + direction},
                device_id_type=MESH,
            ).wait_send()

    pair = 2 if hcount % 2 == 0 else 1
    splits = next(k for k in (SPLIT, 2, 1) if hcount % k == 0)
    sub = HD // splits
    tuples = hcount // splits
    pairs = hcount // pair
    last = (groups - 1) * hcount
    fresh_rows = seq_n * 2 * fk_ref.shape[0]
    lag_end = LAG * jnp.maximum(z, n - 1 - z)

    def combine(h, other_o, other_s, dest_o, dest_s):
        l_a, l_b = own_s[h], other_s[h]
        top = jnp.maximum(l_a, l_b)
        e_a, e_b = jnp.exp2(l_a - top), jnp.exp2(l_b - top)
        mass = e_a + e_b
        share = 1.0 / mass
        dest_o[h] = (
            own_o[h] * (e_a * share) + other_o[h].astype(F32) * (e_b * share)
        ).astype(BF16)
        dest_s[h] = top + jnp.log2(mass)

    nt = (((1,), (1,)), ((), ()))
    tn = (((0,), (0,)), ((), ()))

    penalty = jnp.where(
        jnp.full((1, rows), owner_ref[0], jnp.int32) == z, F32(LOW), F32(0.0)
    )
    cached = kc.shape[0]
    step_keys = 256 if cached % 256 == 0 else cached
    blocks = [(i, i + step_keys) for i in range(0, cached, step_keys)]

    def head_cols(h):
        return pl.ds(pl.multiple_of(h * HD, HD), HD)

    def scores(h, slot):
        cols = head_cols(h)
        q_head = qg[:, cols]
        top = None
        for a, b in blocks:
            part = lax.dot_general(kc[a:b, cols], q_head, nt, preferred_element_type=F32)
            s_buf[slot, a:b, :] = part
            high = jnp.max(part, axis=0, keepdims=True)
            top = high if top is None else jnp.maximum(top, high)
        k_fresh = kf[:, :, :, cols].reshape(fresh_rows, HD)
        part = lax.dot_general(k_fresh, q_head, nt, preferred_element_type=F32)
        s_buf[slot, cached:, :] = part
        m_buf[slot, 0:1, :] = top
        m_buf[slot, 1:2, :] = jnp.max(part, axis=0, keepdims=True)

    def soften(slot, r=slice(None)):
        s_row = scale[0:1, r]
        mask = penalty[:, r]
        top = jnp.maximum(m_buf[slot, 0:1, r] * s_row + mask, m_buf[slot, 1:2, r] * s_row)
        top_c = top - mask
        mass = jnp.zeros_like(top)
        for a, b in blocks + [(cached, cached + fresh_rows)]:
            p = jnp.exp2(s_buf[slot, a:b, r] * s_row - (top_c if a < cached else top))
            p_buf[slot, a:b, r] = p.astype(BF16)
            mass = mass + jnp.sum(p, axis=0, keepdims=True)
        m_buf[slot, 2:3, r] = 1.0 / mass
        m_buf[slot, 3:4, r] = top + jnp.log2(mass)

    def place(g, h, seat, value, store):
        if g < groups - 1 or splits == 1:
            store(g * hcount + h, slice(0, HD), value)
            return
        lanes = slice(seat * sub, (seat + 1) * sub)
        for s in range(splits):
            source = value if s == seat else pltpu.roll(value, (seat - s) % splits * sub, 1)
            store(last + s * tuples + lax.div(h, splits), lanes, source[:, lanes])

    def weigh(h, slot, seat, first=0, end=None):
        cols = head_cols(h)
        end = groups if end is None else end
        r = slice(first * HD, end * HD)
        v_fresh = vf[:, :, :, cols].reshape(fresh_rows, HD)
        o = lax.dot_general(v_fresh, p_buf[slot, cached:, r], tn, preferred_element_type=F32)
        for a, b in blocks:
            o += lax.dot_general(
                vc[a:b, cols], p_buf[slot, a:b, r], tn, preferred_element_type=F32
            )

        o = o * m_buf[slot, 2:3, r]

        def store_o(c, lanes, value):
            own_o[c, :, lanes] = value

        def store_s(c, lanes, value):
            own_s[c, :, lanes] = value

        for g in range(first, end):
            place(g, h, seat, o[:, (g - first) * HD : (g - first + 1) * HD], store_o)
            place(g, h, seat, m_buf[slot, 3:4, g * HD : (g + 1) * HD], store_s)

    def project(g, p):
        deep = pl.ds(pl.multiple_of(p * pair * HD, HD), pair * HD)
        term = lax.dot_general(att[g, deep, :], w[deep, :], tn, preferred_element_type=F32)
        add(acc.at[g * HD : (g + 1) * HD, :], term, p)

    def project_last(s, p):
        deep = pl.ds(pl.multiple_of(p * splits * HD, HD), splits * HD)
        term = lax.dot_general(
            att[groups - 1 + s, deep, 0:sub], w[deep, :], tn, preferred_element_type=F32
        )
        add(acc.at[(groups - 1) * HD + s * sub : (groups - 1) * HD + (s + 1) * sub, :], term, p)

    def add(dest, term, p):
        @pl.when(p == 0)
        def _():
            dest[...] = term

        @pl.when(p > 0)
        def _():
            dest[...] += term

    pieces = [(g * HD, (g + 1) * HD) for g in range(groups - 1)]
    pieces += [((groups - 1) * HD + s * sub, (groups - 1) * HD + (s + 1) * sub) for s in range(splits)]

    def exchange(k):
        a, b = pieces[k]
        copies = []
        for d in range(1, heads_n):
            copies.append(
                pltpu.make_async_remote_copy(
                    src_ref=xs.at[d - 1, a:b],
                    dst_ref=xr.at[d - 1, a:b],
                    send_sem=x_send.at[d - 1],
                    recv_sem=x_recv.at[d - 1, k],
                    device_id={"head": lax.rem(hx + d, heads_n)},
                    device_id_type=MESH,
                )
            )
        return copies

    def exchange_start(k):
        a, b = pieces[k]
        cp = out_ref.shape[1]
        for d, c in enumerate(exchange(k)):
            peer = lax.rem(hx + d + 1, heads_n)
            cols = pl.ds(pl.multiple_of(peer * cp, HD), cp)
            xs[d, a:b] = acc[a:b, cols].astype(BF16)
            c.start()

    def service(t):
        cp_ = t - LAG * z
        in_p = (cp_ >= 0) & (cp_ < chunks)
        cs = t - LAG * (n - 1 - z)
        in_s = (cs >= 0) & (cs < chunks)

        @pl.when(in_p & (z > 0))
        def _():
            arrived(cp_, 1)

        @pl.when(in_p & (z < n - 1))
        def _():
            combine(cp_, pre_o, pre_s, right_o, right_s)
            for c in send(cp_, 1):
                c.start()

        @pl.when(in_s & (z < n - 1))
        def _():
            arrived(cs, -1)

        @pl.when(in_s & (z > 0))
        def _():
            combine(cs, suf_o, suf_s, left_o, left_s)
            for c in send(cs, -1):
                c.start()

    def finish(t):
        f = t - lag_end

        @pl.when((f >= 0) & (f < chunks))
        def _():
            m_a, m_b, m_c = own_s[f], pre_s[f], suf_s[f]
            top = jnp.maximum(m_a, jnp.maximum(m_b, m_c))
            e_a, e_b, e_c = jnp.exp2(m_a - top), jnp.exp2(m_b - top), jnp.exp2(m_c - top)
            share = 1.0 / (e_a + e_b + e_c)
            total_o = (
                own_o[f] * (e_a * share)
                + pre_o[f].astype(F32) * (e_b * share)
                + suf_o[f].astype(F32) * (e_c * share)
            )
            value = total_o.astype(BF16)

            @pl.when(f < last)
            def _():
                h = lax.rem(f, hcount)
                att[f // hcount, head_cols(h), :] = value

            @pl.when(f >= last)
            def _():
                k = f - last
                s, p = lax.div(k, tuples), lax.rem(k, tuples)
                for i in range(splits):
                    turned = value if i == 0 else pltpu.roll(total_o, HD - i * sub, 1).astype(BF16)
                    att[groups - 1 + s, head_cols(p * splits + i), :] = turned

        @pl.when(f == hcount - pairs)
        def _():
            w_load.wait()

        for g in range(groups - 1):
            begin = (g + 1) * hcount - pairs

            @pl.when((f >= begin) & (f < begin + pairs))
            def _(g=g, begin=begin):
                project(g, f - begin)

            if aligned:

                @pl.when(f == begin + pairs - 1)
                def _(g=g):
                    exchange_start(g)

        for s in range(splits):
            begin = last + s * tuples

            stop = begin + tuples - (1 if aligned and s == splits - 1 else 0)

            @pl.when((f >= begin) & (f < stop))
            def _(s=s, begin=begin):
                project_last(s, f - begin)

            if aligned and s < splits - 1:

                @pl.when(f == begin + tuples - 1)
                def _(s=s):
                    exchange_start(groups - 1 + s)

        if aligned:

            @pl.when(f == chunks - 1)
            def _():
                a, b = pieces[-1]
                cp = out_ref.shape[1]
                deep = slice((tuples - 1) * splits * HD, tuples * splits * HD)
                sums = att[groups + splits - 2, deep, 0:sub]

                def total_of(owner):
                    cols = pl.ds(pl.multiple_of(owner * cp, HD), cp)
                    before = 0.0 if tuples == 1 else acc[a:b, cols]
                    return cols, before + lax.dot_general(
                        sums, w[deep, cols], tn, preferred_element_type=F32
                    )

                for d, c in enumerate(exchange(len(pieces) - 1)):
                    xs[d, a:b] = total_of(lax.rem(hx + d + 1, heads_n))[1].astype(BF16)
                    c.start()
                cols, own = total_of(hx)
                acc[a:b, cols] = own

    def near(h):
        return jnp.minimum(h, hcount - 1)

    kv_loads[0].wait()
    for c in fresh_local:
        c.wait()
    for c in fresh_remote[0]:
        c.wait_recv()
    scores(0, 0)
    scores(min(1, hcount - 1), 1)
    for c in sq_copies:
        c.wait_recv()
    norm_total = jnp.sum(squares[...], axis=0)
    scale[...] = lax.rsqrt(norm_total / (HEADS * HD) + EPSILON) * (
        math.log2(math.e) / HD**0.5
    )
    soften(0, slice(0, HD))
    kv_loads[1].wait()
    weigh(0, 0, 0, 0, 1)
    service(0)
    w_load.start()
    if groups > 1:
        soften(0, slice(HD, rows))
        weigh(0, 0, 0, 1, groups)
    soften(1)
    scores(min(2, hcount - 1), 0)

    unroll = max(splits, 2)

    def body(i, carry):
        for u in range(unroll):
            t = unroll * i + u
            if len(cuts) > 1:

                @pl.when(t + 3 == ahead)
                def _():
                    for c in fresh_remote[1]:
                        c.wait_recv()
                    for c in kv_loads[2:]:
                        c.wait()

            @pl.when(t + 1 < hcount)
            def _(t=t, u=u):
                scores(near(t + 3), (u + 1) % 2)
                soften(u % 2)
                weigh(t + 1, (u + 1) % 2, (u + 1) % splits)

            finish(t)
            service(t + 1)
        return carry

    lax.fori_loop(0, -(-(chunks + LAG * (n - 1)) // unroll), body, 0)

    def settle():
        for d in range(1, seq_n):
            for side in (0, 1):
                fresh_wait(d, side, slice(0, width)).wait_send()
        for c in sq_copies:
            c.wait_send()

        @pl.when(z < n - 1)
        def _():
            settle_sends(1)

        @pl.when(z > 0)
        def _():
            settle_sends(-1)

    if aligned:
        cp = out_ref.shape[1]
        mine = pl.ds(pl.multiple_of(hx * cp, HD), cp)
        settle()
        for k, (a, b) in enumerate(pieces):
            summed = acc[a:b, mine]
            for d, c in enumerate(exchange(k)):
                c.wait_recv()
                summed = summed + xr[d, a:b].astype(F32)
            out_ref[a:b, :] = (summed * gate[...]).astype(out_ref.dtype)
        for d in range(1, heads_n):
            pltpu.make_async_remote_copy(
                src_ref=xs.at[d - 1],
                dst_ref=xr.at[d - 1],
                send_sem=x_send.at[d - 1],
                recv_sem=x_recv.at[d - 1, 0],
                device_id={"head": lax.rem(hx + d, heads_n)},
                device_id_type=MESH,
            ).wait_send()
    else:
        out_ref[...] = acc[...]
        settle()


def local(sizes, *args):
    (
        queries,
        query_gain,
        cache_keys,
        cache_values,
        finished_keys,
        finished_values,
        new_keys,
        new_values,
        out_weight,
        time_weight,
        owner,
        step,
    ) = args
    n, heads_n, seq_n = sizes
    rows, width = queries.shape
    hcount = width // HD
    cached, fresh = cache_keys.shape[0], finished_keys.shape[0]
    columns, cp = out_weight.shape[1], time_weight.shape[1]
    freq = time_weight.shape[0]
    aligned = cp % HD == 0
    any_spec = pl.BlockSpec(memory_space=pl.ANY)
    smem = pl.BlockSpec(memory_space=pltpu.SMEM)
    vmem = pl.BlockSpec(memory_space=pltpu.VMEM)
    dma = pltpu.SemaphoreType.DMA
    xcount = max(heads_n - 1, 1)
    groups = rows // HD
    chunks = groups * hcount
    ring = min(chunks, LAG * (n - 1) + 1)
    stat = (chunks, 1, HD)
    keys = cached + seq_n * 2 * fresh
    part = (chunks, HD, HD)
    result = pl.pallas_call(
        functools.partial(kernel, sizes, aligned),
        out_shape=pltpu.VMEM((rows, cp), BF16) if aligned else jax.ShapeDtypeStruct((rows, columns), F32),
        in_specs=[any_spec] * 10 + [smem] * 2,
        out_specs=vmem,
        scratch_shapes=[
            pltpu.VMEM((rows, width), BF16),
            pltpu.VMEM((rows, width), BF16),
            pltpu.VMEM((width,), F32),
            pltpu.VMEM((cached, width), BF16),
            pltpu.VMEM((cached, width), BF16),
            pltpu.VMEM((seq_n, 2, fresh, width), BF16),
            pltpu.VMEM((seq_n, 2, fresh, width), BF16),
            pltpu.VMEM((width, columns), BF16),
            pltpu.VMEM((freq, cp), F32),
            pltpu.VMEM((heads_n, 1, rows), F32),
            pltpu.VMEM((1, rows), F32),
            pltpu.VMEM(part, F32),
            pltpu.VMEM(stat, F32),
            pltpu.VMEM(part, BF16),
            pltpu.VMEM(stat, F32),
            pltpu.VMEM(part, BF16),
            pltpu.VMEM(stat, F32),
            pltpu.VMEM(part, BF16),
            pltpu.VMEM(stat, F32),
            pltpu.VMEM(part, BF16),
            pltpu.VMEM(stat, F32),
            pltpu.VMEM((groups + SPLIT - 1, width, HD), BF16),
            pltpu.VMEM((rows, columns), F32),
            pltpu.VMEM((1, cp), F32),
            pltpu.VMEM((xcount, rows, cp), BF16),
            pltpu.VMEM((xcount, rows, cp), BF16),
            dma((3,)),
            dma((2,)),
            dma((max(seq_n - 1, 1), 2)),
            dma((max(seq_n - 1, 1), 2, 2)),
            dma((xcount,)),
            dma((xcount,)),
            dma((2,)),
            dma((ring,)),
            dma((2,)),
            dma((ring,)),
            dma((xcount,)),
            dma((xcount, groups + SPLIT - 1)),
            pltpu.VMEM((2, keys, rows), F32),
            pltpu.VMEM((2, keys, rows), BF16),
            pltpu.VMEM((2, 4, rows), F32),
            dma((PARTS,)),
            dma((2, 2)),
            pltpu.VMEM((HD // 2 + 1, 1, HD), F32),
        ],
        compiler_params=pltpu.CompilerParams(
            collective_id=0, has_side_effects=True, vmem_limit_bytes=60 * 1024 * 1024
        ),
        name="sweep_attention",
    )(
        queries,
        query_gain,
        cache_keys,
        cache_values,
        finished_keys,
        finished_values,
        new_keys,
        new_values,
        out_weight,
        time_weight,
        owner,
        step,
    )
    if aligned:
        return result
    summed = lax.psum_scatter(result, "head", scatter_dimension=1, tiled=True)
    half = freq // 2
    frequency = jnp.exp(-jnp.log(10000.0) * jnp.arange(half, dtype=F32) / half)
    phases = step[0].astype(F32) * frequency
    embedding = jnp.concatenate([jnp.cos(phases), jnp.sin(phases)])
    time_gate = 1.0 + jnp.dot(embedding, time_weight, precision=lax.Precision.HIGHEST)
    return (time_gate * summed).astype(BF16)


def solution(mesh):
    in_specs = (
        P(("grp", "seq"), "head"),
        P("head"),
        P(("grp", "slab"), "head"),
        P(("grp", "slab"), "head"),
        P(("grp", "slab", "seq"), "head"),
        P(("grp", "slab", "seq"), "head"),
        P(("grp", "slab", "seq"), "head"),
        P(("grp", "slab", "seq"), "head"),
        P("head", "slab"),
        P(None, ("slab", "head")),
        P("grp"),
        P("grp"),
    )
    out_specs = P(("grp", "seq"), ("slab", "head"))
    sizes = (mesh.shape["slab"], mesh.shape["head"], mesh.shape["seq"])
    return jax.shard_map(
        functools.partial(local, sizes),
        mesh=mesh,
        in_specs=in_specs,
        out_specs=out_specs,
        check_vma=False,
    )
```

```python
import functools
import math

import jax
import jax.numpy as jnp
from jax import lax
from jax.experimental import pallas as pl
from jax.experimental.pallas import tpu as pltpu
from jax.sharding import PartitionSpec as P

HEADS = 40
HD = 128
EPSILON = 1e-06
LOW = -1e30
LAG = 5
SPLIT = 2
PARTS = 1
MESH = pl.DeviceIdType.MESH
F32 = jnp.float32
BF16 = jnp.bfloat16


def kernel(
    dims,
    aligned,
    q_ref,
    gain_ref,
    ck_ref,
    cv_ref,
    fk_ref,
    fv_ref,
    nk_ref,
    nv_ref,
    w_ref,
    tw_ref,
    owner_ref,
    step_ref,
    out_ref,
    q,
    qg,
    gain,
    kc,
    vc,
    kf,
    vf,
    w,
    tw,
    squares,
    scale,
    own_o,
    own_s,
    pre_o,
    pre_s,
    suf_o,
    suf_s,
    right_o,
    right_s,
    left_o,
    left_s,
    att,
    acc,
    gate,
    xs,
    xr,
    load_sem,
    fresh_sem,
    fresh_send,
    fresh_recv,
    sq_send,
    sq_recv,
    right_send,
    right_recv,
    left_send,
    left_recv,
    x_send,
    x_recv,
    s_buf,
    p_buf,
    m_buf,
    q_sem,
    kv_sem,
    gauge,
):
    n, heads_n, seq_n = dims
    rows, width = q_ref.shape
    hcount = width // HD
    z = lax.axis_index("slab")
    hx = lax.axis_index("head")
    sq = lax.axis_index("seq")

    groups = rows // HD
    chunks = groups * hcount
    gain_load, w_load, tw_load = [
        pltpu.make_async_copy(src, dst, load_sem.at[i])
        for i, (src, dst) in enumerate([(gain_ref, gain), (w_ref, w), (tw_ref, tw)])
    ]
    ahead = min(max(hcount // 5, 3), hcount)
    parts = PARTS if hcount % PARTS == 0 else 1
    span = width // parts
    q_loads = []
    for g in range(groups):
        for k in range(parts):
            at = (slice(g * HD, (g + 1) * HD), slice(k * span, (k + 1) * span))
            q_loads.append(
                pltpu.make_async_copy(q_ref.at[at], q.at[at], q_sem.at[g * parts + k])
            )
    for c in q_loads:
        c.start()
    gain_load.start()
    barrier = pltpu.get_barrier_semaphore()
    for d in range(1, seq_n):
        pl.semaphore_signal(
            barrier, inc=1, device_id={"seq": lax.rem(sq + d, seq_n)}, device_id_type=MESH
        )
    for d in range(1, heads_n):
        pl.semaphore_signal(
            barrier, inc=1, device_id={"head": lax.rem(hx + d, heads_n)}, device_id_type=MESH
        )

    @pl.when(z > 0)
    def _():
        pl.semaphore_signal(barrier, inc=1, device_id={"slab": z - 1}, device_id_type=MESH)

    @pl.when(z < n - 1)
    def _():
        pl.semaphore_signal(barrier, inc=1, device_id={"slab": z + 1}, device_id_type=MESH)

    def clear(o_ref, s_ref):
        o_ref[...] = jnp.zeros_like(o_ref)
        s_ref[...] = jnp.full((chunks, 1, HD), LOW, F32)

    @pl.when(z == 0)
    def _():
        clear(pre_o, pre_s)

    @pl.when(z == n - 1)
    def _():
        clear(suf_o, suf_s)

    def squares_of(g):
        def step(h, total):
            x = q[g * HD : (g + 1) * HD, pl.ds(pl.multiple_of(h * HD, HD), HD)].astype(F32)
            return total + x * x

        total = jnp.zeros((HD, HD), F32)
        for k in range(parts):
            q_loads[g * parts + k].wait()
            total = lax.fori_loop(
                k * hcount // parts, (k + 1) * hcount // parts, step, total, unroll=True
            )
        squares[hx, g] = jnp.sum(total.T, axis=0, keepdims=True)

    squares_of(0)
    head_cut = ahead * HD
    kv_cuts = [slice(0, head_cut), slice(head_cut, width)] if head_cut < width else [slice(0, width)]
    kv_loads = []
    for k, cols in enumerate(kv_cuts):
        for i, (src, dst) in enumerate([(ck_ref, kc), (cv_ref, vc)]):
            kv_loads.append(pltpu.make_async_copy(src.at[:, cols], dst.at[:, cols], kv_sem.at[k, i]))
    fresh_src = [(fk_ref, kf, 0), (nk_ref, kf, 1), (fv_ref, vf, 0), (nv_ref, vf, 1)]

    ends = (z == 0).astype(jnp.int32) + (z == n - 1).astype(jnp.int32)
    pl.semaphore_wait(barrier, seq_n - 1 + heads_n - 1 + 2 - ends)

    sq_copies = []

    def squares_send(g):
        copies = []
        for d in range(1, heads_n):
            c = pltpu.make_async_remote_copy(
                src_ref=squares.at[hx, g],
                dst_ref=squares.at[hx, g],
                send_sem=sq_send.at[d - 1, g],
                recv_sem=sq_recv.at[d - 1, g],
                device_id={"head": lax.rem(hx + d, heads_n)},
                device_id_type=MESH,
            )
            c.start()
            copies.append(c)
        sq_copies.append(copies)

    squares_send(0)
    for c in kv_loads[:2]:
        c.start()
    for g in range(1, groups):
        squares_of(g)
        squares_send(g)
    tw_load.start()
    for c in kv_loads[2:]:
        c.start()
    fresh_local = []
    for i, (src, dst, part) in enumerate(fresh_src):
        pltpu.make_async_copy(src, dst.at[sq, part], fresh_sem.at[i // 2]).start()
    for side, whole in enumerate((kf, vf)):
        fresh_local.append(pltpu.make_async_copy(whole.at[sq], whole.at[sq], fresh_sem.at[side]))

    edges = [0, ahead * HD, width] if ahead < hcount else [0, width]
    cuts = [slice(a, b) for a, b in zip(edges, edges[1:])]
    fresh_remote = [[] for _ in cuts]

    def fresh_wait(d, side, cols, k=0):
        whole = (kf, vf)[side].at[sq, :, :, cols]
        return pltpu.make_async_remote_copy(
            src_ref=whole,
            dst_ref=whole,
            send_sem=fresh_send.at[d - 1, side],
            recv_sem=fresh_recv.at[d - 1, k, side],
            device_id={"seq": lax.rem(sq + d, seq_n)},
            device_id_type=MESH,
        )

    for k, cols in enumerate(cuts):
        for d in range(1, seq_n):
            for i, (src, dst, part) in enumerate(fresh_src):
                pltpu.make_async_remote_copy(
                    src_ref=src.at[:, cols],
                    dst_ref=dst.at[sq, part, :, cols],
                    send_sem=fresh_send.at[d - 1, i // 2],
                    recv_sem=fresh_recv.at[d - 1, k, i // 2],
                    device_id={"seq": lax.rem(sq + d, seq_n)},
                    device_id_type=MESH,
                ).start()
            fresh_remote[k] += [fresh_wait(d, side, cols, k) for side in (0, 1)]

    gain_load.wait()

    def gain_step(h, carry):
        cols = pl.ds(pl.multiple_of(h * HD, HD), HD)
        qg[:, cols] = (q[:, cols].astype(F32) * gain[cols][None, :]).astype(BF16)
        return carry

    lax.fori_loop(0, hcount, gain_step, 0)
    tw_load.wait()
    if aligned:
        half = tw.shape[0] // 2
        j = lax.broadcasted_iota(jnp.int32, (half, HD), 0).astype(F32)
        frequency = jnp.exp(F32(-math.log(10000.0)) * j / half)
        phases = jnp.full((half, HD), step_ref[0], jnp.int32).astype(F32) * frequency
        cos, sin = jnp.cos(phases), jnp.sin(phases)
        for c in range(tw.shape[1] // HD):
            cols = slice(c * HD, (c + 1) * HD)
            terms = tw[:half, cols] * cos + tw[half:, cols] * sin
            gate[:, cols] = 1.0 + jnp.sum(terms, axis=0, keepdims=True)


    ring = min(chunks, LAG * (n - 1) + 1)

    def send(h, direction):
        if direction > 0:
            pairs, ss, rs = ((right_o, pre_o), (right_s, pre_s)), right_send, right_recv
        else:
            pairs, ss, rs = ((left_o, suf_o), (left_s, suf_s)), left_send, left_recv
        return [
            pltpu.make_async_remote_copy(
                src_ref=src.at[h],
                dst_ref=dst.at[h],
                send_sem=ss.at[i],
                recv_sem=rs.at[lax.rem(h, ring)],
                device_id={"slab": z + direction},
                device_id_type=MESH,
            )
            for i, (src, dst) in enumerate(pairs)
        ]

    def arrived(h, direction):
        ss, rs = (right_send, right_recv) if direction > 0 else (left_send, left_recv)
        pltpu.make_async_remote_copy(
            src_ref=gauge,
            dst_ref=gauge,
            send_sem=ss.at[0],
            recv_sem=rs.at[lax.rem(h, ring)],
            device_id={"slab": z - direction},
            device_id_type=MESH,
        ).wait_recv()

    def settle_sends(direction):
        if direction > 0:
            pairs, ss, rs = ((right_o, pre_o), (right_s, pre_s)), right_send, right_recv
        else:
            pairs, ss, rs = ((left_o, suf_o), (left_s, suf_s)), left_send, left_recv
        for i, (src, dst) in enumerate(pairs):
            pltpu.make_async_remote_copy(
                src_ref=src,
                dst_ref=dst,
                send_sem=ss.at[i],
                recv_sem=rs.at[0],
                device_id={"slab": z + direction},
                device_id_type=MESH,
            ).wait_send()

    pair = 2 if hcount % 2 == 0 else 1
    splits = next(k for k in (SPLIT, 2, 1) if hcount % k == 0)
    sub = HD // splits
    tuples = hcount // splits
    pairs = hcount // pair
    last = (groups - 1) * hcount
    fresh_rows = seq_n * 2 * fk_ref.shape[0]
    lag_end = LAG * jnp.maximum(z, n - 1 - z)

    def combine(h, other_o, other_s, dest_o, dest_s):
        l_a, l_b = own_s[h], other_s[h]
        top = jnp.maximum(l_a, l_b)
        e_a, e_b = jnp.exp2(l_a - top), jnp.exp2(l_b - top)
        mass = e_a + e_b
        share = 1.0 / mass
        dest_o[h] = (
            own_o[h] * (e_a * share) + other_o[h].astype(F32) * (e_b * share)
        ).astype(BF16)
        dest_s[h] = top + jnp.log2(mass)

    nt = (((1,), (1,)), ((), ()))
    tn = (((0,), (0,)), ((), ()))

    penalty = jnp.where(
        jnp.full((1, rows), owner_ref[0], jnp.int32) == z, F32(LOW), F32(0.0)
    )
    cached = kc.shape[0]
    step_keys = 256 if cached % 256 == 0 else cached
    blocks = [(i, i + step_keys) for i in range(0, cached, step_keys)]

    def head_cols(h):
        return pl.ds(pl.multiple_of(h * HD, HD), HD)

    def scores(h, slot):
        cols = head_cols(h)
        q_head = qg[:, cols]
        top = None
        for a, b in blocks:
            part = lax.dot_general(kc[a:b, cols], q_head, nt, preferred_element_type=F32)
            s_buf[slot, a:b, :] = part
            high = jnp.max(part, axis=0, keepdims=True)
            top = high if top is None else jnp.maximum(top, high)
        k_fresh = kf[:, :, :, cols].reshape(fresh_rows, HD)
        part = lax.dot_general(k_fresh, q_head, nt, preferred_element_type=F32)
        s_buf[slot, cached:, :] = part
        m_buf[slot, 0:1, :] = top
        m_buf[slot, 1:2, :] = jnp.max(part, axis=0, keepdims=True)

    def soften(slot, r=slice(None)):
        s_row = scale[0:1, r]
        mask = penalty[:, r]
        top = jnp.maximum(m_buf[slot, 0:1, r] * s_row + mask, m_buf[slot, 1:2, r] * s_row)
        top_c = top - mask
        mass = jnp.zeros_like(top)
        for a, b in blocks + [(cached, cached + fresh_rows)]:
            p = jnp.exp2(s_buf[slot, a:b, r] * s_row - (top_c if a < cached else top))
            p_buf[slot, a:b, r] = p.astype(BF16)
            mass = mass + jnp.sum(p, axis=0, keepdims=True)
        m_buf[slot, 2:3, r] = 1.0 / mass
        m_buf[slot, 3:4, r] = top + jnp.log2(mass)

    def place(g, h, seat, value, store):
        if g < groups - 1 or splits == 1:
            store(g * hcount + h, slice(0, HD), value)
            return
        lanes = slice(seat * sub, (seat + 1) * sub)
        for s in range(splits):
            source = value if s == seat else pltpu.roll(value, (seat - s) % splits * sub, 1)
            store(last + s * tuples + lax.div(h, splits), lanes, source[:, lanes])

    def weigh(h, slot, seat, first=0, end=None):
        cols = head_cols(h)
        end = groups if end is None else end
        r = slice(first * HD, end * HD)
        v_fresh = vf[:, :, :, cols].reshape(fresh_rows, HD)
        o = lax.dot_general(v_fresh, p_buf[slot, cached:, r], tn, preferred_element_type=F32)
        for a, b in blocks:
            o += lax.dot_general(
                vc[a:b, cols], p_buf[slot, a:b, r], tn, preferred_element_type=F32
            )

        o = o * m_buf[slot, 2:3, r]

        def store_o(c, lanes, value):
            own_o[c, :, lanes] = value

        def store_s(c, lanes, value):
            own_s[c, :, lanes] = value

        for g in range(first, end):
            place(g, h, seat, o[:, (g - first) * HD : (g - first + 1) * HD], store_o)
            place(g, h, seat, m_buf[slot, 3:4, g * HD : (g + 1) * HD], store_s)

    def project(g, p):
        deep = pl.ds(pl.multiple_of(p * pair * HD, HD), pair * HD)
        term = lax.dot_general(att[g, deep, :], w[deep, :], tn, preferred_element_type=F32)
        add(acc.at[g * HD : (g + 1) * HD, :], term, p)

    def project_last(s, p):
        deep = pl.ds(pl.multiple_of(p * splits * HD, HD), splits * HD)
        term = lax.dot_general(
            att[groups - 1 + s, deep, 0:sub], w[deep, :], tn, preferred_element_type=F32
        )
        add(acc.at[(groups - 1) * HD + s * sub : (groups - 1) * HD + (s + 1) * sub, :], term, p)

    def add(dest, term, p):
        @pl.when(p == 0)
        def _():
            dest[...] = term

        @pl.when(p > 0)
        def _():
            dest[...] += term

    pieces = [(g * HD, (g + 1) * HD) for g in range(groups - 1)]
    pieces += [((groups - 1) * HD + s * sub, (groups - 1) * HD + (s + 1) * sub) for s in range(splits)]

    def exchange(k):
        a, b = pieces[k]
        copies = []
        for d in range(1, heads_n):
            copies.append(
                pltpu.make_async_remote_copy(
                    src_ref=xs.at[d - 1, a:b],
                    dst_ref=xr.at[d - 1, a:b],
                    send_sem=x_send.at[d - 1],
                    recv_sem=x_recv.at[d - 1, k],
                    device_id={"head": lax.rem(hx + d, heads_n)},
                    device_id_type=MESH,
                )
            )
        return copies

    def exchange_start(k):
        a, b = pieces[k]
        cp = out_ref.shape[1]
        for d, c in enumerate(exchange(k)):
            peer = lax.rem(hx + d + 1, heads_n)
            cols = pl.ds(pl.multiple_of(peer * cp, HD), cp)
            xs[d, a:b] = acc[a:b, cols].astype(BF16)
            c.start()

    def service(t):
        cp_ = t - LAG * z
        in_p = (cp_ >= 0) & (cp_ < chunks)
        cs = t - LAG * (n - 1 - z)
        in_s = (cs >= 0) & (cs < chunks)

        @pl.when(in_p & (z > 0))
        def _():
            arrived(cp_, 1)

        @pl.when(in_p & (z < n - 1))
        def _():
            combine(cp_, pre_o, pre_s, right_o, right_s)
            for c in send(cp_, 1):
                c.start()

        @pl.when(in_s & (z < n - 1))
        def _():
            arrived(cs, -1)

        @pl.when(in_s & (z > 0))
        def _():
            combine(cs, suf_o, suf_s, left_o, left_s)
            for c in send(cs, -1):
                c.start()

    def finish(t):
        f = t - lag_end

        @pl.when((f >= 0) & (f < chunks))
        def _():
            m_a, m_b, m_c = own_s[f], pre_s[f], suf_s[f]
            top = jnp.maximum(m_a, jnp.maximum(m_b, m_c))
            e_a, e_b, e_c = jnp.exp2(m_a - top), jnp.exp2(m_b - top), jnp.exp2(m_c - top)
            share = 1.0 / (e_a + e_b + e_c)
            total_o = (
                own_o[f] * (e_a * share)
                + pre_o[f].astype(F32) * (e_b * share)
                + suf_o[f].astype(F32) * (e_c * share)
            )
            value = total_o.astype(BF16)

            @pl.when(f < last)
            def _():
                h = lax.rem(f, hcount)
                att[f // hcount, head_cols(h), :] = value

            @pl.when(f >= last)
            def _():
                k = f - last
                s, p = lax.div(k, tuples), lax.rem(k, tuples)
                for i in range(splits):
                    turned = value if i == 0 else pltpu.roll(total_o, HD - i * sub, 1).astype(BF16)
                    att[groups - 1 + s, head_cols(p * splits + i), :] = turned

        @pl.when(f == hcount - pairs)
        def _():
            w_load.wait()

        for g in range(groups - 1):
            begin = (g + 1) * hcount - pairs

            @pl.when((f >= begin) & (f < begin + pairs))
            def _(g=g, begin=begin):
                project(g, f - begin)

            if aligned:

                @pl.when(f == begin + pairs - 1)
                def _(g=g):
                    exchange_start(g)

        for s in range(splits):
            begin = last + s * tuples

            stop = begin + tuples - (1 if aligned and s == splits - 1 else 0)

            @pl.when((f >= begin) & (f < stop))
            def _(s=s, begin=begin):
                project_last(s, f - begin)

            if aligned and s < splits - 1:

                @pl.when(f == begin + tuples - 1)
                def _(s=s):
                    exchange_start(groups - 1 + s)

        if aligned:

            @pl.when(f == chunks - 1)
            def _():
                a, b = pieces[-1]
                cp = out_ref.shape[1]
                deep = slice((tuples - 1) * splits * HD, tuples * splits * HD)
                sums = att[groups + splits - 2, deep, 0:sub]

                def total_of(owner):
                    cols = pl.ds(pl.multiple_of(owner * cp, HD), cp)
                    before = 0.0 if tuples == 1 else acc[a:b, cols]
                    return cols, before + lax.dot_general(
                        sums, w[deep, cols], tn, preferred_element_type=F32
                    )

                for d, c in enumerate(exchange(len(pieces) - 1)):
                    xs[d, a:b] = total_of(lax.rem(hx + d + 1, heads_n))[1].astype(BF16)
                    c.start()
                cols, own = total_of(hx)
                acc[a:b, cols] = own

    def near(h):
        return jnp.minimum(h, hcount - 1)

    kv_loads[0].wait()
    for c in fresh_local:
        c.wait()
    for c in fresh_remote[0]:
        c.wait_recv()
    scores(0, 0)
    scores(min(1, hcount - 1), 1)
    def rescale(g):
        for c in sq_copies[g]:
            c.wait_recv()
        norm_total = squares[0, g]
        for d in range(1, heads_n):
            norm_total = norm_total + squares[d, g]
        scale[0:1, g * HD : (g + 1) * HD] = lax.rsqrt(norm_total / (HEADS * HD) + EPSILON) * (
            math.log2(math.e) / HD**0.5
        )

    rescale(0)
    soften(0, slice(0, HD))
    kv_loads[1].wait()
    weigh(0, 0, 0, 0, 1)
    service(0)
    w_load.start()
    for g in range(1, groups):
        rescale(g)
    if groups > 1:
        soften(0, slice(HD, rows))
        weigh(0, 0, 0, 1, groups)
    soften(1)
    scores(min(2, hcount - 1), 0)

    unroll = max(splits, 2)

    def body(i, carry):
        for u in range(unroll):
            t = unroll * i + u
            if len(cuts) > 1:

                @pl.when(t + 3 == ahead)
                def _():
                    for c in fresh_remote[1]:
                        c.wait_recv()
                    for c in kv_loads[2:]:
                        c.wait()

            @pl.when(t + 1 < hcount)
            def _(t=t, u=u):
                scores(near(t + 3), (u + 1) % 2)
                soften(u % 2)
                weigh(t + 1, (u + 1) % 2, (u + 1) % splits)

            finish(t)
            service(t + 1)
        return carry

    lax.fori_loop(0, -(-(chunks + LAG * (n - 1)) // unroll), body, 0)

    def settle():
        for d in range(1, seq_n):
            for side in (0, 1):
                fresh_wait(d, side, slice(0, width)).wait_send()
        for c in [c for copies in sq_copies for c in copies]:
            c.wait_send()

        @pl.when(z < n - 1)
        def _():
            settle_sends(1)

        @pl.when(z > 0)
        def _():
            settle_sends(-1)

    if aligned:
        cp = out_ref.shape[1]
        mine = pl.ds(pl.multiple_of(hx * cp, HD), cp)
        settle()
        for k, (a, b) in enumerate(pieces):
            summed = acc[a:b, mine]
            for d, c in enumerate(exchange(k)):
                c.wait_recv()
                summed = summed + xr[d, a:b].astype(F32)
            out_ref[a:b, :] = (summed * gate[...]).astype(out_ref.dtype)
        for d in range(1, heads_n):
            pltpu.make_async_remote_copy(
                src_ref=xs.at[d - 1],
                dst_ref=xr.at[d - 1],
                send_sem=x_send.at[d - 1],
                recv_sem=x_recv.at[d - 1, 0],
                device_id={"head": lax.rem(hx + d, heads_n)},
                device_id_type=MESH,
            ).wait_send()
    else:
        out_ref[...] = acc[...]
        settle()


def local(sizes, *args):
    (
        queries,
        query_gain,
        cache_keys,
        cache_values,
        finished_keys,
        finished_values,
        new_keys,
        new_values,
        out_weight,
        time_weight,
        owner,
        step,
    ) = args
    n, heads_n, seq_n = sizes
    rows, width = queries.shape
    hcount = width // HD
    cached, fresh = cache_keys.shape[0], finished_keys.shape[0]
    columns, cp = out_weight.shape[1], time_weight.shape[1]
    freq = time_weight.shape[0]
    aligned = cp % HD == 0
    any_spec = pl.BlockSpec(memory_space=pl.ANY)
    smem = pl.BlockSpec(memory_space=pltpu.SMEM)
    vmem = pl.BlockSpec(memory_space=pltpu.VMEM)
    dma = pltpu.SemaphoreType.DMA
    xcount = max(heads_n - 1, 1)
    groups = rows // HD
    chunks = groups * hcount
    ring = min(chunks, LAG * (n - 1) + 1)
    stat = (chunks, 1, HD)
    keys = cached + seq_n * 2 * fresh
    part = (chunks, HD, HD)
    result = pl.pallas_call(
        functools.partial(kernel, sizes, aligned),
        out_shape=pltpu.VMEM((rows, cp), BF16) if aligned else jax.ShapeDtypeStruct((rows, columns), F32),
        in_specs=[any_spec] * 10 + [smem] * 2,
        out_specs=vmem,
        scratch_shapes=[
            pltpu.VMEM((rows, width), BF16),
            pltpu.VMEM((rows, width), BF16),
            pltpu.VMEM((width,), F32),
            pltpu.VMEM((cached, width), BF16),
            pltpu.VMEM((cached, width), BF16),
            pltpu.VMEM((seq_n, 2, fresh, width), BF16),
            pltpu.VMEM((seq_n, 2, fresh, width), BF16),
            pltpu.VMEM((width, columns), BF16),
            pltpu.VMEM((freq, cp), F32),
            pltpu.VMEM((heads_n, groups, 1, HD), F32),
            pltpu.VMEM((1, rows), F32),
            pltpu.VMEM(part, F32),
            pltpu.VMEM(stat, F32),
            pltpu.VMEM(part, BF16),
            pltpu.VMEM(stat, F32),
            pltpu.VMEM(part, BF16),
            pltpu.VMEM(stat, F32),
            pltpu.VMEM(part, BF16),
            pltpu.VMEM(stat, F32),
            pltpu.VMEM(part, BF16),
            pltpu.VMEM(stat, F32),
            pltpu.VMEM((groups + SPLIT - 1, width, HD), BF16),
            pltpu.VMEM((rows, columns), F32),
            pltpu.VMEM((1, cp), F32),
            pltpu.VMEM((xcount, rows, cp), BF16),
            pltpu.VMEM((xcount, rows, cp), BF16),
            dma((3,)),
            dma((2,)),
            dma((max(seq_n - 1, 1), 2)),
            dma((max(seq_n - 1, 1), 2, 2)),
            dma((xcount, groups)),
            dma((xcount, groups)),
            dma((2,)),
            dma((ring,)),
            dma((2,)),
            dma((ring,)),
            dma((xcount,)),
            dma((xcount, groups + SPLIT - 1)),
            pltpu.VMEM((2, keys, rows), F32),
            pltpu.VMEM((2, keys, rows), BF16),
            pltpu.VMEM((2, 4, rows), F32),
            dma((groups * PARTS,)),
            dma((2, 2)),
            pltpu.VMEM((HD // 2 + 1, 1, HD), F32),
        ],
        compiler_params=pltpu.CompilerParams(
            collective_id=0, has_side_effects=True, vmem_limit_bytes=60 * 1024 * 1024
        ),
        name="sweep_attention",
    )(
        queries,
        query_gain,
        cache_keys,
        cache_values,
        finished_keys,
        finished_values,
        new_keys,
        new_values,
        out_weight,
        time_weight,
        owner,
        step,
    )
    if aligned:
        return result
    summed = lax.psum_scatter(result, "head", scatter_dimension=1, tiled=True)
    half = freq // 2
    frequency = jnp.exp(-jnp.log(10000.0) * jnp.arange(half, dtype=F32) / half)
    phases = step[0].astype(F32) * frequency
    embedding = jnp.concatenate([jnp.cos(phases), jnp.sin(phases)])
    time_gate = 1.0 + jnp.dot(embedding, time_weight, precision=lax.Precision.HIGHEST)
    return (time_gate * summed).astype(BF16)


def solution(mesh):
    in_specs = (
        P(("grp", "seq"), "head"),
        P("head"),
        P(("grp", "slab"), "head"),
        P(("grp", "slab"), "head"),
        P(("grp", "slab", "seq"), "head"),
        P(("grp", "slab", "seq"), "head"),
        P(("grp", "slab", "seq"), "head"),
        P(("grp", "slab", "seq"), "head"),
        P("head", "slab"),
        P(None, ("slab", "head")),
        P("grp"),
        P("grp"),
    )
    out_specs = P(("grp", "seq"), ("slab", "head"))
    sizes = (mesh.shape["slab"], mesh.shape["head"], mesh.shape["seq"])
    return jax.shard_map(
        functools.partial(local, sizes),
        mesh=mesh,
        in_specs=in_specs,
        out_specs=out_specs,
        check_vma=False,
    )
```

```python
import functools
import math

import jax
import jax.numpy as jnp
from jax import lax
from jax.experimental import pallas as pl
from jax.experimental.pallas import tpu as pltpu
from jax.sharding import PartitionSpec as P

HEADS = 40
HD = 128
EPSILON = 1e-06
LOW = -1e30
LAG = 5
SPLIT = 2
PARTS = 1
MESH = pl.DeviceIdType.MESH
F32 = jnp.float32
BF16 = jnp.bfloat16


def kernel(
    dims,
    aligned,
    q_ref,
    gain_ref,
    ck_ref,
    cv_ref,
    fk_ref,
    fv_ref,
    nk_ref,
    nv_ref,
    w_ref,
    tw_ref,
    owner_hbm,
    step_hbm,
    out_ref,
    q,
    qg,
    gain,
    kc,
    vc,
    kf,
    vf,
    w,
    tw,
    squares,
    scale,
    own_o,
    own_s,
    pre_o,
    pre_s,
    suf_o,
    suf_s,
    right_o,
    right_s,
    left_o,
    left_s,
    att,
    acc,
    gate,
    xs,
    xr,
    load_sem,
    fresh_sem,
    fresh_send,
    fresh_recv,
    sq_send,
    sq_recv,
    right_send,
    right_recv,
    left_send,
    left_recv,
    x_send,
    x_recv,
    s_buf,
    p_buf,
    m_buf,
    q_sem,
    kv_sem,
    gauge,
    raw_o,
    raw_s,
    owner_ref,
    step_ref,
    scalar_sem,
):
    n, heads_n, seq_n = dims
    rows, width = q_ref.shape
    hcount = width // HD
    z = lax.axis_index("slab")
    hx = lax.axis_index("head")
    sq = lax.axis_index("seq")

    groups = rows // HD
    chunks = groups * hcount
    gain_load, w_load, tw_load = [
        pltpu.make_async_copy(src, dst, load_sem.at[i])
        for i, (src, dst) in enumerate([(gain_ref, gain), (w_ref, w), (tw_ref, tw)])
    ]
    ahead = min(max(hcount // 5, 3), hcount)
    parts = PARTS if hcount % PARTS == 0 else 1
    span = width // parts
    q_loads = []
    for g in range(groups):
        for k in range(parts):
            at = (slice(g * HD, (g + 1) * HD), slice(k * span, (k + 1) * span))
            q_loads.append(
                pltpu.make_async_copy(q_ref.at[at], q.at[at], q_sem.at[g * parts + k])
            )
    for c in q_loads:
        c.start()
    gain_load.start()
    scalars = [
        pltpu.make_async_copy(owner_hbm, owner_ref, scalar_sem.at[0]),
        pltpu.make_async_copy(step_hbm, step_ref, scalar_sem.at[1]),
    ]
    for c in scalars:
        c.start()
    barrier = pltpu.get_barrier_semaphore()
    for d in range(1, seq_n):
        pl.semaphore_signal(
            barrier, inc=1, device_id={"seq": lax.rem(sq + d, seq_n)}, device_id_type=MESH
        )
    for d in range(1, heads_n):
        pl.semaphore_signal(
            barrier, inc=1, device_id={"head": lax.rem(hx + d, heads_n)}, device_id_type=MESH
        )

    @pl.when(z > 0)
    def _():
        pl.semaphore_signal(barrier, inc=1, device_id={"slab": z - 1}, device_id_type=MESH)

    @pl.when(z < n - 1)
    def _():
        pl.semaphore_signal(barrier, inc=1, device_id={"slab": z + 1}, device_id_type=MESH)

    def clear(o_ref, s_ref):
        o_ref[...] = jnp.zeros_like(o_ref)
        s_ref[...] = jnp.full((chunks, 1, HD), LOW, F32)

    @pl.when(z == 0)
    def _():
        clear(pre_o, pre_s)

    @pl.when(z == n - 1)
    def _():
        clear(suf_o, suf_s)

    def squares_of(g):
        def step(h, total):
            x = q[g * HD : (g + 1) * HD, pl.ds(pl.multiple_of(h * HD, HD), HD)].astype(F32)
            return total + x * x

        total = jnp.zeros((HD, HD), F32)
        for k in range(parts):
            q_loads[g * parts + k].wait()
            total = lax.fori_loop(
                k * hcount // parts, (k + 1) * hcount // parts, step, total, unroll=True
            )
        squares[hx, g] = jnp.sum(total.T, axis=0, keepdims=True)

    squares_of(0)
    head_cut = ahead * HD
    kv_cuts = [slice(0, head_cut), slice(head_cut, width)] if head_cut < width else [slice(0, width)]
    kv_loads = []
    for k, cols in enumerate(kv_cuts):
        for i, (src, dst) in enumerate([(ck_ref, kc), (cv_ref, vc)]):
            kv_loads.append(pltpu.make_async_copy(src.at[:, cols], dst.at[:, cols], kv_sem.at[k, i]))
    fresh_src = [(fk_ref, kf, 0), (nk_ref, kf, 1), (fv_ref, vf, 0), (nv_ref, vf, 1)]

    ends = (z == 0).astype(jnp.int32) + (z == n - 1).astype(jnp.int32)
    pl.semaphore_wait(barrier, seq_n - 1 + heads_n - 1 + 2 - ends)

    sq_copies = []

    def squares_send(g):
        copies = []
        for d in range(1, heads_n):
            c = pltpu.make_async_remote_copy(
                src_ref=squares.at[hx, g],
                dst_ref=squares.at[hx, g],
                send_sem=sq_send.at[d - 1, g],
                recv_sem=sq_recv.at[d - 1, g],
                device_id={"head": lax.rem(hx + d, heads_n)},
                device_id_type=MESH,
            )
            c.start()
            copies.append(c)
        sq_copies.append(copies)

    squares_send(0)
    for c in kv_loads[:2]:
        c.start()
    for g in range(1, groups):
        squares_of(g)
        squares_send(g)
    tw_load.start()
    for c in kv_loads[2:]:
        c.start()
    fresh_local = []
    for i, (src, dst, part) in enumerate(fresh_src):
        pltpu.make_async_copy(src, dst.at[sq, part], fresh_sem.at[i // 2]).start()
    for side, whole in enumerate((kf, vf)):
        fresh_local.append(pltpu.make_async_copy(whole.at[sq], whole.at[sq], fresh_sem.at[side]))

    edges = [0, ahead * HD, width] if ahead < hcount else [0, width]
    cuts = [slice(a, b) for a, b in zip(edges, edges[1:])]
    fresh_remote = [[] for _ in cuts]

    def fresh_wait(d, side, cols, k=0):
        whole = (kf, vf)[side].at[sq, :, :, cols]
        return pltpu.make_async_remote_copy(
            src_ref=whole,
            dst_ref=whole,
            send_sem=fresh_send.at[d - 1, side],
            recv_sem=fresh_recv.at[d - 1, k, side],
            device_id={"seq": lax.rem(sq + d, seq_n)},
            device_id_type=MESH,
        )

    for k, cols in enumerate(cuts):
        for d in range(1, seq_n):
            for i, (src, dst, part) in enumerate(fresh_src):
                pltpu.make_async_remote_copy(
                    src_ref=src.at[:, cols],
                    dst_ref=dst.at[sq, part, :, cols],
                    send_sem=fresh_send.at[d - 1, i // 2],
                    recv_sem=fresh_recv.at[d - 1, k, i // 2],
                    device_id={"seq": lax.rem(sq + d, seq_n)},
                    device_id_type=MESH,
                ).start()
            fresh_remote[k] += [fresh_wait(d, side, cols, k) for side in (0, 1)]

    gain_load.wait()

    def gain_step(h, carry):
        cols = pl.ds(pl.multiple_of(h * HD, HD), HD)
        qg[:, cols] = (q[:, cols].astype(F32) * gain[cols][None, :]).astype(BF16)
        return carry

    lax.fori_loop(0, hcount, gain_step, 0)
    tw_load.wait()
    for c in scalars:
        c.wait()
    if aligned:
        half = tw.shape[0] // 2
        j = lax.broadcasted_iota(jnp.int32, (half, HD), 0).astype(F32)
        frequency = jnp.exp(F32(-math.log(10000.0)) * j / half)
        phases = jnp.full((half, HD), step_ref[0, 0], jnp.int32).astype(F32) * frequency
        cos, sin = jnp.cos(phases), jnp.sin(phases)
        for c in range(tw.shape[1] // HD):
            cols = slice(c * HD, (c + 1) * HD)
            terms = tw[:half, cols] * cos + tw[half:, cols] * sin
            gate[:, cols] = 1.0 + jnp.sum(terms, axis=0, keepdims=True)


    ring = min(chunks, LAG * (n - 1) + 1)

    def send(h, direction):
        if direction > 0:
            pairs, ss, rs = ((right_o, pre_o), (right_s, pre_s)), right_send, right_recv
        else:
            pairs, ss, rs = ((left_o, suf_o), (left_s, suf_s)), left_send, left_recv
        return [
            pltpu.make_async_remote_copy(
                src_ref=src.at[h],
                dst_ref=dst.at[h],
                send_sem=ss.at[i],
                recv_sem=rs.at[lax.rem(h, ring)],
                device_id={"slab": z + direction},
                device_id_type=MESH,
            )
            for i, (src, dst) in enumerate(pairs)
        ]

    def arrived(h, direction):
        ss, rs = (right_send, right_recv) if direction > 0 else (left_send, left_recv)
        pltpu.make_async_remote_copy(
            src_ref=gauge,
            dst_ref=gauge,
            send_sem=ss.at[0],
            recv_sem=rs.at[lax.rem(h, ring)],
            device_id={"slab": z - direction},
            device_id_type=MESH,
        ).wait_recv()

    def settle_sends(direction):
        if direction > 0:
            pairs, ss, rs = ((right_o, pre_o), (right_s, pre_s)), right_send, right_recv
        else:
            pairs, ss, rs = ((left_o, suf_o), (left_s, suf_s)), left_send, left_recv
        for i, (src, dst) in enumerate(pairs):
            pltpu.make_async_remote_copy(
                src_ref=src,
                dst_ref=dst,
                send_sem=ss.at[i],
                recv_sem=rs.at[0],
                device_id={"slab": z + direction},
                device_id_type=MESH,
            ).wait_send()

    pair = 2 if hcount % 2 == 0 else 1
    splits = next(k for k in (SPLIT, 2, 1) if hcount % k == 0)
    sub = HD // splits
    tuples = hcount // splits
    pairs = hcount // pair
    last = (groups - 1) * hcount
    fresh_rows = seq_n * 2 * fk_ref.shape[0]
    lag_end = LAG * jnp.maximum(z, n - 1 - z)

    def combine(h, other_o, other_s, dest_o, dest_s):
        l_a, l_b = own_s[h], other_s[h]
        top = jnp.maximum(l_a, l_b)
        e_a, e_b = jnp.exp2(l_a - top), jnp.exp2(l_b - top)
        mass = e_a + e_b
        share = 1.0 / mass
        dest_o[h] = (
            own_o[h] * (e_a * share) + other_o[h].astype(F32) * (e_b * share)
        ).astype(BF16)
        dest_s[h] = top + jnp.log2(mass)

    nt = (((1,), (1,)), ((), ()))
    tn = (((0,), (0,)), ((), ()))

    penalty = jnp.where(
        jnp.full((1, rows), owner_ref[0, 0], jnp.int32) == z, F32(LOW), F32(0.0)
    )
    cached = kc.shape[0]
    step_keys = 256 if cached % 256 == 0 else cached
    blocks = [(i, i + step_keys) for i in range(0, cached, step_keys)]

    def head_cols(h):
        return pl.ds(pl.multiple_of(h * HD, HD), HD)

    def scores(h, slot):
        cols = head_cols(h)
        q_head = qg[:, cols]
        top = None
        for a, b in blocks:
            part = lax.dot_general(kc[a:b, cols], q_head, nt, preferred_element_type=F32)
            s_buf[slot, a:b, :] = part
            high = jnp.max(part, axis=0, keepdims=True)
            top = high if top is None else jnp.maximum(top, high)
        k_fresh = kf[:, :, :, cols].reshape(fresh_rows, HD)
        part = lax.dot_general(k_fresh, q_head, nt, preferred_element_type=F32)
        s_buf[slot, cached:, :] = part
        m_buf[slot, 0:1, :] = top
        m_buf[slot, 1:2, :] = jnp.max(part, axis=0, keepdims=True)

    def soften(slot, r=slice(None)):
        s_row = scale[0:1, r]
        mask = penalty[:, r]
        top = jnp.maximum(m_buf[slot, 0:1, r] * s_row + mask, m_buf[slot, 1:2, r] * s_row)
        top_c = top - mask
        mass = jnp.zeros_like(top)
        for a, b in blocks + [(cached, cached + fresh_rows)]:
            p = jnp.exp2(s_buf[slot, a:b, r] * s_row - (top_c if a < cached else top))
            p_buf[slot, a:b, r] = p.astype(BF16)
            mass = mass + jnp.sum(p, axis=0, keepdims=True)
        m_buf[slot, 2:3, r] = 1.0 / mass
        m_buf[slot, 3:4, r] = top + jnp.log2(mass)

    packed = splits > 1

    def pack(c):
        k = c - last
        s, p = lax.div(k, tuples), lax.rem(k, tuples)
        seat_o = lax.broadcasted_iota(jnp.int32, (HD, HD), 1) // sub
        seat_s = lax.broadcasted_iota(jnp.int32, (1, HD), 1) // sub
        value, stats = jnp.zeros((HD, HD), F32), jnp.zeros((1, HD), F32)
        for i in range(splits):
            turn = lax.rem((i - s + splits) * sub, HD)
            value = jnp.where(seat_o == i, pltpu.roll(raw_o[p * splits + i], turn, 1), value)
            stats = jnp.where(seat_s == i, pltpu.roll(raw_s[p * splits + i], turn, 1), stats)
        own_o[c] = value
        own_s[c] = stats

    def weigh(h, slot, first=0, end=None):
        cols = head_cols(h)
        end = groups if end is None else end
        r = slice(first * HD, end * HD)
        v_fresh = vf[:, :, :, cols].reshape(fresh_rows, HD)
        o = lax.dot_general(v_fresh, p_buf[slot, cached:, r], tn, preferred_element_type=F32)
        for a, b in blocks:
            o += lax.dot_general(
                vc[a:b, cols], p_buf[slot, a:b, r], tn, preferred_element_type=F32
            )

        o = o * m_buf[slot, 2:3, r]

        for g in range(first, end):
            to_o, to_s, at = own_o, own_s, g * hcount + h
            if packed and g == groups - 1:
                to_o, to_s, at = raw_o, raw_s, h
            to_o[at] = o[:, (g - first) * HD : (g - first + 1) * HD]
            to_s[at] = m_buf[slot, 3:4, g * HD : (g + 1) * HD]

    def project(g, p):
        deep = pl.ds(pl.multiple_of(p * pair * HD, HD), pair * HD)
        term = lax.dot_general(att[g, deep, :], w[deep, :], tn, preferred_element_type=F32)
        add(acc.at[g * HD : (g + 1) * HD, :], term, p)

    def project_last(s, p):
        deep = pl.ds(pl.multiple_of(p * splits * HD, HD), splits * HD)
        term = lax.dot_general(
            att[groups - 1 + s, deep, 0:sub], w[deep, :], tn, preferred_element_type=F32
        )
        add(acc.at[(groups - 1) * HD + s * sub : (groups - 1) * HD + (s + 1) * sub, :], term, p)

    def add(dest, term, p):
        @pl.when(p == 0)
        def _():
            dest[...] = term

        @pl.when(p > 0)
        def _():
            dest[...] += term

    pieces = [(g * HD, (g + 1) * HD) for g in range(groups - 1)]
    pieces += [((groups - 1) * HD + s * sub, (groups - 1) * HD + (s + 1) * sub) for s in range(splits)]

    def exchange(k):
        a, b = pieces[k]
        copies = []
        for d in range(1, heads_n):
            copies.append(
                pltpu.make_async_remote_copy(
                    src_ref=xs.at[d - 1, a:b],
                    dst_ref=xr.at[d - 1, a:b],
                    send_sem=x_send.at[d - 1],
                    recv_sem=x_recv.at[d - 1, k],
                    device_id={"head": lax.rem(hx + d, heads_n)},
                    device_id_type=MESH,
                )
            )
        return copies

    def exchange_start(k):
        a, b = pieces[k]
        cp = out_ref.shape[1]
        for d, c in enumerate(exchange(k)):
            peer = lax.rem(hx + d + 1, heads_n)
            cols = pl.ds(pl.multiple_of(peer * cp, HD), cp)
            xs[d, a:b] = acc[a:b, cols].astype(BF16)
            c.start()

    def service(t):
        cp_ = t - LAG * z
        in_p = (cp_ >= 0) & (cp_ < chunks)
        cs = t - LAG * (n - 1 - z)
        in_s = (cs >= 0) & (cs < chunks)

        @pl.when(in_p & (z > 0))
        def _():
            arrived(cp_, 1)

        @pl.when(in_p & (z < n - 1))
        def _():
            combine(cp_, pre_o, pre_s, right_o, right_s)
            for c in send(cp_, 1):
                c.start()

        @pl.when(in_s & (z < n - 1))
        def _():
            arrived(cs, -1)

        @pl.when(in_s & (z > 0))
        def _():
            combine(cs, suf_o, suf_s, left_o, left_s)
            for c in send(cs, -1):
                c.start()

    def finish(t):
        f = t - lag_end

        @pl.when((f >= 0) & (f < chunks))
        def _():
            m_a, m_b, m_c = own_s[f], pre_s[f], suf_s[f]
            top = jnp.maximum(m_a, jnp.maximum(m_b, m_c))
            e_a, e_b, e_c = jnp.exp2(m_a - top), jnp.exp2(m_b - top), jnp.exp2(m_c - top)
            share = 1.0 / (e_a + e_b + e_c)
            total_o = (
                own_o[f] * (e_a * share)
                + pre_o[f].astype(F32) * (e_b * share)
                + suf_o[f].astype(F32) * (e_c * share)
            )
            value = total_o.astype(BF16)

            @pl.when(f < last)
            def _():
                h = lax.rem(f, hcount)
                att[f // hcount, head_cols(h), :] = value

            @pl.when(f >= last)
            def _():
                k = f - last
                s, p = lax.div(k, tuples), lax.rem(k, tuples)
                for i in range(splits):
                    turned = value if i == 0 else pltpu.roll(total_o, HD - i * sub, 1).astype(BF16)
                    att[groups - 1 + s, head_cols(p * splits + i), :] = turned

        @pl.when(f == hcount - pairs)
        def _():
            w_load.wait()

        for g in range(groups - 1):
            begin = (g + 1) * hcount - pairs

            @pl.when((f >= begin) & (f < begin + pairs))
            def _(g=g, begin=begin):
                project(g, f - begin)

            if aligned:

                @pl.when(f == begin + pairs - 1)
                def _(g=g):
                    exchange_start(g)

        for s in range(splits):
            begin = last + s * tuples

            stop = begin + tuples - (1 if aligned and s == splits - 1 else 0)

            @pl.when((f >= begin) & (f < stop))
            def _(s=s, begin=begin):
                project_last(s, f - begin)

            if aligned and s < splits - 1:

                @pl.when(f == begin + tuples - 1)
                def _(s=s):
                    exchange_start(groups - 1 + s)

        if aligned:

            @pl.when(f == chunks - 1)
            def _():
                a, b = pieces[-1]
                cp = out_ref.shape[1]
                deep = slice((tuples - 1) * splits * HD, tuples * splits * HD)
                sums = att[groups + splits - 2, deep, 0:sub]

                def total_of(owner):
                    cols = pl.ds(pl.multiple_of(owner * cp, HD), cp)
                    before = 0.0 if tuples == 1 else acc[a:b, cols]
                    return cols, before + lax.dot_general(
                        sums, w[deep, cols], tn, preferred_element_type=F32
                    )

                for d, c in enumerate(exchange(len(pieces) - 1)):
                    xs[d, a:b] = total_of(lax.rem(hx + d + 1, heads_n))[1].astype(BF16)
                    c.start()
                cols, own = total_of(hx)
                acc[a:b, cols] = own

    def near(h):
        return jnp.minimum(h, hcount - 1)

    kv_loads[0].wait()
    for c in fresh_local:
        c.wait()
    for c in fresh_remote[0]:
        c.wait_recv()
    scores(0, 0)
    scores(min(1, hcount - 1), 1)
    def rescale(g):
        for c in sq_copies[g]:
            c.wait_recv()
        norm_total = squares[0, g]
        for d in range(1, heads_n):
            norm_total = norm_total + squares[d, g]
        scale[0:1, g * HD : (g + 1) * HD] = lax.rsqrt(norm_total / (HEADS * HD) + EPSILON) * (
            math.log2(math.e) / HD**0.5
        )

    rescale(0)
    soften(0, slice(0, HD))
    kv_loads[1].wait()
    weigh(0, 0, 0, 1)
    service(0)
    w_load.start()
    for g in range(1, groups):
        rescale(g)
    if groups > 1:
        soften(0, slice(HD, rows))
        weigh(0, 0, 1, groups)
    soften(1)
    scores(min(2, hcount - 1), 0)

    unroll = 2

    def body(i, carry):
        for u in range(unroll):
            t = unroll * i + u
            if len(cuts) > 1:

                @pl.when(t + 3 == ahead)
                def _():
                    for c in fresh_remote[1]:
                        c.wait_recv()
                    for c in kv_loads[2:]:
                        c.wait()

            @pl.when(t + 1 < hcount)
            def _(t=t, u=u):
                scores(near(t + 3), (u + 1) % 2)
                soften(u % 2)
                weigh(t + 1, (u + 1) % 2)

            if packed:
                c = t + 1 + tuples

                @pl.when((c >= last) & (c < chunks))
                def _(c=c):
                    pack(c)

            finish(t)
            service(t + 1)
        return carry

    lax.fori_loop(0, -(-(chunks + LAG * (n - 1)) // unroll), body, 0)

    def settle():
        for d in range(1, seq_n):
            for side in (0, 1):
                fresh_wait(d, side, slice(0, width)).wait_send()
        for c in [c for copies in sq_copies for c in copies]:
            c.wait_send()

        @pl.when(z < n - 1)
        def _():
            settle_sends(1)

        @pl.when(z > 0)
        def _():
            settle_sends(-1)

    if aligned:
        cp = out_ref.shape[1]
        mine = pl.ds(pl.multiple_of(hx * cp, HD), cp)
        settle()
        for k, (a, b) in enumerate(pieces):
            summed = acc[a:b, mine]
            for d, c in enumerate(exchange(k)):
                c.wait_recv()
                summed = summed + xr[d, a:b].astype(F32)
            out_ref[a:b, :] = (summed * gate[...]).astype(out_ref.dtype)
        for d in range(1, heads_n):
            pltpu.make_async_remote_copy(
                src_ref=xs.at[d - 1],
                dst_ref=xr.at[d - 1],
                send_sem=x_send.at[d - 1],
                recv_sem=x_recv.at[d - 1, 0],
                device_id={"head": lax.rem(hx + d, heads_n)},
                device_id_type=MESH,
            ).wait_send()
    else:
        out_ref[...] = acc[...]
        settle()


def local(sizes, *args):
    (
        queries,
        query_gain,
        cache_keys,
        cache_values,
        finished_keys,
        finished_values,
        new_keys,
        new_values,
        out_weight,
        time_weight,
        owner,
        step,
    ) = args
    n, heads_n, seq_n = sizes
    rows, width = queries.shape
    hcount = width // HD
    cached, fresh = cache_keys.shape[0], finished_keys.shape[0]
    columns, cp = out_weight.shape[1], time_weight.shape[1]
    freq = time_weight.shape[0]
    aligned = cp % HD == 0
    any_spec = pl.BlockSpec(memory_space=pl.ANY)
    vmem = pl.BlockSpec(memory_space=pltpu.VMEM)
    dma = pltpu.SemaphoreType.DMA
    xcount = max(heads_n - 1, 1)
    groups = rows // HD
    chunks = groups * hcount
    ring = min(chunks, LAG * (n - 1) + 1)
    stat = (chunks, 1, HD)
    keys = cached + seq_n * 2 * fresh
    part = (chunks, HD, HD)
    result = pl.pallas_call(
        functools.partial(kernel, sizes, aligned),
        out_shape=pltpu.VMEM((rows, cp), BF16) if aligned else jax.ShapeDtypeStruct((rows, columns), F32),
        in_specs=[any_spec] * 12,
        out_specs=vmem,
        scratch_shapes=[
            pltpu.VMEM((rows, width), BF16),
            pltpu.VMEM((rows, width), BF16),
            pltpu.VMEM((width,), F32),
            pltpu.VMEM((cached, width), BF16),
            pltpu.VMEM((cached, width), BF16),
            pltpu.VMEM((seq_n, 2, fresh, width), BF16),
            pltpu.VMEM((seq_n, 2, fresh, width), BF16),
            pltpu.VMEM((width, columns), BF16),
            pltpu.VMEM((freq, cp), F32),
            pltpu.VMEM((heads_n, groups, 1, HD), F32),
            pltpu.VMEM((1, rows), F32),
            pltpu.VMEM(part, F32),
            pltpu.VMEM(stat, F32),
            pltpu.VMEM(part, BF16),
            pltpu.VMEM(stat, F32),
            pltpu.VMEM(part, BF16),
            pltpu.VMEM(stat, F32),
            pltpu.VMEM(part, BF16),
            pltpu.VMEM(stat, F32),
            pltpu.VMEM(part, BF16),
            pltpu.VMEM(stat, F32),
            pltpu.VMEM((groups + SPLIT - 1, width, HD), BF16),
            pltpu.VMEM((rows, columns), F32),
            pltpu.VMEM((1, cp), F32),
            pltpu.VMEM((xcount, rows, cp), BF16),
            pltpu.VMEM((xcount, rows, cp), BF16),
            dma((3,)),
            dma((2,)),
            dma((max(seq_n - 1, 1), 2)),
            dma((max(seq_n - 1, 1), 2, 2)),
            dma((xcount, groups)),
            dma((xcount, groups)),
            dma((2,)),
            dma((ring,)),
            dma((2,)),
            dma((ring,)),
            dma((xcount,)),
            dma((xcount, groups + SPLIT - 1)),
            pltpu.VMEM((2, keys, rows), F32),
            pltpu.VMEM((2, keys, rows), BF16),
            pltpu.VMEM((2, 4, rows), F32),
            dma((groups * PARTS,)),
            dma((2, 2)),
            pltpu.VMEM((HD // 2 + 1, 1, HD), F32),
            pltpu.VMEM((hcount, HD, HD), F32),
            pltpu.VMEM((hcount, 1, HD), F32),
            pltpu.SMEM((1, 1), jnp.int32),
            pltpu.SMEM((1, 1), jnp.int32),
            dma((2,)),
        ],
        compiler_params=pltpu.CompilerParams(
            collective_id=0, has_side_effects=True, vmem_limit_bytes=60 * 1024 * 1024
        ),
        name="sweep_attention",
    )(
        queries,
        query_gain,
        cache_keys,
        cache_values,
        finished_keys,
        finished_values,
        new_keys,
        new_values,
        out_weight,
        time_weight,
        owner,
        step,
    )
    if aligned:
        return result
    summed = lax.psum_scatter(result, "head", scatter_dimension=1, tiled=True)
    half = freq // 2
    frequency = jnp.exp(-jnp.log(10000.0) * jnp.arange(half, dtype=F32) / half)
    phases = step[0, 0].astype(F32) * frequency
    embedding = jnp.concatenate([jnp.cos(phases), jnp.sin(phases)])
    time_gate = 1.0 + jnp.dot(embedding, time_weight, precision=lax.Precision.HIGHEST)
    return (time_gate * summed).astype(BF16)


def solution(mesh):
    in_specs = (
        P(("grp", "seq"), "head"),
        P("head"),
        P(("grp", "slab"), "head"),
        P(("grp", "slab"), "head"),
        P(("grp", "slab", "seq"), "head"),
        P(("grp", "slab", "seq"), "head"),
        P(("grp", "slab", "seq"), "head"),
        P(("grp", "slab", "seq"), "head"),
        P("head", "slab"),
        P(None, ("slab", "head")),
        P("grp", None),
        P("grp", None),
    )
    out_specs = P(("grp", "seq"), ("slab", "head"))
    sizes = (mesh.shape["slab"], mesh.shape["head"], mesh.shape["seq"])
    mapped = jax.shard_map(
        functools.partial(local, sizes),
        mesh=mesh,
        in_specs=in_specs,
        out_specs=out_specs,
        check_vma=False,
    )

    def run(*args):
        return mapped(*args[:-2], args[-2].reshape(-1, 1), args[-1].reshape(-1, 1))

    return run
```

```python
import functools
import math

import jax
import jax.numpy as jnp
from jax import lax
from jax.experimental import pallas as pl
from jax.experimental.pallas import tpu as pltpu
from jax.sharding import PartitionSpec as P

HEADS = 40
HD = 128
EPSILON = 1e-06
LOW = -1e30
LAG = 5
SPLIT = 2
PARTS = 1
MESH = pl.DeviceIdType.MESH
F32 = jnp.float32
BF16 = jnp.bfloat16


def kernel(
    dims,
    aligned,
    q_ref,
    gain_ref,
    ck_ref,
    cv_ref,
    fk_ref,
    fv_ref,
    nk_ref,
    nv_ref,
    w_ref,
    tw_ref,
    owner_hbm,
    step_hbm,
    out_ref,
    q,
    qg,
    gain,
    kc,
    vc,
    kf,
    vf,
    w,
    tw,
    squares,
    scale,
    own_o,
    own_s,
    pre_o,
    pre_s,
    suf_o,
    suf_s,
    right_o,
    right_s,
    left_o,
    left_s,
    att,
    acc,
    gate,
    xs,
    xr,
    load_sem,
    fresh_sem,
    fresh_send,
    fresh_recv,
    sq_send,
    sq_recv,
    right_send,
    right_recv,
    left_send,
    left_recv,
    x_send,
    x_recv,
    s_buf,
    p_buf,
    m_buf,
    q_sem,
    kv_sem,
    gauge,
    raw_o,
    raw_s,
    owner_ref,
    step_ref,
    scalar_sem,
):
    n, heads_n, seq_n = dims
    rows, width = q_ref.shape
    hcount = width // HD
    z = lax.axis_index("slab")
    hx = lax.axis_index("head")
    sq = lax.axis_index("seq")

    groups = rows // HD
    chunks = groups * hcount
    gain_load, w_load, tw_load = [
        pltpu.make_async_copy(src, dst, load_sem.at[i])
        for i, (src, dst) in enumerate([(gain_ref, gain), (w_ref, w), (tw_ref, tw)])
    ]
    ahead = min(max(hcount // 5, 3), hcount)
    parts = PARTS if hcount % PARTS == 0 else 1
    span = width // parts
    q_loads = []
    for g in range(groups):
        for k in range(parts):
            at = (slice(g * HD, (g + 1) * HD), slice(k * span, (k + 1) * span))
            q_loads.append(
                pltpu.make_async_copy(q_ref.at[at], q.at[at], q_sem.at[g * parts + k])
            )
    for c in q_loads:
        c.start()
    gain_load.start()
    scalars = [
        pltpu.make_async_copy(owner_hbm, owner_ref, scalar_sem.at[0]),
        pltpu.make_async_copy(step_hbm, step_ref, scalar_sem.at[1]),
    ]
    for c in scalars:
        c.start()
    barrier = pltpu.get_barrier_semaphore()
    for d in range(1, seq_n):
        pl.semaphore_signal(
            barrier, inc=1, device_id={"seq": lax.rem(sq + d, seq_n)}, device_id_type=MESH
        )
    for d in range(1, heads_n):
        pl.semaphore_signal(
            barrier, inc=1, device_id={"head": lax.rem(hx + d, heads_n)}, device_id_type=MESH
        )

    @pl.when(z > 0)
    def _():
        pl.semaphore_signal(barrier, inc=1, device_id={"slab": z - 1}, device_id_type=MESH)

    @pl.when(z < n - 1)
    def _():
        pl.semaphore_signal(barrier, inc=1, device_id={"slab": z + 1}, device_id_type=MESH)

    def clear(o_ref, s_ref):
        o_ref[...] = jnp.zeros_like(o_ref)
        s_ref[...] = jnp.full((chunks, 1, HD), LOW, F32)

    @pl.when(z == 0)
    def _():
        clear(pre_o, pre_s)

    @pl.when(z == n - 1)
    def _():
        clear(suf_o, suf_s)

    def squares_of(g):
        def step(h, total):
            x = q[g * HD : (g + 1) * HD, pl.ds(pl.multiple_of(h * HD, HD), HD)].astype(F32)
            return total + x * x

        total = jnp.zeros((HD, HD), F32)
        for k in range(parts):
            q_loads[g * parts + k].wait()
            total = lax.fori_loop(
                k * hcount // parts, (k + 1) * hcount // parts, step, total, unroll=True
            )
        squares[hx, g] = jnp.sum(total.T, axis=0, keepdims=True)

    squares_of(0)
    head_cut = ahead * HD
    kv_cuts = [slice(0, head_cut), slice(head_cut, width)] if head_cut < width else [slice(0, width)]
    kv_loads = []
    for k, cols in enumerate(kv_cuts):
        for i, (src, dst) in enumerate([(ck_ref, kc), (cv_ref, vc)]):
            kv_loads.append(pltpu.make_async_copy(src.at[:, cols], dst.at[:, cols], kv_sem.at[k, i]))
    fresh_src = [(fk_ref, kf, 0), (nk_ref, kf, 1), (fv_ref, vf, 0), (nv_ref, vf, 1)]

    ends = (z == 0).astype(jnp.int32) + (z == n - 1).astype(jnp.int32)
    pl.semaphore_wait(barrier, seq_n - 1 + heads_n - 1 + 2 - ends)

    sq_copies = []

    def squares_send(g):
        copies = []
        for d in range(1, heads_n):
            c = pltpu.make_async_remote_copy(
                src_ref=squares.at[hx, g],
                dst_ref=squares.at[hx, g],
                send_sem=sq_send.at[d - 1, g],
                recv_sem=sq_recv.at[d - 1, g],
                device_id={"head": lax.rem(hx + d, heads_n)},
                device_id_type=MESH,
            )
            c.start()
            copies.append(c)
        sq_copies.append(copies)

    squares_send(0)
    for c in kv_loads[:2]:
        c.start()
    for g in range(1, groups):
        squares_of(g)
        squares_send(g)
    tw_load.start()
    for c in kv_loads[2:]:
        c.start()
    fresh_local = []
    for i, (src, dst, part) in enumerate(fresh_src):
        pltpu.make_async_copy(src, dst.at[sq, part], fresh_sem.at[i // 2]).start()
    for side, whole in enumerate((kf, vf)):
        fresh_local.append(pltpu.make_async_copy(whole.at[sq], whole.at[sq], fresh_sem.at[side]))

    edges = [0, ahead * HD, width] if ahead < hcount else [0, width]
    cuts = [slice(a, b) for a, b in zip(edges, edges[1:])]
    fresh_remote = [[] for _ in cuts]

    def fresh_wait(d, side, cols, k=0):
        whole = (kf, vf)[side].at[sq, :, :, cols]
        return pltpu.make_async_remote_copy(
            src_ref=whole,
            dst_ref=whole,
            send_sem=fresh_send.at[d - 1, side],
            recv_sem=fresh_recv.at[d - 1, k, side],
            device_id={"seq": lax.rem(sq + d, seq_n)},
            device_id_type=MESH,
        )

    for k, cols in enumerate(cuts):
        for d in range(1, seq_n):
            for i, (src, dst, part) in enumerate(fresh_src):
                pltpu.make_async_remote_copy(
                    src_ref=src.at[:, cols],
                    dst_ref=dst.at[sq, part, :, cols],
                    send_sem=fresh_send.at[d - 1, i // 2],
                    recv_sem=fresh_recv.at[d - 1, k, i // 2],
                    device_id={"seq": lax.rem(sq + d, seq_n)},
                    device_id_type=MESH,
                ).start()
            fresh_remote[k] += [fresh_wait(d, side, cols, k) for side in (0, 1)]

    gain_load.wait()

    def gain_step(h, carry):
        cols = pl.ds(pl.multiple_of(h * HD, HD), HD)
        qg[:, cols] = (q[:, cols].astype(F32) * gain[cols][None, :]).astype(BF16)
        return carry

    lax.fori_loop(0, hcount, gain_step, 0)
    tw_load.wait()
    for c in scalars:
        c.wait()
    if aligned:
        half = tw.shape[0] // 2
        j = lax.broadcasted_iota(jnp.int32, (half, HD), 0).astype(F32)
        frequency = jnp.exp(F32(-math.log(10000.0)) * j / half)
        phases = jnp.full((half, HD), step_ref[0, 0], jnp.int32).astype(F32) * frequency
        cos, sin = jnp.cos(phases), jnp.sin(phases)
        for c in range(tw.shape[1] // HD):
            cols = slice(c * HD, (c + 1) * HD)
            terms = tw[:half, cols] * cos + tw[half:, cols] * sin
            gate[:, cols] = 1.0 + jnp.sum(terms, axis=0, keepdims=True)


    ring = min(chunks, LAG * (n - 1) + 1)

    def send(h, direction):
        if direction > 0:
            pairs, ss, rs = ((right_o, pre_o), (right_s, pre_s)), right_send, right_recv
        else:
            pairs, ss, rs = ((left_o, suf_o), (left_s, suf_s)), left_send, left_recv
        return [
            pltpu.make_async_remote_copy(
                src_ref=src.at[h],
                dst_ref=dst.at[h],
                send_sem=ss.at[i],
                recv_sem=rs.at[lax.rem(h, ring)],
                device_id={"slab": z + direction},
                device_id_type=MESH,
            )
            for i, (src, dst) in enumerate(pairs)
        ]

    def arrived(h, direction):
        ss, rs = (right_send, right_recv) if direction > 0 else (left_send, left_recv)
        pltpu.make_async_remote_copy(
            src_ref=gauge,
            dst_ref=gauge,
            send_sem=ss.at[0],
            recv_sem=rs.at[lax.rem(h, ring)],
            device_id={"slab": z - direction},
            device_id_type=MESH,
        ).wait_recv()

    def settle_sends(direction):
        if direction > 0:
            pairs, ss, rs = ((right_o, pre_o), (right_s, pre_s)), right_send, right_recv
        else:
            pairs, ss, rs = ((left_o, suf_o), (left_s, suf_s)), left_send, left_recv
        for i, (src, dst) in enumerate(pairs):
            pltpu.make_async_remote_copy(
                src_ref=src,
                dst_ref=dst,
                send_sem=ss.at[i],
                recv_sem=rs.at[0],
                device_id={"slab": z + direction},
                device_id_type=MESH,
            ).wait_send()

    pair = 2 if hcount % 2 == 0 else 1
    splits = next(k for k in (SPLIT, 2, 1) if hcount % k == 0)
    sub = HD // splits
    tuples = hcount // splits
    pairs = hcount // pair
    last = (groups - 1) * hcount
    fresh_rows = seq_n * 2 * fk_ref.shape[0]
    lag_end = LAG * jnp.maximum(z, n - 1 - z)

    def combine(h, other_o, other_s, dest_o, dest_s):
        l_a, l_b = own_s[h], other_s[h]
        top = jnp.maximum(l_a, l_b)
        e_a, e_b = jnp.exp2(l_a - top), jnp.exp2(l_b - top)
        mass = e_a + e_b
        share = 1.0 / mass
        dest_o[h] = (
            own_o[h] * (e_a * share) + other_o[h].astype(F32) * (e_b * share)
        ).astype(BF16)
        dest_s[h] = top + jnp.log2(mass)

    nt = (((1,), (1,)), ((), ()))
    tn = (((0,), (0,)), ((), ()))

    penalty = jnp.where(
        jnp.full((1, rows), owner_ref[0, 0], jnp.int32) == z, F32(LOW), F32(0.0)
    )
    cached = kc.shape[0]
    step_keys = 256 if cached % 256 == 0 else cached
    blocks = [(i, i + step_keys) for i in range(0, cached, step_keys)]

    def head_cols(h):
        return pl.ds(pl.multiple_of(h * HD, HD), HD)

    def scores(h, slot):
        cols = head_cols(h)
        q_head = qg[:, cols]
        top = None
        for a, b in blocks:
            part = lax.dot_general(kc[a:b, cols], q_head, nt, preferred_element_type=F32)
            s_buf[slot, a:b, :] = part
            high = jnp.max(part, axis=0, keepdims=True)
            top = high if top is None else jnp.maximum(top, high)
        k_fresh = kf[:, :, :, cols].reshape(fresh_rows, HD)
        part = lax.dot_general(k_fresh, q_head, nt, preferred_element_type=F32)
        s_buf[slot, cached:, :] = part
        m_buf[slot, 0:1, :] = top
        m_buf[slot, 1:2, :] = jnp.max(part, axis=0, keepdims=True)

    def soften(slot, r=slice(None)):
        s_row = scale[0:1, r]
        mask = penalty[:, r]
        top = jnp.maximum(m_buf[slot, 0:1, r] * s_row + mask, m_buf[slot, 1:2, r] * s_row)
        top_c = top - mask
        mass = jnp.zeros_like(top)
        for a, b in blocks + [(cached, cached + fresh_rows)]:
            p = jnp.exp2(s_buf[slot, a:b, r] * s_row - (top_c if a < cached else top))
            p_buf[slot, a:b, r] = p.astype(BF16)
            mass = mass + jnp.sum(p, axis=0, keepdims=True)
        m_buf[slot, 2:3, r] = 1.0 / mass
        m_buf[slot, 3:4, r] = top + jnp.log2(mass)

    packed = splits > 1

    def pack(c):
        k = c - last
        s, p = lax.div(k, tuples), lax.rem(k, tuples)
        seat_o = lax.broadcasted_iota(jnp.int32, (HD, HD), 1) // sub
        seat_s = lax.broadcasted_iota(jnp.int32, (1, HD), 1) // sub
        value, stats = jnp.zeros((HD, HD), F32), jnp.zeros((1, HD), F32)
        for i in range(splits):
            turn = lax.rem((i - s + splits) * sub, HD)
            value = jnp.where(seat_o == i, pltpu.roll(raw_o[p * splits + i], turn, 1), value)
            stats = jnp.where(seat_s == i, pltpu.roll(raw_s[p * splits + i], turn, 1), stats)
        own_o[c] = value
        own_s[c] = stats

    def weigh(h, slot, first=0, end=None):
        cols = head_cols(h)
        end = groups if end is None else end
        r = slice(first * HD, end * HD)
        v_fresh = vf[:, :, :, cols].reshape(fresh_rows, HD)
        o = lax.dot_general(v_fresh, p_buf[slot, cached:, r], tn, preferred_element_type=F32)
        for a, b in blocks:
            o += lax.dot_general(
                vc[a:b, cols], p_buf[slot, a:b, r], tn, preferred_element_type=F32
            )

        o = o * m_buf[slot, 2:3, r]

        for g in range(first, end):
            to_o, to_s, at = own_o, own_s, g * hcount + h
            if packed and g == groups - 1:
                to_o, to_s, at = raw_o, raw_s, h
            to_o[at] = o[:, (g - first) * HD : (g - first + 1) * HD]
            to_s[at] = m_buf[slot, 3:4, g * HD : (g + 1) * HD]

    def project(g, p):
        deep = pl.ds(pl.multiple_of(p * pair * HD, HD), pair * HD)
        term = lax.dot_general(att[g, deep, :], w[deep, :], tn, preferred_element_type=F32)
        add(acc.at[g * HD : (g + 1) * HD, :], term, p)

    def project_last(s, p):
        deep = pl.ds(pl.multiple_of(p * splits * HD, HD), splits * HD)
        term = lax.dot_general(
            att[groups - 1 + s, deep, 0:sub], w[deep, :], tn, preferred_element_type=F32
        )
        add(acc.at[(groups - 1) * HD + s * sub : (groups - 1) * HD + (s + 1) * sub, :], term, p)

    def add(dest, term, p):
        @pl.when(p == 0)
        def _():
            dest[...] = term

        @pl.when(p > 0)
        def _():
            dest[...] += term

    pieces = [(g * HD, (g + 1) * HD) for g in range(groups - 1)]
    pieces += [((groups - 1) * HD + s * sub, (groups - 1) * HD + (s + 1) * sub) for s in range(splits)]

    def exchange(k):
        a, b = pieces[k]
        copies = []
        for d in range(1, heads_n):
            copies.append(
                pltpu.make_async_remote_copy(
                    src_ref=xs.at[d - 1, a:b],
                    dst_ref=xr.at[d - 1, a:b],
                    send_sem=x_send.at[d - 1],
                    recv_sem=x_recv.at[d - 1, k],
                    device_id={"head": lax.rem(hx + d, heads_n)},
                    device_id_type=MESH,
                )
            )
        return copies

    def exchange_start(k):
        a, b = pieces[k]
        cp = out_ref.shape[1]
        for d, c in enumerate(exchange(k)):
            peer = lax.rem(hx + d + 1, heads_n)
            cols = pl.ds(pl.multiple_of(peer * cp, HD), cp)
            xs[d, a:b] = acc[a:b, cols].astype(BF16)
            c.start()

    def service(t):
        cp_ = t - LAG * z
        in_p = (cp_ >= 0) & (cp_ < chunks)
        cs = t - LAG * (n - 1 - z)
        in_s = (cs >= 0) & (cs < chunks)

        @pl.when(in_p & (z > 0))
        def _():
            arrived(cp_, 1)

        @pl.when(in_p & (z < n - 1))
        def _():
            combine(cp_, pre_o, pre_s, right_o, right_s)
            for c in send(cp_, 1)[::-1]:
                c.start()

        @pl.when(in_s & (z < n - 1))
        def _():
            arrived(cs, -1)

        @pl.when(in_s & (z > 0))
        def _():
            combine(cs, suf_o, suf_s, left_o, left_s)
            for c in send(cs, -1)[::-1]:
                c.start()

    def finish(t):
        f = t - lag_end

        @pl.when((f >= 0) & (f < chunks))
        def _():
            m_a, m_b, m_c = own_s[f], pre_s[f], suf_s[f]
            top = jnp.maximum(m_a, jnp.maximum(m_b, m_c))
            e_a, e_b, e_c = jnp.exp2(m_a - top), jnp.exp2(m_b - top), jnp.exp2(m_c - top)
            share = 1.0 / (e_a + e_b + e_c)
            total_o = (
                own_o[f] * (e_a * share)
                + pre_o[f].astype(F32) * (e_b * share)
                + suf_o[f].astype(F32) * (e_c * share)
            )
            value = total_o.astype(BF16)

            @pl.when(f < last)
            def _():
                h = lax.rem(f, hcount)
                att[f // hcount, head_cols(h), :] = value

            @pl.when(f >= last)
            def _():
                k = f - last
                s, p = lax.div(k, tuples), lax.rem(k, tuples)
                for i in range(splits):
                    turned = value if i == 0 else pltpu.roll(total_o, HD - i * sub, 1).astype(BF16)
                    att[groups - 1 + s, head_cols(p * splits + i), :] = turned

        @pl.when(f == hcount - pairs)
        def _():
            w_load.wait()

        for g in range(groups - 1):
            begin = (g + 1) * hcount - pairs

            @pl.when((f >= begin) & (f < begin + pairs))
            def _(g=g, begin=begin):
                project(g, f - begin)

            if aligned:

                @pl.when(f == begin + pairs - 1)
                def _(g=g):
                    exchange_start(g)

        for s in range(splits):
            begin = last + s * tuples

            stop = begin + tuples - (1 if aligned and s == splits - 1 else 0)

            @pl.when((f >= begin) & (f < stop))
            def _(s=s, begin=begin):
                project_last(s, f - begin)

            if aligned and s < splits - 1:

                @pl.when(f == begin + tuples - 1)
                def _(s=s):
                    exchange_start(groups - 1 + s)

        if aligned:

            @pl.when(f == chunks - 1)
            def _():
                a, b = pieces[-1]
                cp = out_ref.shape[1]
                deep = slice((tuples - 1) * splits * HD, tuples * splits * HD)
                sums = att[groups + splits - 2, deep, 0:sub]

                def total_of(owner):
                    cols = pl.ds(pl.multiple_of(owner * cp, HD), cp)
                    before = 0.0 if tuples == 1 else acc[a:b, cols]
                    return cols, before + lax.dot_general(
                        sums, w[deep, cols], tn, preferred_element_type=F32
                    )

                for d, c in enumerate(exchange(len(pieces) - 1)):
                    xs[d, a:b] = total_of(lax.rem(hx + d + 1, heads_n))[1].astype(BF16)
                    c.start()
                cols, own = total_of(hx)
                acc[a:b, cols] = own

    def near(h):
        return jnp.minimum(h, hcount - 1)

    kv_loads[0].wait()
    for c in fresh_local:
        c.wait()
    for c in fresh_remote[0]:
        c.wait_recv()
    scores(0, 0)
    scores(min(1, hcount - 1), 1)
    def rescale(g):
        for c in sq_copies[g]:
            c.wait_recv()
        norm_total = squares[0, g]
        for d in range(1, heads_n):
            norm_total = norm_total + squares[d, g]
        scale[0:1, g * HD : (g + 1) * HD] = lax.rsqrt(norm_total / (HEADS * HD) + EPSILON) * (
            math.log2(math.e) / HD**0.5
        )

    rescale(0)
    soften(0, slice(0, HD))
    kv_loads[1].wait()
    weigh(0, 0, 0, 1)
    service(0)
    w_load.start()
    for g in range(1, groups):
        rescale(g)
    if groups > 1:
        soften(0, slice(HD, rows))
        weigh(0, 0, 1, groups)
    soften(1)
    scores(min(2, hcount - 1), 0)

    unroll = 2

    def body(i, carry):
        for u in range(unroll):
            t = unroll * i + u
            if len(cuts) > 1:

                @pl.when(t + 3 == ahead)
                def _():
                    for c in fresh_remote[1]:
                        c.wait_recv()
                    for c in kv_loads[2:]:
                        c.wait()

            @pl.when(t + 1 < hcount)
            def _(t=t, u=u):
                scores(near(t + 3), (u + 1) % 2)
                soften(u % 2)
                weigh(t + 1, (u + 1) % 2)

            if packed:
                c = t + 1 + tuples

                @pl.when((c >= last) & (c < chunks))
                def _(c=c):
                    pack(c)

            finish(t)
            service(t + 1)
        return carry

    lax.fori_loop(0, -(-(chunks + LAG * (n - 1)) // unroll), body, 0)

    def settle():
        for d in range(1, seq_n):
            for side in (0, 1):
                fresh_wait(d, side, slice(0, width)).wait_send()
        for c in [c for copies in sq_copies for c in copies]:
            c.wait_send()

        @pl.when(z < n - 1)
        def _():
            settle_sends(1)

        @pl.when(z > 0)
        def _():
            settle_sends(-1)

    if aligned:
        cp = out_ref.shape[1]
        mine = pl.ds(pl.multiple_of(hx * cp, HD), cp)
        settle()
        for k, (a, b) in enumerate(pieces):
            summed = acc[a:b, mine]
            for d, c in enumerate(exchange(k)):
                c.wait_recv()
                summed = summed + xr[d, a:b].astype(F32)
            out_ref[a:b, :] = (summed * gate[...]).astype(out_ref.dtype)
        for d in range(1, heads_n):
            pltpu.make_async_remote_copy(
                src_ref=xs.at[d - 1],
                dst_ref=xr.at[d - 1],
                send_sem=x_send.at[d - 1],
                recv_sem=x_recv.at[d - 1, 0],
                device_id={"head": lax.rem(hx + d, heads_n)},
                device_id_type=MESH,
            ).wait_send()
    else:
        out_ref[...] = acc[...]
        settle()


def local(sizes, *args):
    (
        queries,
        query_gain,
        cache_keys,
        cache_values,
        finished_keys,
        finished_values,
        new_keys,
        new_values,
        out_weight,
        time_weight,
        owner,
        step,
    ) = args
    n, heads_n, seq_n = sizes
    rows, width = queries.shape
    hcount = width // HD
    cached, fresh = cache_keys.shape[0], finished_keys.shape[0]
    columns, cp = out_weight.shape[1], time_weight.shape[1]
    freq = time_weight.shape[0]
    aligned = cp % HD == 0
    any_spec = pl.BlockSpec(memory_space=pl.ANY)
    vmem = pl.BlockSpec(memory_space=pltpu.VMEM)
    dma = pltpu.SemaphoreType.DMA
    xcount = max(heads_n - 1, 1)
    groups = rows // HD
    chunks = groups * hcount
    ring = min(chunks, LAG * (n - 1) + 1)
    stat = (chunks, 1, HD)
    keys = cached + seq_n * 2 * fresh
    part = (chunks, HD, HD)
    result = pl.pallas_call(
        functools.partial(kernel, sizes, aligned),
        out_shape=pltpu.VMEM((rows, cp), BF16) if aligned else jax.ShapeDtypeStruct((rows, columns), F32),
        in_specs=[any_spec] * 12,
        out_specs=vmem,
        scratch_shapes=[
            pltpu.VMEM((rows, width), BF16),
            pltpu.VMEM((rows, width), BF16),
            pltpu.VMEM((width,), F32),
            pltpu.VMEM((cached, width), BF16),
            pltpu.VMEM((cached, width), BF16),
            pltpu.VMEM((seq_n, 2, fresh, width), BF16),
            pltpu.VMEM((seq_n, 2, fresh, width), BF16),
            pltpu.VMEM((width, columns), BF16),
            pltpu.VMEM((freq, cp), F32),
            pltpu.VMEM((heads_n, groups, 1, HD), F32),
            pltpu.VMEM((1, rows), F32),
            pltpu.VMEM(part, F32),
            pltpu.VMEM(stat, F32),
            pltpu.VMEM(part, BF16),
            pltpu.VMEM(stat, F32),
            pltpu.VMEM(part, BF16),
            pltpu.VMEM(stat, F32),
            pltpu.VMEM(part, BF16),
            pltpu.VMEM(stat, F32),
            pltpu.VMEM(part, BF16),
            pltpu.VMEM(stat, F32),
            pltpu.VMEM((groups + SPLIT - 1, width, HD), BF16),
            pltpu.VMEM((rows, columns), F32),
            pltpu.VMEM((1, cp), F32),
            pltpu.VMEM((xcount, rows, cp), BF16),
            pltpu.VMEM((xcount, rows, cp), BF16),
            dma((3,)),
            dma((2,)),
            dma((max(seq_n - 1, 1), 2)),
            dma((max(seq_n - 1, 1), 2, 2)),
            dma((xcount, groups)),
            dma((xcount, groups)),
            dma((2,)),
            dma((ring,)),
            dma((2,)),
            dma((ring,)),
            dma((xcount,)),
            dma((xcount, groups + SPLIT - 1)),
            pltpu.VMEM((2, keys, rows), F32),
            pltpu.VMEM((2, keys, rows), BF16),
            pltpu.VMEM((2, 4, rows), F32),
            dma((groups * PARTS,)),
            dma((2, 2)),
            pltpu.VMEM((HD // 2 + 1, 1, HD), F32),
            pltpu.VMEM((hcount, HD, HD), F32),
            pltpu.VMEM((hcount, 1, HD), F32),
            pltpu.SMEM((1, 1), jnp.int32),
            pltpu.SMEM((1, 1), jnp.int32),
            dma((2,)),
        ],
        compiler_params=pltpu.CompilerParams(
            collective_id=0, has_side_effects=True, vmem_limit_bytes=60 * 1024 * 1024
        ),
        name="sweep_attention",
    )(
        queries,
        query_gain,
        cache_keys,
        cache_values,
        finished_keys,
        finished_values,
        new_keys,
        new_values,
        out_weight,
        time_weight,
        owner,
        step,
    )
    if aligned:
        return result
    summed = lax.psum_scatter(result, "head", scatter_dimension=1, tiled=True)
    half = freq // 2
    frequency = jnp.exp(-jnp.log(10000.0) * jnp.arange(half, dtype=F32) / half)
    phases = step[0, 0].astype(F32) * frequency
    embedding = jnp.concatenate([jnp.cos(phases), jnp.sin(phases)])
    time_gate = 1.0 + jnp.dot(embedding, time_weight, precision=lax.Precision.HIGHEST)
    return (time_gate * summed).astype(BF16)


def solution(mesh):
    in_specs = (
        P(("grp", "seq"), "head"),
        P("head"),
        P(("grp", "slab"), "head"),
        P(("grp", "slab"), "head"),
        P(("grp", "slab", "seq"), "head"),
        P(("grp", "slab", "seq"), "head"),
        P(("grp", "slab", "seq"), "head"),
        P(("grp", "slab", "seq"), "head"),
        P("head", "slab"),
        P(None, ("slab", "head")),
        P("grp", None),
        P("grp", None),
    )
    out_specs = P(("grp", "seq"), ("slab", "head"))
    sizes = (mesh.shape["slab"], mesh.shape["head"], mesh.shape["seq"])
    mapped = jax.shard_map(
        functools.partial(local, sizes),
        mesh=mesh,
        in_specs=in_specs,
        out_specs=out_specs,
        check_vma=False,
    )

    def run(*args):
        return mapped(*args[:-2], args[-2].reshape(-1, 1), args[-1].reshape(-1, 1))

    return run
```

```python
import functools
import math

import jax
import jax.numpy as jnp
from jax import lax
from jax.experimental import pallas as pl
from jax.experimental.pallas import tpu as pltpu
from jax.sharding import PartitionSpec as P

HEADS = 40
HD = 128
EPSILON = 1e-06
LOW = -1e30
LAG = 5
SPLIT = 2
PARTS = 1
MESH = pl.DeviceIdType.MESH
F32 = jnp.float32
BF16 = jnp.bfloat16


def kernel(
    dims,
    aligned,
    q_ref,
    gain_ref,
    ck_ref,
    cv_ref,
    fk_ref,
    fv_ref,
    nk_ref,
    nv_ref,
    w_ref,
    tw_ref,
    owner_hbm,
    step_hbm,
    out_ref,
    q,
    qg,
    gain,
    kc,
    vc,
    kf,
    vf,
    w,
    tw,
    squares,
    scale,
    own_o,
    own_s,
    pre_o,
    pre_s,
    suf_o,
    suf_s,
    right_o,
    right_s,
    left_o,
    left_s,
    att,
    acc,
    gate,
    xs,
    xr,
    load_sem,
    fresh_sem,
    fresh_send,
    fresh_recv,
    sq_send,
    sq_recv,
    right_send,
    right_recv,
    left_send,
    left_recv,
    x_send,
    x_recv,
    s_buf,
    p_buf,
    m_buf,
    q_sem,
    kv_sem,
    gauge,
    raw_o,
    raw_s,
    owner_ref,
    step_ref,
    scalar_sem,
):
    n, heads_n, seq_n = dims
    rows, width = q_ref.shape
    hcount = width // HD
    z = lax.axis_index("slab")
    hx = lax.axis_index("head")
    sq = lax.axis_index("seq")

    groups = rows // HD
    chunks = groups * hcount
    gain_load, w_load, tw_load = [
        pltpu.make_async_copy(src, dst, load_sem.at[i])
        for i, (src, dst) in enumerate([(gain_ref, gain), (w_ref, w), (tw_ref, tw)])
    ]
    ahead = min(max(hcount // 5, 3), hcount)
    parts = PARTS if hcount % PARTS == 0 else 1
    span = width // parts
    q_loads = []
    for g in range(groups):
        for k in range(parts):
            at = (slice(g * HD, (g + 1) * HD), slice(k * span, (k + 1) * span))
            q_loads.append(
                pltpu.make_async_copy(q_ref.at[at], q.at[at], q_sem.at[g * parts + k])
            )
    for c in q_loads:
        c.start()
    gain_load.start()
    scalars = [
        pltpu.make_async_copy(owner_hbm, owner_ref, scalar_sem.at[0]),
        pltpu.make_async_copy(step_hbm, step_ref, scalar_sem.at[1]),
    ]
    for c in scalars:
        c.start()
    barrier = pltpu.get_barrier_semaphore()
    for d in range(1, seq_n):
        pl.semaphore_signal(
            barrier, inc=1, device_id={"seq": lax.rem(sq + d, seq_n)}, device_id_type=MESH
        )
    for d in range(1, heads_n):
        pl.semaphore_signal(
            barrier, inc=1, device_id={"head": lax.rem(hx + d, heads_n)}, device_id_type=MESH
        )

    @pl.when(z > 0)
    def _():
        pl.semaphore_signal(barrier, inc=1, device_id={"slab": z - 1}, device_id_type=MESH)

    @pl.when(z < n - 1)
    def _():
        pl.semaphore_signal(barrier, inc=1, device_id={"slab": z + 1}, device_id_type=MESH)

    def clear(o_ref, s_ref):
        o_ref[...] = jnp.zeros_like(o_ref)
        s_ref[...] = jnp.full((chunks, 1, HD), LOW, F32)

    @pl.when(z == 0)
    def _():
        clear(pre_o, pre_s)

    @pl.when(z == n - 1)
    def _():
        clear(suf_o, suf_s)

    def squares_of(g):
        def step(h, total):
            x = q[g * HD : (g + 1) * HD, pl.ds(pl.multiple_of(h * HD, HD), HD)].astype(F32)
            return total + x * x

        total = jnp.zeros((HD, HD), F32)
        for k in range(parts):
            q_loads[g * parts + k].wait()
            total = lax.fori_loop(
                k * hcount // parts, (k + 1) * hcount // parts, step, total, unroll=True
            )
        squares[hx, g] = jnp.sum(total.T, axis=0, keepdims=True)

    squares_of(0)
    head_cut = ahead * HD
    kv_cuts = [slice(0, head_cut), slice(head_cut, width)] if head_cut < width else [slice(0, width)]
    kv_loads = []
    for k, cols in enumerate(kv_cuts):
        for i, (src, dst) in enumerate([(ck_ref, kc), (cv_ref, vc)]):
            kv_loads.append(pltpu.make_async_copy(src.at[:, cols], dst.at[:, cols], kv_sem.at[k, i]))
    fresh_src = [(fk_ref, kf, 0), (nk_ref, kf, 1), (fv_ref, vf, 0), (nv_ref, vf, 1)]

    ends = (z == 0).astype(jnp.int32) + (z == n - 1).astype(jnp.int32)
    pl.semaphore_wait(barrier, seq_n - 1 + heads_n - 1 + 2 - ends)

    sq_copies = []

    def squares_send(g):
        copies = []
        for d in range(1, heads_n):
            c = pltpu.make_async_remote_copy(
                src_ref=squares.at[hx, g],
                dst_ref=squares.at[hx, g],
                send_sem=sq_send.at[d - 1, g],
                recv_sem=sq_recv.at[d - 1, g],
                device_id={"head": lax.rem(hx + d, heads_n)},
                device_id_type=MESH,
            )
            c.start()
            copies.append(c)
        sq_copies.append(copies)

    squares_send(0)
    for c in kv_loads[:2]:
        c.start()
    for g in range(1, groups):
        squares_of(g)
        squares_send(g)
    tw_load.start()
    for c in kv_loads[2:]:
        c.start()
    fresh_local = []
    for i, (src, dst, part) in enumerate(fresh_src):
        pltpu.make_async_copy(src, dst.at[sq, part], fresh_sem.at[i // 2]).start()
    for side, whole in enumerate((kf, vf)):
        fresh_local.append(pltpu.make_async_copy(whole.at[sq], whole.at[sq], fresh_sem.at[side]))

    edges = [0, ahead * HD, width] if ahead < hcount else [0, width]
    cuts = [slice(a, b) for a, b in zip(edges, edges[1:])]
    fresh_remote = [[] for _ in cuts]

    def fresh_wait(d, side, cols, k=0):
        whole = (kf, vf)[side].at[sq, :, :, cols]
        return pltpu.make_async_remote_copy(
            src_ref=whole,
            dst_ref=whole,
            send_sem=fresh_send.at[d - 1, side],
            recv_sem=fresh_recv.at[d - 1, k, side],
            device_id={"seq": lax.rem(sq + d, seq_n)},
            device_id_type=MESH,
        )

    for k, cols in enumerate(cuts):
        for d in range(1, seq_n):
            for i, (src, dst, part) in enumerate(fresh_src):
                pltpu.make_async_remote_copy(
                    src_ref=src.at[:, cols],
                    dst_ref=dst.at[sq, part, :, cols],
                    send_sem=fresh_send.at[d - 1, i // 2],
                    recv_sem=fresh_recv.at[d - 1, k, i // 2],
                    device_id={"seq": lax.rem(sq + d, seq_n)},
                    device_id_type=MESH,
                ).start()
            fresh_remote[k] += [fresh_wait(d, side, cols, k) for side in (0, 1)]

    gain_load.wait()

    def gain_step(h, carry):
        cols = pl.ds(pl.multiple_of(h * HD, HD), HD)
        qg[:, cols] = (q[:, cols].astype(F32) * gain[cols][None, :]).astype(BF16)
        return carry

    lax.fori_loop(0, hcount, gain_step, 0)
    tw_load.wait()
    for c in scalars:
        c.wait()
    if aligned:
        half = tw.shape[0] // 2
        j = lax.broadcasted_iota(jnp.int32, (half, HD), 0).astype(F32)
        frequency = jnp.exp(F32(-math.log(10000.0)) * j / half)
        phases = jnp.full((half, HD), step_ref[0, 0], jnp.int32).astype(F32) * frequency
        cos, sin = jnp.cos(phases), jnp.sin(phases)
        for c in range(tw.shape[1] // HD):
            cols = slice(c * HD, (c + 1) * HD)
            terms = tw[:half, cols] * cos + tw[half:, cols] * sin
            gate[:, cols] = 1.0 + jnp.sum(terms, axis=0, keepdims=True)


    ring = min(chunks, LAG * (n - 1) + 1)

    def send(h, direction):
        if direction > 0:
            pairs, ss, rs = ((right_o, pre_o), (right_s, pre_s)), right_send, right_recv
        else:
            pairs, ss, rs = ((left_o, suf_o), (left_s, suf_s)), left_send, left_recv
        return [
            pltpu.make_async_remote_copy(
                src_ref=src.at[h],
                dst_ref=dst.at[h],
                send_sem=ss.at[i],
                recv_sem=rs.at[lax.rem(h, ring)],
                device_id={"slab": z + direction},
                device_id_type=MESH,
            )
            for i, (src, dst) in enumerate(pairs)
        ]

    def arrived(h, direction):
        ss, rs = (right_send, right_recv) if direction > 0 else (left_send, left_recv)
        pltpu.make_async_remote_copy(
            src_ref=gauge,
            dst_ref=gauge,
            send_sem=ss.at[0],
            recv_sem=rs.at[lax.rem(h, ring)],
            device_id={"slab": z - direction},
            device_id_type=MESH,
        ).wait_recv()

    def settle_sends(direction):
        if direction > 0:
            pairs, ss, rs = ((right_o, pre_o), (right_s, pre_s)), right_send, right_recv
        else:
            pairs, ss, rs = ((left_o, suf_o), (left_s, suf_s)), left_send, left_recv
        for i, (src, dst) in enumerate(pairs):
            pltpu.make_async_remote_copy(
                src_ref=src,
                dst_ref=dst,
                send_sem=ss.at[i],
                recv_sem=rs.at[0],
                device_id={"slab": z + direction},
                device_id_type=MESH,
            ).wait_send()

    pair = 2 if hcount % 2 == 0 else 1
    splits = next(k for k in (SPLIT, 2, 1) if hcount % k == 0)
    sub = HD // splits
    tuples = hcount // splits
    pairs = hcount // pair
    last = (groups - 1) * hcount
    fresh_rows = seq_n * 2 * fk_ref.shape[0]
    lag_end = LAG * jnp.maximum(z, n - 1 - z)

    def combine(h, other_o, other_s, dest_o, dest_s):
        l_a, l_b = own_s[h], other_s[h]
        top = jnp.maximum(l_a, l_b)
        e_a, e_b = jnp.exp2(l_a - top), jnp.exp2(l_b - top)
        mass = e_a + e_b
        share = 1.0 / mass
        dest_o[h] = (
            own_o[h] * (e_a * share) + other_o[h].astype(F32) * (e_b * share)
        ).astype(BF16)
        dest_s[h] = top + jnp.log2(mass)

    nt = (((1,), (1,)), ((), ()))
    tn = (((0,), (0,)), ((), ()))

    penalty = jnp.where(
        jnp.full((1, rows), owner_ref[0, 0], jnp.int32) == z, F32(LOW), F32(0.0)
    )
    cached = kc.shape[0]
    step_keys = 256 if cached % 256 == 0 else cached
    blocks = [(i, i + step_keys) for i in range(0, cached, step_keys)]

    def head_cols(h):
        return pl.ds(pl.multiple_of(h * HD, HD), HD)

    def scores(h, slot):
        cols = head_cols(h)
        q_head = qg[:, cols]
        top = None
        for a, b in blocks:
            part = lax.dot_general(kc[a:b, cols], q_head, nt, preferred_element_type=F32)
            s_buf[slot, a:b, :] = part
            high = jnp.max(part, axis=0, keepdims=True)
            top = high if top is None else jnp.maximum(top, high)
        k_fresh = kf[:, :, :, cols].reshape(fresh_rows, HD)
        part = lax.dot_general(k_fresh, q_head, nt, preferred_element_type=F32)
        s_buf[slot, cached:, :] = part
        m_buf[slot, 0:1, :] = top
        m_buf[slot, 1:2, :] = jnp.max(part, axis=0, keepdims=True)

    def soften(slot, r=slice(None)):
        s_row = scale[0:1, r]
        mask = penalty[:, r]
        top = jnp.maximum(m_buf[slot, 0:1, r] * s_row + mask, m_buf[slot, 1:2, r] * s_row)
        top_c = top - mask
        mass = jnp.zeros_like(top)
        for a, b in blocks + [(cached, cached + fresh_rows)]:
            p = jnp.exp2(s_buf[slot, a:b, r] * s_row - (top_c if a < cached else top))
            p_buf[slot, a:b, r] = p.astype(BF16)
            mass = mass + jnp.sum(p, axis=0, keepdims=True)
        m_buf[slot, 2:3, r] = 1.0 / mass
        m_buf[slot, 3:4, r] = top + jnp.log2(mass)

    packed = splits > 1

    def pack(c):
        k = c - last
        s, p = lax.div(k, tuples), lax.rem(k, tuples)
        seat_o = lax.broadcasted_iota(jnp.int32, (HD, HD), 1) // sub
        seat_s = lax.broadcasted_iota(jnp.int32, (1, HD), 1) // sub
        value, stats = jnp.zeros((HD, HD), F32), jnp.zeros((1, HD), F32)
        for i in range(splits):
            turn = lax.rem((i - s + splits) * sub, HD)
            value = jnp.where(seat_o == i, pltpu.roll(raw_o[p * splits + i], turn, 1), value)
            stats = jnp.where(seat_s == i, pltpu.roll(raw_s[p * splits + i], turn, 1), stats)
        own_o[c] = value
        own_s[c] = stats

    def weigh(h, slot, first=0, end=None):
        cols = head_cols(h)
        end = groups if end is None else end
        r = slice(first * HD, end * HD)
        v_fresh = vf[:, :, :, cols].reshape(fresh_rows, HD)
        o = lax.dot_general(v_fresh, p_buf[slot, cached:, r], tn, preferred_element_type=F32)
        for a, b in blocks:
            o += lax.dot_general(
                vc[a:b, cols], p_buf[slot, a:b, r], tn, preferred_element_type=F32
            )

        o = o * m_buf[slot, 2:3, r]

        for g in range(first, end):
            to_o, to_s, at = own_o, own_s, g * hcount + h
            if packed and g == groups - 1:
                to_o, to_s, at = raw_o, raw_s, h
            to_o[at] = o[:, (g - first) * HD : (g - first + 1) * HD]
            to_s[at] = m_buf[slot, 3:4, g * HD : (g + 1) * HD]

    def project(g, p):
        deep = pl.ds(pl.multiple_of(p * pair * HD, HD), pair * HD)
        term = lax.dot_general(att[g, deep, :], w[deep, :], tn, preferred_element_type=F32)
        add(acc.at[g * HD : (g + 1) * HD, :], term, p)

    def project_last(s, p):
        deep = pl.ds(pl.multiple_of(p * splits * HD, HD), splits * HD)
        term = lax.dot_general(
            att[groups - 1 + s, deep, 0:sub], w[deep, :], tn, preferred_element_type=F32
        )
        add(acc.at[(groups - 1) * HD + s * sub : (groups - 1) * HD + (s + 1) * sub, :], term, p)

    def add(dest, term, p):
        @pl.when(p == 0)
        def _():
            dest[...] = term

        @pl.when(p > 0)
        def _():
            dest[...] += term

    pieces = [(g * HD, (g + 1) * HD) for g in range(groups - 1)]
    pieces += [((groups - 1) * HD + s * sub, (groups - 1) * HD + (s + 1) * sub) for s in range(splits)]

    def exchange(k):
        a, b = pieces[k]
        copies = []
        for d in range(1, heads_n):
            copies.append(
                pltpu.make_async_remote_copy(
                    src_ref=xs.at[d - 1, a:b],
                    dst_ref=xr.at[d - 1, a:b],
                    send_sem=x_send.at[d - 1],
                    recv_sem=x_recv.at[d - 1, k],
                    device_id={"head": lax.rem(hx + d, heads_n)},
                    device_id_type=MESH,
                )
            )
        return copies

    def exchange_start(k):
        a, b = pieces[k]
        cp = out_ref.shape[1]
        for d, c in enumerate(exchange(k)):
            peer = lax.rem(hx + d + 1, heads_n)
            cols = pl.ds(pl.multiple_of(peer * cp, HD), cp)
            xs[d, a:b] = acc[a:b, cols].astype(BF16)
            c.start()

    def service(t):
        cp_ = t - LAG * z
        in_p = (cp_ >= 0) & (cp_ < chunks)
        cs = t - LAG * (n - 1 - z)
        in_s = (cs >= 0) & (cs < chunks)

        @pl.when(in_p & (z > 0))
        def _():
            arrived(cp_, 1)

        @pl.when(in_p & (z < n - 1))
        def _():
            combine(cp_, pre_o, pre_s, right_o, right_s)
            for c in send(cp_, 1)[::-1]:
                c.start()

        @pl.when(in_s & (z < n - 1))
        def _():
            arrived(cs, -1)

        @pl.when(in_s & (z > 0))
        def _():
            combine(cs, suf_o, suf_s, left_o, left_s)
            for c in send(cs, -1)[::-1]:
                c.start()

    def finish(t):
        f = t - lag_end

        @pl.when((f >= 0) & (f < chunks))
        def _():
            m_a, m_b, m_c = own_s[f], pre_s[f], suf_s[f]
            top = jnp.maximum(m_a, jnp.maximum(m_b, m_c))
            e_a, e_b, e_c = jnp.exp2(m_a - top), jnp.exp2(m_b - top), jnp.exp2(m_c - top)
            share = 1.0 / (e_a + e_b + e_c)
            total_o = (
                own_o[f] * (e_a * share)
                + pre_o[f].astype(F32) * (e_b * share)
                + suf_o[f].astype(F32) * (e_c * share)
            )
            value = total_o.astype(BF16)

            @pl.when(f < last)
            def _():
                h = lax.rem(f, hcount)
                att[f // hcount, head_cols(h), :] = value

            @pl.when(f >= last)
            def _():
                k = f - last
                s, p = lax.div(k, tuples), lax.rem(k, tuples)
                for i in range(splits):
                    turned = value if i == 0 else pltpu.roll(total_o, HD - i * sub, 1).astype(BF16)
                    att[groups - 1 + s, head_cols(p * splits + i), :] = turned

        @pl.when(f == hcount - pairs)
        def _():
            w_load.wait()

        for g in range(groups - 1):
            begin = (g + 1) * hcount - pairs

            @pl.when((f >= begin) & (f < begin + pairs))
            def _(g=g, begin=begin):
                project(g, f - begin)

            if aligned:

                @pl.when(f == begin + pairs - 1)
                def _(g=g):
                    exchange_start(g)

        for s in range(splits):
            begin = last + s * tuples

            stop = begin + tuples - (1 if aligned and s == splits - 1 else 0)

            @pl.when((f >= begin) & (f < stop))
            def _(s=s, begin=begin):
                project_last(s, f - begin)

            if aligned and s < splits - 1:

                @pl.when(f == begin + tuples - 1)
                def _(s=s):
                    exchange_start(groups - 1 + s)

        if aligned:

            @pl.when(f == chunks - 1)
            def _():
                a, b = pieces[-1]
                cp = out_ref.shape[1]
                deep = slice((tuples - 1) * splits * HD, tuples * splits * HD)
                sums = att[groups + splits - 2, deep, 0:sub]

                def total_of(owner):
                    cols = pl.ds(pl.multiple_of(owner * cp, HD), cp)
                    before = 0.0 if tuples == 1 else acc[a:b, cols]
                    return cols, before + lax.dot_general(
                        sums, w[deep, cols], tn, preferred_element_type=F32
                    )

                for d, c in enumerate(exchange(len(pieces) - 1)):
                    xs[d, a:b] = total_of(lax.rem(hx + d + 1, heads_n))[1].astype(BF16)
                    c.start()
                cols, own = total_of(hx)
                acc[a:b, cols] = own

    def near(h):
        return jnp.minimum(h, hcount - 1)

    kv_loads[0].wait()
    for c in fresh_local:
        c.wait()
    for c in fresh_remote[0]:
        c.wait_recv()
    scores(0, 0)
    scores(min(1, hcount - 1), 1)
    def rescale(g):
        for c in sq_copies[g]:
            c.wait_recv()
        norm_total = squares[0, g]
        for d in range(1, heads_n):
            norm_total = norm_total + squares[d, g]
        scale[0:1, g * HD : (g + 1) * HD] = lax.rsqrt(norm_total / (HEADS * HD) + EPSILON) * (
            math.log2(math.e) / HD**0.5
        )

    rescale(0)
    soften(0, slice(0, HD))
    kv_loads[1].wait()
    weigh(0, 0, 0, 1)
    service(0)
    w_load.start()
    early = hcount > 1 and groups > 1
    if early:
        soften(1, slice(0, HD))
        weigh(1, 1, 0, 1)
        service(1)
    for g in range(1, groups):
        rescale(g)
    if groups > 1:
        soften(0, slice(HD, rows))
        weigh(0, 0, 1, groups)
    soften(1, slice(HD, rows) if early else slice(None))
    scores(min(2, hcount - 1), 0)

    unroll = 2

    def body(i, carry):
        for u in range(unroll):
            t = unroll * i + u
            if len(cuts) > 1:

                @pl.when(t + 3 == ahead)
                def _():
                    for c in fresh_remote[1]:
                        c.wait_recv()
                    for c in kv_loads[2:]:
                        c.wait()

            @pl.when(t + 1 < hcount)
            def _(t=t, u=u):
                scores(near(t + 3), (u + 1) % 2)
                soften(u % 2)
                weigh(t + 1, (u + 1) % 2)

            if packed:
                c = t + 1 + tuples

                @pl.when((c >= last) & (c < chunks))
                def _(c=c):
                    pack(c)

            finish(t)
            if early and u == 0:

                @pl.when(t > 0)
                def _(t=t):
                    service(t + 1)

            else:
                service(t + 1)
        return carry

    lax.fori_loop(0, -(-(chunks + LAG * (n - 1)) // unroll), body, 0)

    def settle():
        for d in range(1, seq_n):
            for side in (0, 1):
                fresh_wait(d, side, slice(0, width)).wait_send()
        for c in [c for copies in sq_copies for c in copies]:
            c.wait_send()

        @pl.when(z < n - 1)
        def _():
            settle_sends(1)

        @pl.when(z > 0)
        def _():
            settle_sends(-1)

    if aligned:
        cp = out_ref.shape[1]
        mine = pl.ds(pl.multiple_of(hx * cp, HD), cp)
        settle()
        for k, (a, b) in enumerate(pieces):
            summed = acc[a:b, mine]
            for d, c in enumerate(exchange(k)):
                c.wait_recv()
                summed = summed + xr[d, a:b].astype(F32)
            out_ref[a:b, :] = (summed * gate[...]).astype(out_ref.dtype)
        for d in range(1, heads_n):
            pltpu.make_async_remote_copy(
                src_ref=xs.at[d - 1],
                dst_ref=xr.at[d - 1],
                send_sem=x_send.at[d - 1],
                recv_sem=x_recv.at[d - 1, 0],
                device_id={"head": lax.rem(hx + d, heads_n)},
                device_id_type=MESH,
            ).wait_send()
    else:
        out_ref[...] = acc[...]
        settle()


def local(sizes, *args):
    (
        queries,
        query_gain,
        cache_keys,
        cache_values,
        finished_keys,
        finished_values,
        new_keys,
        new_values,
        out_weight,
        time_weight,
        owner,
        step,
    ) = args
    n, heads_n, seq_n = sizes
    rows, width = queries.shape
    hcount = width // HD
    cached, fresh = cache_keys.shape[0], finished_keys.shape[0]
    columns, cp = out_weight.shape[1], time_weight.shape[1]
    freq = time_weight.shape[0]
    aligned = cp % HD == 0
    any_spec = pl.BlockSpec(memory_space=pl.ANY)
    vmem = pl.BlockSpec(memory_space=pltpu.VMEM)
    dma = pltpu.SemaphoreType.DMA
    xcount = max(heads_n - 1, 1)
    groups = rows // HD
    chunks = groups * hcount
    ring = min(chunks, LAG * (n - 1) + 1)
    stat = (chunks, 1, HD)
    keys = cached + seq_n * 2 * fresh
    part = (chunks, HD, HD)
    result = pl.pallas_call(
        functools.partial(kernel, sizes, aligned),
        out_shape=pltpu.VMEM((rows, cp), BF16) if aligned else jax.ShapeDtypeStruct((rows, columns), F32),
        in_specs=[any_spec] * 12,
        out_specs=vmem,
        scratch_shapes=[
            pltpu.VMEM((rows, width), BF16),
            pltpu.VMEM((rows, width), BF16),
            pltpu.VMEM((width,), F32),
            pltpu.VMEM((cached, width), BF16),
            pltpu.VMEM((cached, width), BF16),
            pltpu.VMEM((seq_n, 2, fresh, width), BF16),
            pltpu.VMEM((seq_n, 2, fresh, width), BF16),
            pltpu.VMEM((width, columns), BF16),
            pltpu.VMEM((freq, cp), F32),
            pltpu.VMEM((heads_n, groups, 1, HD), F32),
            pltpu.VMEM((1, rows), F32),
            pltpu.VMEM(part, F32),
            pltpu.VMEM(stat, F32),
            pltpu.VMEM(part, BF16),
            pltpu.VMEM(stat, F32),
            pltpu.VMEM(part, BF16),
            pltpu.VMEM(stat, F32),
            pltpu.VMEM(part, BF16),
            pltpu.VMEM(stat, F32),
            pltpu.VMEM(part, BF16),
            pltpu.VMEM(stat, F32),
            pltpu.VMEM((groups + SPLIT - 1, width, HD), BF16),
            pltpu.VMEM((rows, columns), F32),
            pltpu.VMEM((1, cp), F32),
            pltpu.VMEM((xcount, rows, cp), BF16),
            pltpu.VMEM((xcount, rows, cp), BF16),
            dma((3,)),
            dma((2,)),
            dma((max(seq_n - 1, 1), 2)),
            dma((max(seq_n - 1, 1), 2, 2)),
            dma((xcount, groups)),
            dma((xcount, groups)),
            dma((2,)),
            dma((ring,)),
            dma((2,)),
            dma((ring,)),
            dma((xcount,)),
            dma((xcount, groups + SPLIT - 1)),
            pltpu.VMEM((2, keys, rows), F32),
            pltpu.VMEM((2, keys, rows), BF16),
            pltpu.VMEM((2, 4, rows), F32),
            dma((groups * PARTS,)),
            dma((2, 2)),
            pltpu.VMEM((HD // 2 + 1, 1, HD), F32),
            pltpu.VMEM((hcount, HD, HD), F32),
            pltpu.VMEM((hcount, 1, HD), F32),
            pltpu.SMEM((1, 1), jnp.int32),
            pltpu.SMEM((1, 1), jnp.int32),
            dma((2,)),
        ],
        compiler_params=pltpu.CompilerParams(
            collective_id=0, has_side_effects=True, vmem_limit_bytes=60 * 1024 * 1024
        ),
        name="sweep_attention",
    )(
        queries,
        query_gain,
        cache_keys,
        cache_values,
        finished_keys,
        finished_values,
        new_keys,
        new_values,
        out_weight,
        time_weight,
        owner,
        step,
    )
    if aligned:
        return result
    summed = lax.psum_scatter(result, "head", scatter_dimension=1, tiled=True)
    half = freq // 2
    frequency = jnp.exp(-jnp.log(10000.0) * jnp.arange(half, dtype=F32) / half)
    phases = step[0, 0].astype(F32) * frequency
    embedding = jnp.concatenate([jnp.cos(phases), jnp.sin(phases)])
    time_gate = 1.0 + jnp.dot(embedding, time_weight, precision=lax.Precision.HIGHEST)
    return (time_gate * summed).astype(BF16)


def solution(mesh):
    in_specs = (
        P(("grp", "seq"), "head"),
        P("head"),
        P(("grp", "slab"), "head"),
        P(("grp", "slab"), "head"),
        P(("grp", "slab", "seq"), "head"),
        P(("grp", "slab", "seq"), "head"),
        P(("grp", "slab", "seq"), "head"),
        P(("grp", "slab", "seq"), "head"),
        P("head", "slab"),
        P(None, ("slab", "head")),
        P("grp", None),
        P("grp", None),
    )
    out_specs = P(("grp", "seq"), ("slab", "head"))
    sizes = (mesh.shape["slab"], mesh.shape["head"], mesh.shape["seq"])
    mapped = jax.shard_map(
        functools.partial(local, sizes),
        mesh=mesh,
        in_specs=in_specs,
        out_specs=out_specs,
        check_vma=False,
    )

    def run(*args):
        return mapped(*args[:-2], args[-2].reshape(-1, 1), args[-1].reshape(-1, 1))

    return run
```

```python
import functools
import math

import jax
import jax.numpy as jnp
from jax import lax
from jax.experimental import pallas as pl
from jax.experimental.pallas import tpu as pltpu
from jax.sharding import PartitionSpec as P

HEADS = 40
HD = 128
EPSILON = 1e-06
LOW = -1e30
LAG = 5
SPLIT = 2
PARTS = 1
MESH = pl.DeviceIdType.MESH
F32 = jnp.float32
BF16 = jnp.bfloat16


def kernel(
    dims,
    aligned,
    q_ref,
    gain_ref,
    ck_ref,
    cv_ref,
    fk_ref,
    fv_ref,
    nk_ref,
    nv_ref,
    w_ref,
    tw_ref,
    owner_hbm,
    step_hbm,
    out_ref,
    q,
    qg,
    gain,
    kc,
    vc,
    kf,
    vf,
    w,
    tw,
    squares,
    scale,
    own_o,
    own_s,
    pre_o,
    pre_s,
    suf_o,
    suf_s,
    right_o,
    right_s,
    left_o,
    left_s,
    att,
    acc,
    gate,
    xs,
    xr,
    load_sem,
    fresh_sem,
    fresh_send,
    fresh_recv,
    sq_send,
    sq_recv,
    right_send,
    right_recv,
    left_send,
    left_recv,
    x_send,
    x_recv,
    s_buf,
    p_buf,
    m_buf,
    q_sem,
    kv_sem,
    gauge,
    raw_o,
    raw_s,
    owner_ref,
    step_ref,
    scalar_sem,
):
    n, heads_n, seq_n = dims
    rows, width = q_ref.shape
    hcount = width // HD
    z = lax.axis_index("slab")
    hx = lax.axis_index("head")
    sq = lax.axis_index("seq")

    groups = rows // HD
    chunks = groups * hcount
    gain_load, w_load, tw_load = [
        pltpu.make_async_copy(src, dst, load_sem.at[i])
        for i, (src, dst) in enumerate([(gain_ref, gain), (w_ref, w), (tw_ref, tw)])
    ]
    ahead = min(max(hcount // 5, 3), hcount)
    parts = PARTS if hcount % PARTS == 0 else 1
    span = width // parts
    q_loads = []
    for g in range(groups):
        for k in range(parts):
            at = (slice(g * HD, (g + 1) * HD), slice(k * span, (k + 1) * span))
            q_loads.append(
                pltpu.make_async_copy(q_ref.at[at], q.at[at], q_sem.at[g * parts + k])
            )
    for c in q_loads:
        c.start()
    gain_load.start()
    scalars = [
        pltpu.make_async_copy(owner_hbm, owner_ref, scalar_sem.at[0]),
        pltpu.make_async_copy(step_hbm, step_ref, scalar_sem.at[1]),
    ]
    for c in scalars:
        c.start()
    barrier = pltpu.get_barrier_semaphore()
    for d in range(1, seq_n):
        pl.semaphore_signal(
            barrier, inc=1, device_id={"seq": lax.rem(sq + d, seq_n)}, device_id_type=MESH
        )
    for d in range(1, heads_n):
        pl.semaphore_signal(
            barrier, inc=1, device_id={"head": lax.rem(hx + d, heads_n)}, device_id_type=MESH
        )

    @pl.when(z > 0)
    def _():
        pl.semaphore_signal(barrier, inc=1, device_id={"slab": z - 1}, device_id_type=MESH)

    @pl.when(z < n - 1)
    def _():
        pl.semaphore_signal(barrier, inc=1, device_id={"slab": z + 1}, device_id_type=MESH)

    def clear(o_ref, s_ref):
        o_ref[...] = jnp.zeros_like(o_ref)
        s_ref[...] = jnp.full((chunks, 1, HD), LOW, F32)

    @pl.when(z == 0)
    def _():
        clear(pre_o, pre_s)

    @pl.when(z == n - 1)
    def _():
        clear(suf_o, suf_s)

    def squares_of(g):
        def step(h, total):
            x = q[g * HD : (g + 1) * HD, pl.ds(pl.multiple_of(h * HD, HD), HD)].astype(F32)
            return total + x * x

        total = jnp.zeros((HD, HD), F32)
        for k in range(parts):
            q_loads[g * parts + k].wait()
            total = lax.fori_loop(
                k * hcount // parts, (k + 1) * hcount // parts, step, total, unroll=True
            )
        squares[hx, g] = jnp.sum(total.T, axis=0, keepdims=True)

    squares_of(0)
    head_cut = ahead * HD
    kv_cuts = [slice(0, head_cut), slice(head_cut, width)] if head_cut < width else [slice(0, width)]
    kv_loads = []
    for k, cols in enumerate(kv_cuts):
        for i, (src, dst) in enumerate([(ck_ref, kc), (cv_ref, vc)]):
            kv_loads.append(pltpu.make_async_copy(src.at[:, cols], dst.at[:, cols], kv_sem.at[k, i]))
    fresh_src = [(fk_ref, kf, 0), (nk_ref, kf, 1), (fv_ref, vf, 0), (nv_ref, vf, 1)]

    ends = (z == 0).astype(jnp.int32) + (z == n - 1).astype(jnp.int32)
    pl.semaphore_wait(barrier, seq_n - 1 + heads_n - 1 + 2 - ends)

    sq_copies = []

    def squares_send(g):
        copies = []
        for d in range(1, heads_n):
            c = pltpu.make_async_remote_copy(
                src_ref=squares.at[hx, g],
                dst_ref=squares.at[hx, g],
                send_sem=sq_send.at[d - 1, g],
                recv_sem=sq_recv.at[d - 1, g],
                device_id={"head": lax.rem(hx + d, heads_n)},
                device_id_type=MESH,
            )
            c.start()
            copies.append(c)
        sq_copies.append(copies)

    squares_send(0)
    for c in kv_loads[:2]:
        c.start()
    for g in range(1, groups):
        squares_of(g)
        squares_send(g)
    tw_load.start()
    for c in kv_loads[2:]:
        c.start()
    fresh_local = []
    for i, (src, dst, part) in enumerate(fresh_src):
        pltpu.make_async_copy(src, dst.at[sq, part], fresh_sem.at[i // 2]).start()
    for side, whole in enumerate((kf, vf)):
        fresh_local.append(pltpu.make_async_copy(whole.at[sq], whole.at[sq], fresh_sem.at[side]))

    edges = [0, ahead * HD, width] if ahead < hcount else [0, width]
    cuts = [slice(a, b) for a, b in zip(edges, edges[1:])]
    fresh_remote = [[] for _ in cuts]

    def fresh_wait(d, side, cols, k=0):
        whole = (kf, vf)[side].at[sq, :, :, cols]
        return pltpu.make_async_remote_copy(
            src_ref=whole,
            dst_ref=whole,
            send_sem=fresh_send.at[d - 1, side],
            recv_sem=fresh_recv.at[d - 1, k, side],
            device_id={"seq": lax.rem(sq + d, seq_n)},
            device_id_type=MESH,
        )

    for k, cols in enumerate(cuts):
        for d in range(1, seq_n):
            for i, (src, dst, part) in enumerate(fresh_src):
                pltpu.make_async_remote_copy(
                    src_ref=src.at[:, cols],
                    dst_ref=dst.at[sq, part, :, cols],
                    send_sem=fresh_send.at[d - 1, i // 2],
                    recv_sem=fresh_recv.at[d - 1, k, i // 2],
                    device_id={"seq": lax.rem(sq + d, seq_n)},
                    device_id_type=MESH,
                ).start()
            fresh_remote[k] += [fresh_wait(d, side, cols, k) for side in (0, 1)]

    gain_load.wait()

    def gain_step(h, carry):
        cols = pl.ds(pl.multiple_of(h * HD, HD), HD)
        qg[:, cols] = (q[:, cols].astype(F32) * gain[cols][None, :]).astype(BF16)
        return carry

    lax.fori_loop(0, hcount, gain_step, 0)
    tw_load.wait()
    for c in scalars:
        c.wait()
    if aligned:
        half = tw.shape[0] // 2
        j = lax.broadcasted_iota(jnp.int32, (half, HD), 0).astype(F32)
        frequency = jnp.exp(F32(-math.log(10000.0)) * j / half)
        phases = jnp.full((half, HD), step_ref[0, 0], jnp.int32).astype(F32) * frequency
        cos, sin = jnp.cos(phases), jnp.sin(phases)
        for c in range(tw.shape[1] // HD):
            cols = slice(c * HD, (c + 1) * HD)
            terms = tw[:half, cols] * cos + tw[half:, cols] * sin
            gate[:, cols] = 1.0 + jnp.sum(terms, axis=0, keepdims=True)


    ring = min(chunks, LAG * (n - 1) + 1)

    def send(h, direction):
        if direction > 0:
            pairs, ss, rs = ((right_o, pre_o), (right_s, pre_s)), right_send, right_recv
        else:
            pairs, ss, rs = ((left_o, suf_o), (left_s, suf_s)), left_send, left_recv
        return [
            pltpu.make_async_remote_copy(
                src_ref=src.at[h],
                dst_ref=dst.at[h],
                send_sem=ss.at[i],
                recv_sem=rs.at[lax.rem(h, ring)],
                device_id={"slab": z + direction},
                device_id_type=MESH,
            )
            for i, (src, dst) in enumerate(pairs)
        ]

    def arrived(h, direction):
        ss, rs = (right_send, right_recv) if direction > 0 else (left_send, left_recv)
        pltpu.make_async_remote_copy(
            src_ref=gauge,
            dst_ref=gauge,
            send_sem=ss.at[0],
            recv_sem=rs.at[lax.rem(h, ring)],
            device_id={"slab": z - direction},
            device_id_type=MESH,
        ).wait_recv()

    def settle_sends(direction):
        if direction > 0:
            pairs, ss, rs = ((right_o, pre_o), (right_s, pre_s)), right_send, right_recv
        else:
            pairs, ss, rs = ((left_o, suf_o), (left_s, suf_s)), left_send, left_recv
        for i, (src, dst) in enumerate(pairs):
            pltpu.make_async_remote_copy(
                src_ref=src,
                dst_ref=dst,
                send_sem=ss.at[i],
                recv_sem=rs.at[0],
                device_id={"slab": z + direction},
                device_id_type=MESH,
            ).wait_send()

    pair = 2 if hcount % 2 == 0 else 1
    splits = next(k for k in (SPLIT, 2, 1) if hcount % k == 0)
    sub = HD // splits
    tuples = hcount // splits
    pairs = hcount // pair
    last = (groups - 1) * hcount
    fresh_rows = seq_n * 2 * fk_ref.shape[0]
    lag_end = LAG * jnp.maximum(z, n - 1 - z)

    def combine(h, other_o, other_s, dest_o, dest_s):
        l_a, l_b = own_s[h], other_s[h]
        top = jnp.maximum(l_a, l_b)
        e_a, e_b = jnp.exp2(l_a - top), jnp.exp2(l_b - top)
        mass = e_a + e_b
        share = 1.0 / mass
        dest_o[h] = (
            own_o[h] * (e_a * share) + other_o[h].astype(F32) * (e_b * share)
        ).astype(BF16)
        dest_s[h] = top + jnp.log2(mass)

    nt = (((1,), (1,)), ((), ()))
    tn = (((0,), (0,)), ((), ()))

    penalty = jnp.where(
        jnp.full((1, rows), owner_ref[0, 0], jnp.int32) == z, F32(LOW), F32(0.0)
    )
    cached = kc.shape[0]
    step_keys = 256 if cached % 256 == 0 else cached
    blocks = [(i, i + step_keys) for i in range(0, cached, step_keys)]

    def head_cols(h):
        return pl.ds(pl.multiple_of(h * HD, HD), HD)

    def scores(h, slot):
        cols = head_cols(h)
        q_head = qg[:, cols]
        top = None
        for a, b in blocks:
            part = lax.dot_general(kc[a:b, cols], q_head, nt, preferred_element_type=F32)
            s_buf[slot, a:b, :] = part
            high = jnp.max(part, axis=0, keepdims=True)
            top = high if top is None else jnp.maximum(top, high)
        k_fresh = kf[:, :, :, cols].reshape(fresh_rows, HD)
        part = lax.dot_general(k_fresh, q_head, nt, preferred_element_type=F32)
        s_buf[slot, cached:, :] = part
        m_buf[slot, 0:1, :] = top
        m_buf[slot, 1:2, :] = jnp.max(part, axis=0, keepdims=True)

    def soften(slot, r=slice(None)):
        s_row = scale[0:1, r]
        mask = penalty[:, r]
        top = jnp.maximum(m_buf[slot, 0:1, r] * s_row + mask, m_buf[slot, 1:2, r] * s_row)
        top_c = top - mask
        mass = jnp.zeros_like(top)
        for a, b in blocks + [(cached, cached + fresh_rows)]:
            p = jnp.exp2(s_buf[slot, a:b, r] * s_row - (top_c if a < cached else top))
            p_buf[slot, a:b, r] = p.astype(BF16)
            mass = mass + jnp.sum(p, axis=0, keepdims=True)
        m_buf[slot, 2:3, r] = 1.0 / mass
        m_buf[slot, 3:4, r] = top + jnp.log2(mass)

    packed = splits > 1

    def pack(c):
        k = c - last
        s, p = lax.div(k, tuples), lax.rem(k, tuples)
        seat_o = lax.broadcasted_iota(jnp.int32, (HD, HD), 1) // sub
        seat_s = lax.broadcasted_iota(jnp.int32, (1, HD), 1) // sub
        value, stats = jnp.zeros((HD, HD), F32), jnp.zeros((1, HD), F32)
        for i in range(splits):
            turn = lax.rem((i - s + splits) * sub, HD)
            value = jnp.where(seat_o == i, pltpu.roll(raw_o[p * splits + i], turn, 1), value)
            stats = jnp.where(seat_s == i, pltpu.roll(raw_s[p * splits + i], turn, 1), stats)
        own_o[c] = value
        own_s[c] = stats

    def weigh(h, slot, first=0, end=None):
        cols = head_cols(h)
        end = groups if end is None else end
        r = slice(first * HD, end * HD)
        v_fresh = vf[:, :, :, cols].reshape(fresh_rows, HD)
        o = lax.dot_general(v_fresh, p_buf[slot, cached:, r], tn, preferred_element_type=F32)
        for a, b in blocks:
            o += lax.dot_general(
                vc[a:b, cols], p_buf[slot, a:b, r], tn, preferred_element_type=F32
            )

        o = o * m_buf[slot, 2:3, r]

        for g in range(first, end):
            to_o, to_s, at = own_o, own_s, g * hcount + h
            if packed and g == groups - 1:
                to_o, to_s, at = raw_o, raw_s, h
            to_o[at] = o[:, (g - first) * HD : (g - first + 1) * HD]
            to_s[at] = m_buf[slot, 3:4, g * HD : (g + 1) * HD]

    def project(g, p):
        deep = pl.ds(pl.multiple_of(p * pair * HD, HD), pair * HD)
        term = lax.dot_general(att[g, deep, :], w[deep, :], tn, preferred_element_type=F32)
        add(acc.at[g * HD : (g + 1) * HD, :], term, p)

    def project_last(s, p):
        deep = pl.ds(pl.multiple_of(p * splits * HD, HD), splits * HD)
        term = lax.dot_general(
            att[groups - 1 + s, deep, 0:sub], w[deep, :], tn, preferred_element_type=F32
        )
        add(acc.at[(groups - 1) * HD + s * sub : (groups - 1) * HD + (s + 1) * sub, :], term, p)

    def add(dest, term, p):
        @pl.when(p == 0)
        def _():
            dest[...] = term

        @pl.when(p > 0)
        def _():
            dest[...] += term

    pieces = [(g * HD, (g + 1) * HD) for g in range(groups - 1)]
    pieces += [((groups - 1) * HD + s * sub, (groups - 1) * HD + (s + 1) * sub) for s in range(splits)]

    def exchange(k):
        a, b = pieces[k]
        copies = []
        for d in range(1, heads_n):
            copies.append(
                pltpu.make_async_remote_copy(
                    src_ref=xs.at[d - 1, a:b],
                    dst_ref=xr.at[d - 1, a:b],
                    send_sem=x_send.at[d - 1],
                    recv_sem=x_recv.at[d - 1, k],
                    device_id={"head": lax.rem(hx + d, heads_n)},
                    device_id_type=MESH,
                )
            )
        return copies

    def exchange_start(k):
        a, b = pieces[k]
        cp = out_ref.shape[1]
        for d, c in enumerate(exchange(k)):
            peer = lax.rem(hx + d + 1, heads_n)
            cols = pl.ds(pl.multiple_of(peer * cp, HD), cp)
            xs[d, a:b] = acc[a:b, cols].astype(BF16)
            c.start()

    def service(t):
        cp_ = t - LAG * z
        in_p = (cp_ >= 0) & (cp_ < chunks)
        cs = t - LAG * (n - 1 - z)
        in_s = (cs >= 0) & (cs < chunks)

        @pl.when(in_s & (z < n - 1))
        def _():
            arrived(cs, -1)

        @pl.when(in_s & (z > 0))
        def _():
            combine(cs, suf_o, suf_s, left_o, left_s)
            for c in send(cs, -1)[::-1]:
                c.start()

        @pl.when(in_p & (z > 0))
        def _():
            arrived(cp_, 1)

        @pl.when(in_p & (z < n - 1))
        def _():
            combine(cp_, pre_o, pre_s, right_o, right_s)
            for c in send(cp_, 1)[::-1]:
                c.start()

    def finish(t):
        f = t - lag_end

        @pl.when((f >= 0) & (f < chunks))
        def _():
            m_a, m_b, m_c = own_s[f], pre_s[f], suf_s[f]
            top = jnp.maximum(m_a, jnp.maximum(m_b, m_c))
            e_a, e_b, e_c = jnp.exp2(m_a - top), jnp.exp2(m_b - top), jnp.exp2(m_c - top)
            share = 1.0 / (e_a + e_b + e_c)
            total_o = (
                own_o[f] * (e_a * share)
                + pre_o[f].astype(F32) * (e_b * share)
                + suf_o[f].astype(F32) * (e_c * share)
            )
            value = total_o.astype(BF16)

            @pl.when(f < last)
            def _():
                h = lax.rem(f, hcount)
                att[f // hcount, head_cols(h), :] = value

            @pl.when(f >= last)
            def _():
                k = f - last
                s, p = lax.div(k, tuples), lax.rem(k, tuples)
                for i in range(splits):
                    turned = value if i == 0 else pltpu.roll(total_o, HD - i * sub, 1).astype(BF16)
                    att[groups - 1 + s, head_cols(p * splits + i), :] = turned

        @pl.when(f == hcount - pairs)
        def _():
            w_load.wait()

        for g in range(groups - 1):
            begin = (g + 1) * hcount - pairs

            @pl.when((f >= begin) & (f < begin + pairs))
            def _(g=g, begin=begin):
                project(g, f - begin)

            if aligned:

                @pl.when(f == begin + pairs - 1)
                def _(g=g):
                    exchange_start(g)

        for s in range(splits):
            begin = last + s * tuples

            stop = begin + tuples - (1 if aligned and s == splits - 1 else 0)

            @pl.when((f >= begin) & (f < stop))
            def _(s=s, begin=begin):
                project_last(s, f - begin)

            if aligned and s < splits - 1:

                @pl.when(f == begin + tuples - 1)
                def _(s=s):
                    exchange_start(groups - 1 + s)

        if aligned:

            @pl.when(f == chunks - 1)
            def _():
                a, b = pieces[-1]
                cp = out_ref.shape[1]
                deep = slice((tuples - 1) * splits * HD, tuples * splits * HD)
                sums = att[groups + splits - 2, deep, 0:sub]

                def total_of(owner):
                    cols = pl.ds(pl.multiple_of(owner * cp, HD), cp)
                    before = 0.0 if tuples == 1 else acc[a:b, cols]
                    return cols, before + lax.dot_general(
                        sums, w[deep, cols], tn, preferred_element_type=F32
                    )

                for d, c in enumerate(exchange(len(pieces) - 1)):
                    xs[d, a:b] = total_of(lax.rem(hx + d + 1, heads_n))[1].astype(BF16)
                    c.start()
                cols, own = total_of(hx)
                acc[a:b, cols] = own

    def near(h):
        return jnp.minimum(h, hcount - 1)

    kv_loads[0].wait()
    for c in fresh_local:
        c.wait()
    for c in fresh_remote[0]:
        c.wait_recv()
    scores(0, 0)
    scores(min(1, hcount - 1), 1)
    def rescale(g):
        for c in sq_copies[g]:
            c.wait_recv()
        norm_total = squares[0, g]
        for d in range(1, heads_n):
            norm_total = norm_total + squares[d, g]
        scale[0:1, g * HD : (g + 1) * HD] = lax.rsqrt(norm_total / (HEADS * HD) + EPSILON) * (
            math.log2(math.e) / HD**0.5
        )

    rescale(0)
    soften(0, slice(0, HD))
    kv_loads[1].wait()
    weigh(0, 0, 0, 1)
    service(0)
    w_load.start()
    early = hcount > 1 and groups > 1
    if early:
        soften(1, slice(0, HD))
        weigh(1, 1, 0, 1)
        service(1)
    for g in range(1, groups):
        rescale(g)
    if groups > 1:
        soften(0, slice(HD, rows))
        weigh(0, 0, 1, groups)
    soften(1, slice(HD, rows) if early else slice(None))
    scores(min(2, hcount - 1), 0)

    unroll = 2

    def body(i, carry):
        for u in range(unroll):
            t = unroll * i + u
            if len(cuts) > 1:

                @pl.when(t + 3 == ahead)
                def _():
                    for c in fresh_remote[1]:
                        c.wait_recv()
                    for c in kv_loads[2:]:
                        c.wait()

            @pl.when(t + 1 < hcount)
            def _(t=t, u=u):
                scores(near(t + 3), (u + 1) % 2)
                soften(u % 2)
                weigh(t + 1, (u + 1) % 2)

            if packed:
                c = t + 1 + tuples

                @pl.when((c >= last) & (c < chunks))
                def _(c=c):
                    pack(c)

            finish(t)
            if early and u == 0:

                @pl.when(t > 0)
                def _(t=t):
                    service(t + 1)

            else:
                service(t + 1)
        return carry

    lax.fori_loop(0, -(-(chunks + LAG * (n - 1)) // unroll), body, 0)

    def settle():
        for d in range(1, seq_n):
            for side in (0, 1):
                fresh_wait(d, side, slice(0, width)).wait_send()
        for c in [c for copies in sq_copies for c in copies]:
            c.wait_send()

        @pl.when(z < n - 1)
        def _():
            settle_sends(1)

        @pl.when(z > 0)
        def _():
            settle_sends(-1)

    if aligned:
        cp = out_ref.shape[1]
        mine = pl.ds(pl.multiple_of(hx * cp, HD), cp)
        settle()
        for k, (a, b) in enumerate(pieces):
            summed = acc[a:b, mine]
            for d, c in enumerate(exchange(k)):
                c.wait_recv()
                summed = summed + xr[d, a:b].astype(F32)
            out_ref[a:b, :] = (summed * gate[...]).astype(out_ref.dtype)
        for d in range(1, heads_n):
            pltpu.make_async_remote_copy(
                src_ref=xs.at[d - 1],
                dst_ref=xr.at[d - 1],
                send_sem=x_send.at[d - 1],
                recv_sem=x_recv.at[d - 1, 0],
                device_id={"head": lax.rem(hx + d, heads_n)},
                device_id_type=MESH,
            ).wait_send()
    else:
        out_ref[...] = acc[...]
        settle()


def local(sizes, *args):
    (
        queries,
        query_gain,
        cache_keys,
        cache_values,
        finished_keys,
        finished_values,
        new_keys,
        new_values,
        out_weight,
        time_weight,
        owner,
        step,
    ) = args
    n, heads_n, seq_n = sizes
    rows, width = queries.shape
    hcount = width // HD
    cached, fresh = cache_keys.shape[0], finished_keys.shape[0]
    columns, cp = out_weight.shape[1], time_weight.shape[1]
    freq = time_weight.shape[0]
    aligned = cp % HD == 0
    any_spec = pl.BlockSpec(memory_space=pl.ANY)
    vmem = pl.BlockSpec(memory_space=pltpu.VMEM)
    dma = pltpu.SemaphoreType.DMA
    xcount = max(heads_n - 1, 1)
    groups = rows // HD
    chunks = groups * hcount
    ring = min(chunks, LAG * (n - 1) + 1)
    stat = (chunks, 1, HD)
    keys = cached + seq_n * 2 * fresh
    part = (chunks, HD, HD)
    result = pl.pallas_call(
        functools.partial(kernel, sizes, aligned),
        out_shape=pltpu.VMEM((rows, cp), BF16) if aligned else jax.ShapeDtypeStruct((rows, columns), F32),
        in_specs=[any_spec] * 12,
        out_specs=vmem,
        scratch_shapes=[
            pltpu.VMEM((rows, width), BF16),
            pltpu.VMEM((rows, width), BF16),
            pltpu.VMEM((width,), F32),
            pltpu.VMEM((cached, width), BF16),
            pltpu.VMEM((cached, width), BF16),
            pltpu.VMEM((seq_n, 2, fresh, width), BF16),
            pltpu.VMEM((seq_n, 2, fresh, width), BF16),
            pltpu.VMEM((width, columns), BF16),
            pltpu.VMEM((freq, cp), F32),
            pltpu.VMEM((heads_n, groups, 1, HD), F32),
            pltpu.VMEM((1, rows), F32),
            pltpu.VMEM(part, F32),
            pltpu.VMEM(stat, F32),
            pltpu.VMEM(part, BF16),
            pltpu.VMEM(stat, F32),
            pltpu.VMEM(part, BF16),
            pltpu.VMEM(stat, F32),
            pltpu.VMEM(part, BF16),
            pltpu.VMEM(stat, F32),
            pltpu.VMEM(part, BF16),
            pltpu.VMEM(stat, F32),
            pltpu.VMEM((groups + SPLIT - 1, width, HD), BF16),
            pltpu.VMEM((rows, columns), F32),
            pltpu.VMEM((1, cp), F32),
            pltpu.VMEM((xcount, rows, cp), BF16),
            pltpu.VMEM((xcount, rows, cp), BF16),
            dma((3,)),
            dma((2,)),
            dma((max(seq_n - 1, 1), 2)),
            dma((max(seq_n - 1, 1), 2, 2)),
            dma((xcount, groups)),
            dma((xcount, groups)),
            dma((2,)),
            dma((ring,)),
            dma((2,)),
            dma((ring,)),
            dma((xcount,)),
            dma((xcount, groups + SPLIT - 1)),
            pltpu.VMEM((2, keys, rows), F32),
            pltpu.VMEM((2, keys, rows), BF16),
            pltpu.VMEM((2, 4, rows), F32),
            dma((groups * PARTS,)),
            dma((2, 2)),
            pltpu.VMEM((HD // 2 + 1, 1, HD), F32),
            pltpu.VMEM((hcount, HD, HD), F32),
            pltpu.VMEM((hcount, 1, HD), F32),
            pltpu.SMEM((1, 1), jnp.int32),
            pltpu.SMEM((1, 1), jnp.int32),
            dma((2,)),
        ],
        compiler_params=pltpu.CompilerParams(
            collective_id=0, has_side_effects=True, vmem_limit_bytes=60 * 1024 * 1024
        ),
        name="sweep_attention",
    )(
        queries,
        query_gain,
        cache_keys,
        cache_values,
        finished_keys,
        finished_values,
        new_keys,
        new_values,
        out_weight,
        time_weight,
        owner,
        step,
    )
    if aligned:
        return result
    summed = lax.psum_scatter(result, "head", scatter_dimension=1, tiled=True)
    half = freq // 2
    frequency = jnp.exp(-jnp.log(10000.0) * jnp.arange(half, dtype=F32) / half)
    phases = step[0, 0].astype(F32) * frequency
    embedding = jnp.concatenate([jnp.cos(phases), jnp.sin(phases)])
    time_gate = 1.0 + jnp.dot(embedding, time_weight, precision=lax.Precision.HIGHEST)
    return (time_gate * summed).astype(BF16)


def solution(mesh):
    in_specs = (
        P(("grp", "seq"), "head"),
        P("head"),
        P(("grp", "slab"), "head"),
        P(("grp", "slab"), "head"),
        P(("grp", "slab", "seq"), "head"),
        P(("grp", "slab", "seq"), "head"),
        P(("grp", "slab", "seq"), "head"),
        P(("grp", "slab", "seq"), "head"),
        P("head", "slab"),
        P(None, ("slab", "head")),
        P("grp", None),
        P("grp", None),
    )
    out_specs = P(("grp", "seq"), ("slab", "head"))
    sizes = (mesh.shape["slab"], mesh.shape["head"], mesh.shape["seq"])
    mapped = jax.shard_map(
        functools.partial(local, sizes),
        mesh=mesh,
        in_specs=in_specs,
        out_specs=out_specs,
        check_vma=False,
    )

    def run(*args):
        return mapped(*args[:-2], args[-2].reshape(-1, 1), args[-1].reshape(-1, 1))

    return run
```
